32 devices in a mesh: seg: 8 (over z, x), bin: 4 (over y, core).
Axes of the slice: x: 2, y: 2, z: 4, core: 2. Of those that a mesh axis runs over, the one named last changes fastest.
Arguments:
- magnet_real: bfloat16 [64, 8, 32768], P('seg', None, 'bin'), may hold values from -8 to 8
- magnet_imag: bfloat16 [64, 8, 32768], P('seg', None, 'bin'), may hold values from -8 to 8
- detector_real: bfloat16 [64, 2, 32768], P('seg', None, 'bin'), may hold values from -8 to 8
- detector_imag: bfloat16 [64, 2, 32768], P('seg', None, 'bin'), may hold values from -8 to 8
- valid: int32 [64], P('seg'), may hold values 0 or 1
- intersection: float32 [32768], P('bin'), may hold values from 0.1 to 1
Outputs:
- cleaned_real: float32 [64, 32768], P('seg', 'bin')
- cleaned_imag: float32 [64, 32768], P('seg', 'bin')
- estimate: float32 [64], P('seg')
The draws below stay inside these ranges and needn't reach their ends.
Inputs may be any that keep to these rules, and one draw needn't show every extreme that they name: `valid`: 1 keeps a segment in the spectral sums, 0 vetoes it.
All inputs are finite; a program needn't handle non-finite values. No bound on the sum of `valid` on one device may be relied on, other than what follows from the above.
Results may differ from the reference program's by a relative error of at most 0.0005.
Values sent between devices are 32-bit elements; how exact they have to be, the bound alone decides.
A program may use at most 64 MiB of HBM per device.

```python
import math
import jax
import jax.numpy as jnp
from jax import lax

CHANNELS = 8
DETECTORS = 2
BINS = 32768
SEGS = 64


def schumann_sources(key):
    base = jax.random.fold_in(key, 9173)
    first, second = jax.random.split(base, 2)
    shape = (SEGS, 3, BINS)
    spread = 0.70710677
    src_real = jax.random.normal(first, shape, jnp.float32) * spread
    src_imag = jax.random.normal(second, shape, jnp.float32) * spread
    return (src_real, src_imag)


def complex_mixing(key, salt, rows):
    base = jax.random.fold_in(key, salt)
    first, second = jax.random.split(base, 2)
    spread = 0.57735027
    mix_real = jax.random.normal(first, (rows, 3, BINS), jnp.float32) * spread
    mix_imag = jax.random.normal(second, (rows, 3, BINS), jnp.float32) * spread
    return (mix_real, mix_imag)


def mixed_part(key, salt, rows, noise_scale, component):
    src_real, src_imag = schumann_sources(key)
    mix_real, mix_imag = complex_mixing(key, salt, rows)
    total = jnp.zeros((SEGS, rows, BINS), jnp.float32)
    for source in range(3):
        field_real = src_real[:, None, source, :]
        field_imag = src_imag[:, None, source, :]
        coeff_real = mix_real[None, :, source, :]
        coeff_imag = mix_imag[None, :, source, :]
        if component == 1:
            total = total + coeff_real * field_imag + coeff_imag * field_real
        else:
            total = total + coeff_real * field_real - coeff_imag * field_imag
    noise_key = jax.random.fold_in(key, salt + 1 + component)
    noise = jax.random.normal(noise_key, (SEGS, rows, BINS), jnp.float32) * noise_scale
    return total + noise


def magnet_component(key, component):
    values = mixed_part(key, 101, CHANNELS, 0.6, component)
    return jnp.clip(values, -8.0, 8.0).astype(jnp.bfloat16)


def detector_component(key, component):
    values = mixed_part(key, 211, DETECTORS, 0.7, component)
    return jnp.clip(values, -8.0, 8.0).astype(jnp.bfloat16)


def draw_magnet_real(key, part):
    return magnet_component(key, 0)


def draw_magnet_imag(key, part):
    return magnet_component(key, 1)


def draw_detector_real(key, part):
    return detector_component(key, 0)


def draw_detector_imag(key, part):
    return detector_component(key, 1)


def touch_ends(values, key, smallest, largest):
    longest = values.shape.index(max(values.shape))
    spots = []
    for shift in (0, 1):
        where = [jax.random.randint(jax.random.fold_in(key, axis), (), 0, length) for axis, length in enumerate(values.shape)]
        where[longest] = (where[longest] + shift) % values.shape[longest]
        spots.append(tuple(where))
    return values.at[spots[0]].set(smallest).at[spots[1]].set(largest)


def shard_levels(own_key, dims, cuts, least, top_value):
    loudness, own = 1.0, jax.random.fold_in(own_key, 6)
    for dim, parts in cuts:
        heights = jnp.exp(jax.random.uniform(jax.random.fold_in(own, dim), (parts,), jnp.float32, least / len(cuts), top_value / len(cuts)))
        loudness = loudness * jnp.repeat(heights, dims[dim] // parts).reshape([-1 if axis == dim else 1 for axis in range(len(dims))])
    return loudness


def setup_inputs(seed: int = 0) -> dict:
    seeds = jax.random.split(jax.random.key(seed), 7)
    return {
        "magnet_real": draw_magnet_real(jax.random.fold_in(seeds[6], 71), 0),
        "magnet_imag": draw_magnet_imag(jax.random.fold_in(seeds[6], 71), 0),
        "detector_real": draw_detector_real(jax.random.fold_in(seeds[6], 71), 0),
        "detector_imag": draw_detector_imag(jax.random.fold_in(seeds[6], 71), 0),
        "valid": touch_ends((jax.random.randint(seeds[4], (SEGS,), 0, 4) < 3).astype(jnp.int32), jax.random.fold_in(seeds[4], 1), 0, 1),
        "intersection": jnp.clip(jnp.exp(math.log(1.0) - 2.3025851 * jax.random.uniform(seeds[5], (BINS,), jnp.float32) ** shard_levels(seeds[5], (BINS,), ((0, 4),), -0.2, 0.2)), 0.1, 1.0),
    }


def wiener_solve(s_real, s_imag, p_real, p_imag):
    channels = s_real.shape[0]
    matrix_size = 2 * channels

    def matrix_entry(i, j):
        if i < channels and j < channels:
            value = s_real[i, j]
        elif i < channels:
            value = -s_imag[i, j - channels]
        elif j < channels:
            value = s_imag[i - channels, j]
        else:
            value = s_real[i - channels, j - channels]
        if i == j:
            value = value + 1.0
        return value

    def right_entry(i):
        if i < channels:
            return p_real[i]
        return p_imag[i - channels]
    factor = [[None] * matrix_size for i in range(matrix_size)]
    for j in range(matrix_size):
        running = matrix_entry(j, j)
        for k in range(j):
            running = running - factor[j][k] * factor[j][k]
        factor[j][j] = jnp.sqrt(running)
        inverse = 1.0 / factor[j][j]
        for i in range(j + 1, matrix_size):
            running = matrix_entry(i, j)
            for k in range(j):
                running = running - factor[i][k] * factor[j][k]
            factor[i][j] = running * inverse
    forward = []
    for i in range(matrix_size):
        running = right_entry(i)
        for k in range(i):
            running = running - factor[i][k] * forward[k]
        forward.append(running / factor[i][i])
    backward = [None] * matrix_size
    for i in reversed(range(matrix_size)):
        running = forward[i]
        for k in range(i + 1, matrix_size):
            running = running - factor[k][i] * backward[k]
        backward[i] = running / factor[i][i]
    return (jnp.stack(backward[:channels]), jnp.stack(backward[channels:]))

def reference(magnet_real, magnet_imag, detector_real, detector_imag, valid, intersection):
    block_bins = math.gcd(BINS, 1024)
    block_count = BINS // block_bins
    keep = valid.astype(jnp.float32)[:, None, None]

    def contract(left, right):
        return jnp.einsum('scf,sdf->cdf', left, right, precision=lax.Precision.HIGHEST)

    def project(filt, field):
        return jnp.einsum('ckf,scf->skf', filt, field, precision=lax.Precision.HIGHEST)

    def block_work(start):
        field_real = lax.dynamic_slice_in_dim(magnet_real, start, block_bins, 2).astype(jnp.float32)
        field_imag = lax.dynamic_slice_in_dim(magnet_imag, start, block_bins, 2).astype(jnp.float32)
        strain_real = lax.dynamic_slice_in_dim(detector_real, start, block_bins, 2).astype(jnp.float32)
        strain_imag = lax.dynamic_slice_in_dim(detector_imag, start, block_bins, 2).astype(jnp.float32)
        kept_real = field_real * keep
        kept_imag = field_imag * keep
        s_real = contract(kept_real, field_real) + contract(kept_imag, field_imag)
        s_imag = contract(kept_imag, field_real) - contract(kept_real, field_imag)
        p_real = contract(kept_real, strain_real) + contract(kept_imag, strain_imag)
        p_imag = contract(kept_imag, strain_real) - contract(kept_real, strain_imag)
        filt_real, filt_imag = wiener_solve(s_real, s_imag, p_real, p_imag)
        clean_real = strain_real - project(filt_real, field_real) - project(filt_imag, field_imag)
        clean_imag = strain_imag - project(filt_real, field_imag) + project(filt_imag, field_real)
        cross_real = clean_real[:, 0] * clean_real[:, 1] + clean_imag[:, 0] * clean_imag[:, 1]
        cross_imag = clean_imag[:, 0] * clean_real[:, 1] - clean_real[:, 0] * clean_imag[:, 1]
        return (cross_real, cross_imag)
    block_starts = jnp.arange(block_count, dtype=jnp.int32) * block_bins
    real_blocks, imag_blocks = lax.map(block_work, block_starts)
    cleaned_real = jnp.moveaxis(real_blocks, 0, 1).reshape(SEGS, BINS)
    cleaned_imag = jnp.moveaxis(imag_blocks, 0, 1).reshape(SEGS, BINS)
    summed = jnp.dot(cleaned_real, intersection, precision=lax.Precision.HIGHEST)
    estimate = summed / jnp.sqrt(jnp.sum(intersection * intersection))
    return (cleaned_real, cleaned_imag, estimate)
```

```python
import functools
import heapq

import jax
import jax.numpy as jnp
from jax import lax
from jax.experimental import pallas as pl
from jax.experimental.pallas import tpu as pltpu
from jax.sharding import PartitionSpec as P

LANES = 128
MESH = pl.DeviceIdType.MESH
RS_WEIGHTS = [1.0, 1.0, 1.5]


def largest_divisor(value, limit):
    return max(d for d in range(1, limit + 1) if value % d == 0)


def cadd_mul_conj(acc, a, b):
    return (acc[0] - a[0] * b[0] - a[1] * b[1], acc[1] - a[1] * b[0] + a[0] * b[1])


def csub_mul(acc, a, b):
    return (acc[0] - a[0] * b[0] + a[1] * b[1], acc[1] - a[0] * b[1] - a[1] * b[0])


def csub_conj_mul(acc, a, b):
    return (acc[0] - a[0] * b[0] - a[1] * b[1], acc[1] - a[0] * b[1] + a[1] * b[0])


def wiener_solve(below, diag, right):
    channels = len(diag)
    detectors = len(right[0])
    diag = list(diag)
    inverse = [None] * channels
    low = [[None] * channels for _ in range(channels)]
    for j in range(channels):
        inverse[j] = 1.0 / diag[j]
        for i in range(j + 1, channels):
            low[i][j] = (below[i][j][0] * inverse[j], below[i][j][1] * inverse[j])
        for i in range(j + 1, channels):
            a, l = below[i][j], low[i][j]
            diag[i] = diag[i] - l[0] * a[0] - l[1] * a[1]
            for k in range(j + 1, i):
                below[i][k] = cadd_mul_conj(below[i][k], l, below[k][j])
    out = []
    for det in range(detectors):
        y = []
        for i in range(channels):
            run = right[i][det]
            for k in range(i):
                run = csub_mul(run, low[i][k], y[k])
            y.append(run)
        w = [None] * channels
        for i in reversed(range(channels)):
            run = (y[i][0] * inverse[i], y[i][1] * inverse[i])
            for k in range(i + 1, channels):
                run = csub_conj_mul(run, low[k][i], w[k])
            w[i] = run
        out.append(w)
    return out


def step_weights(stages):
    return RS_WEIGHTS if stages == len(RS_WEIGHTS) else [1.0] * stages


def flood_order(n, stages, parts, weights, gather):
    free = [0.0] * stages
    heap, order, count = [], [], {}

    def send(now, st, q, k):
        free[st] = max(now, free[st]) + weights[st]
        heapq.heappush(heap, (free[st] + 0.6, st, q, k))

    if gather:
        for k in range(parts):
            for st in range(stages):
                send(0.0, st, 0, k)
    else:
        for q in first_order(n, stages):
            for k in range(parts):
                send(0.0, 0, q, k)
    while heap:
        now, st, q, k = heapq.heappop(heap)
        order.append((st, q, k))
        bit = n >> (st + 1)
        if gather:
            for to in range(st):
                send(now, to, q + bit, k)
        else:
            d = q - bit
            count[d, k] = count.get((d, k), 0) + 1
            if d and count[d, k] == stages - d.bit_length():
                send(now, stages - d.bit_length(), d, k)
    return order


def first_order(n, stages):
    def key(q):
        return [q >> bit & 1 for bit in range(stages)]

    return sorted(range(n // 2, n), key=key, reverse=True)


def halving_kernel(
    sizes, mr_ref, mi_ref, hr_ref, hi_ref, valid_ref, inter_ref,
    cr_ref, ci_ref, est_ref,
    s_ref, recv_ref, w_ref, mfr_ref, mfi_ref, hfr_ref, hfi_ref, ebuf_ref, erecv_ref,
    rs_send, rs_recv, ag_send, ag_recv, e_send, e_recv,
):
    n_seg, n_bin, segs, channels, detectors, blocks, chunks, wchunks = sizes
    stages = n_seg.bit_length() - 1
    half = channels // 2
    nblk = blocks // n_seg
    groups = channels + 2 * detectors
    per = groups // chunks
    wrows = 2 * channels * detectors
    wper = wrows // wchunks

    me = lax.axis_index("seg")
    my_bin = lax.axis_index("bin")
    bits = [lax.rem(lax.div(me, 1 << st), 2) for st in range(stages)]
    partner = [me + (1 - 2 * bits[st]) * (1 << st) for st in range(stages)]
    peers = [lax.rem(my_bin + d, n_bin) for d in range(1, n_bin)]

    barrier = pltpu.get_barrier_semaphore()
    for st in range(stages):
        pl.semaphore_signal(barrier, inc=1, device_id=(partner[st], my_bin), device_id_type=MESH)
    for peer in peers:
        pl.semaphore_signal(barrier, inc=1, device_id=(me, peer), device_id_type=MESH)

    def position(q):
        pos = 0
        for st in range(stages):
            digit = lax.rem(lax.div(q, n_seg >> (st + 1)), 2)
            pos = pos + (bits[st] + digit - 2 * bits[st] * digit) * (n_seg >> (st + 1))
        return pos

    sub = lax.broadcasted_iota(jnp.int32, (channels, LANES), 0)

    def spectra(q):
        pos = position(q)

        def body(blk, carry):
            b = pos * nblk + blk
            lanes = pl.ds(pl.multiple_of(b * LANES, LANES), LANES)
            acc = None
            for s in range(segs):
                mr = mr_ref[s, :, lanes].astype(jnp.float32)
                mi = mi_ref[s, :, lanes].astype(jnp.float32)
                hr = hr_ref[s, :, lanes].astype(jnp.float32)
                hi = hi_ref[s, :, lanes].astype(jnp.float32)
                mfr_ref[b, pl.ds(s * channels, channels), :] = mr
                mfi_ref[b, pl.ds(s * channels, channels), :] = mi
                hfr_ref[b, pl.ds(s * detectors, detectors), :] = hr
                hfi_ref[b, pl.ds(s * detectors, detectors), :] = hi
                v = valid_ref[s].astype(jnp.float32)
                kr, ki = mr * v, mi * v
                terms = [kr * mr + ki * mi]
                for r in range(1, half + 1):
                    br = pltpu.roll(mr, channels - r, 0)
                    bi = pltpu.roll(mi, channels - r, 0)
                    terms.append(kr * br + ki * bi)
                    terms.append(ki * br - kr * bi)
                for k in range(detectors):
                    br = jnp.broadcast_to(hr[k : k + 1], (channels, LANES))
                    bi = jnp.broadcast_to(hi[k : k + 1], (channels, LANES))
                    terms.append(kr * br + ki * bi)
                    terms.append(ki * br - kr * bi)
                acc = terms if acc is None else [a + t for a, t in zip(acc, terms)]
            packed = jnp.where(sub < half, acc[channels - 1], acc[channels])
            rows = acc[: channels - 1] + [packed] + acc[channels + 1 :]
            for g in range(groups):
                at = pl.multiple_of((g % per) * nblk * channels + blk * channels, channels)
                s_ref[q, g // per, pl.ds(at, channels), :] = rows[g]
            return carry

        lax.fori_loop(0, nblk, body, 0)

    def rs_copy(st, q, k):
        return pltpu.make_async_remote_copy(
            src_ref=s_ref.at[q, k],
            dst_ref=recv_ref.at[q - 1, k],
            send_sem=rs_send.at[q - 1, k],
            recv_sem=rs_recv.at[q - 1, k],
            device_id=(partner[st], my_bin),
            device_id_type=MESH,
        )

    first = first_order(n_seg, stages)
    assert first[0] == n_seg - 1
    spectra(first[0])
    pl.semaphore_wait(barrier, stages + n_bin - 1)
    for k in range(chunks):
        rs_copy(0, first[0], k).start()

    def mirrored(i, low):
        q = 0 if low else n_seg // 2
        for bit in range(stages - 1):
            digit = 1 - lax.rem(lax.div(i, n_seg >> (bit + 2)), 2)
            q = q + digit * (1 << bit)
        return q

    def early(i, carry):
        q = mirrored(i, False)
        spectra(q)
        for k in range(chunks):
            rs_copy(0, q, k).start()
        return carry

    lax.fori_loop(1, n_seg // 2, early, 0)

    def late(i, carry):
        spectra(mirrored(i, True))
        return carry

    lax.fori_loop(0, n_seg // 2, late, 0)

    got = {}
    for st, q, k in flood_order(n_seg, stages, chunks, step_weights(stages), False):
        rs_copy(st, q, k).wait_recv()
        d = q - (n_seg >> (st + 1))
        s_ref[d, k] = s_ref[d, k] + recv_ref[q - 1, k]
        got[d, k] = got.get((d, k), 0) + 1
        if d and got[d, k] == stages - d.bit_length():
            rs_copy(stages - d.bit_length(), d, k).start()

    def entry(g, row):
        start = (g % per) * nblk * channels + row
        if nblk == 1:
            return s_ref[0, g // per, pl.ds(start, 1), :]
        return s_ref[0, g // per, pl.ds(start, nblk, stride=channels), :]

    def above(a, b):
        r = b - a
        if r < half:
            return (entry(2 * r - 1, a), entry(2 * r, a))
        if r == half:
            return (entry(channels - 1, a), -entry(channels - 1, a + half))
        r = channels - r
        return (entry(2 * r - 1, b), -entry(2 * r, b))

    below = [[None] * channels for _ in range(channels)]
    for i in range(channels):
        for j in range(i):
            value = above(j, i)
            below[i][j] = (value[0], -value[1])
    diag = [entry(0, c) + 1.0 for c in range(channels)]
    right = [
        [(entry(channels + 2 * k, c), entry(channels + 2 * k + 1, c)) for k in range(detectors)]
        for c in range(channels)
    ]
    filt = wiener_solve(below, diag, right)
    for k in range(detectors):
        for c in range(channels):
            for part in range(2):
                e = (k * channels + c) * 2 + part
                w_ref[0, e // wper, pl.ds((e % wper) * nblk, nblk), :] = filt[k][c][part]

    def ag_copy(st, q, k):
        to = q + (n_seg >> (st + 1))
        return pltpu.make_async_remote_copy(
            src_ref=w_ref.at[q, k],
            dst_ref=w_ref.at[to, k],
            send_sem=ag_send.at[to - 1, k],
            recv_sem=ag_recv.at[to - 1, k],
            device_id=(partner[st], my_bin),
            device_id_type=MESH,
        )

    def clean(q, carry):
        pos = position(q)

        def body(blk, carry):
            num, sq = carry
            b = pos * nblk + blk
            lanes = pl.ds(pl.multiple_of(b * LANES, LANES), LANES)
            g = [
                (
                    hfr_ref[b, pl.ds(k, segs, stride=detectors), :],
                    hfi_ref[b, pl.ds(k, segs, stride=detectors), :],
                )
                for k in range(detectors)
            ]
            for c in range(channels):
                m = (
                    mfr_ref[b, pl.ds(c, segs, stride=channels), :],
                    mfi_ref[b, pl.ds(c, segs, stride=channels), :],
                )
                for k in range(detectors):
                    e = (k * channels + c) * 2
                    w = [
                        w_ref[q, f // wper, pl.ds((f % wper) * nblk + blk, 1), :]
                        for f in (e, e + 1)
                    ]
                    g[k] = csub_conj_mul(g[k], w, m)
            real = g[0][0] * g[1][0] + g[0][1] * g[1][1]
            imag = g[0][1] * g[1][0] - g[0][0] * g[1][1]
            cr_ref[:, lanes] = real
            ci_ref[:, lanes] = imag
            weight = inter_ref[pl.ds(b, 1), :]
            return num + real * weight, sq + weight * weight

        return lax.fori_loop(0, nblk, body, carry)

    for k in range(wchunks):
        for st in range(stages):
            ag_copy(st, 0, k).start()
    sums = clean(0, (jnp.zeros((segs, LANES), jnp.float32), jnp.zeros((1, LANES), jnp.float32)))
    seen = {}
    for st, q, k in flood_order(n_seg, stages, wchunks, step_weights(stages), True):
        ag_copy(st, q, k).wait_recv()
        to = q + (n_seg >> (st + 1))
        for on in range(st):
            ag_copy(on, to, k).start()
        seen[to] = seen.get(to, 0) + 1
        if seen[to] == wchunks:
            sums = clean(to, sums)
    num, sq = sums
    ebuf_ref[pl.ds(0, segs), :] = num
    ebuf_ref[pl.ds(segs, segs), :] = jnp.broadcast_to(sq, (segs, LANES))

    def e_copy(d):
        return pltpu.make_async_remote_copy(
            src_ref=ebuf_ref,
            dst_ref=erecv_ref.at[d],
            send_sem=e_send.at[d],
            recv_sem=e_recv.at[d],
            device_id=(me, peers[d]),
            device_id_type=MESH,
        )

    for d in range(n_bin - 1):
        e_copy(d).start()
    for q in range(1, n_seg):
        st = stages - q.bit_length()
        for k in range(chunks):
            rs_copy(st, q, k).wait_send()
        for k in range(wchunks):
            ag_copy(st, q - (n_seg >> (st + 1)), k).wait_send()
    total = ebuf_ref[...]
    for d in range(n_bin - 1):
        e_copy(d).wait_recv()
        total = total + erecv_ref[d]
    total = jnp.sum(total, axis=1, keepdims=True)
    est_ref[...] = jnp.broadcast_to(total[:segs] / jnp.sqrt(total[segs:]), (segs, LANES))
    for d in range(n_bin - 1):
        e_copy(d).wait_send()


def halving_on_device(n_seg, n_bin, magnet_real, magnet_imag, detector_real, detector_imag, valid, intersection):
    segs, channels, bins = magnet_real.shape
    detectors = detector_real.shape[1]
    blocks = bins // LANES
    nblk = blocks // n_seg
    groups = channels + 2 * detectors
    chunks = largest_divisor(groups, 4)
    wrows = 2 * channels * detectors
    wchunks = largest_divisor(wrows, 2)
    rows = groups // chunks * nblk * channels
    f32 = jnp.float32
    sizes = (n_seg, n_bin, segs, channels, detectors, blocks, chunks, wchunks)
    vmem = pl.BlockSpec(memory_space=pltpu.VMEM)
    cleaned_real, cleaned_imag, estimate = pl.pallas_call(
        functools.partial(halving_kernel, sizes),
        out_shape=(
            jax.ShapeDtypeStruct((segs, bins), f32),
            jax.ShapeDtypeStruct((segs, bins), f32),
            jax.ShapeDtypeStruct((segs, LANES), f32),
        ),
        in_specs=[vmem] * 4 + [pl.BlockSpec(memory_space=pltpu.SMEM), vmem],
        out_specs=(vmem, vmem, vmem),
        scratch_shapes=[
            pltpu.VMEM((n_seg, chunks, rows, LANES), f32),
            pltpu.VMEM((n_seg - 1, chunks, rows, LANES), f32),
            pltpu.VMEM((n_seg, wchunks, wrows // wchunks * nblk, LANES), f32),
            pltpu.VMEM((blocks, segs * channels, LANES), f32),
            pltpu.VMEM((blocks, segs * channels, LANES), f32),
            pltpu.VMEM((blocks, segs * detectors, LANES), f32),
            pltpu.VMEM((blocks, segs * detectors, LANES), f32),
            pltpu.VMEM((2 * segs, LANES), f32),
            pltpu.VMEM((n_bin - 1, 2 * segs, LANES), f32),
        ]
        + [
            pltpu.SemaphoreType.DMA((n_seg - 1, chunks)),
            pltpu.SemaphoreType.DMA((n_seg - 1, chunks)),
            pltpu.SemaphoreType.DMA((n_seg - 1, wchunks)),
            pltpu.SemaphoreType.DMA((n_seg - 1, wchunks)),
            pltpu.SemaphoreType.DMA((n_bin - 1,)),
            pltpu.SemaphoreType.DMA((n_bin - 1,)),
        ],
        compiler_params=pltpu.CompilerParams(
            collective_id=0, has_side_effects=True, vmem_limit_bytes=56 * 1024 * 1024
        ),
    )(
        magnet_real, magnet_imag, detector_real, detector_imag, valid,
        intersection.reshape(blocks, LANES),
    )
    return cleaned_real, cleaned_imag, estimate[:, 0]


LINE = 4
ROW_US = 0.01128
HOP_US = (0.0, 2.6, 3.0, 3.4)
GROUP_SETS = ((0, 1), (2, 3))


def split_pieces(nblk):
    sizes = [1] * nblk
    return [(n, "A") for n in sizes[:-1]] + [(sizes[-1], "B")]


def ag_modes(count):
    direct = min(2, count - 1)
    return "".join("C" if p < 2 else "Y" if p < count - 1 - direct else "Z" for p in range(count - 1)) + "2"


def tick_order(pieces):
    first = [p for p, (_, kind) in enumerate(pieces) if kind == "A"]
    order = [(first[0], 0), (first[0], 1)]
    for p, nxt in zip(first, first[1:] + [None]):
        if nxt is not None:
            order += [(nxt, 0), (nxt, 1)]
        order += [(p, 2), (p, 3)]
    return order + [(p, 3) for p, (_, kind) in enumerate(pieces) if kind == "B"]


class Planner:
    def __init__(self, pieces, modes, order, depth, rows, wrows):
        self.pieces, self.modes, self.order, self.depth = pieces, modes, order, depth
        self.rows, self.wrows = rows, wrows
        self.clock = [2.0, 2.0]
        self.link, self.message, self.steps = {}, {}, []

    def send(self, role, key, path, rows):
        start = self.clock[role]
        for name in path:
            start = max(start, self.link.get(name, 0.0))
            self.link[name] = start + rows * ROW_US
        self.message[key] = start + rows * ROW_US + HOP_US[len(path)]

    def waits(self, op):
        kind, p = op[0], op[1]
        if kind == "XR":
            return [[("x", 0, p, op[2])], [("x", 1, p, op[2])]]
        if kind == "ZI":
            return [[], [("z", 1, p, op[2])]]
        if kind == "FIN":
            return [[("z", 0, p, 0), ("z", 0, p, 1)], [("z", 1, p, 2), ("z", 1, p, 3)]]
        if kind == "AGX":
            return [[("ax", 0, p)], [("ax", 1, p)]]
        if kind == "RL":
            return [[], [("a", 1, p, op[2], 0)]]
        if kind == "AG":
            both = [[("a", r, p, op[2], op[3])] for r in range(2)]
            if self.modes[p] in "CY" and op[3] == 0:
                both[1] = []
            return both
        return [[], []]

    def column(self, p, side, rows, chain):
        self.send(0, ("a", 1, p, 2, side), ["in"], rows)
        self.send(1, ("a", 0, p, 2, side), ["out"], rows)
        self.send(1, ("a", 1, p, 1, side), ["mid"], rows)
        if not chain:
            self.send(0, ("a", 1, p, 0, side), ["in", "mid"], rows)
            self.send(1, ("a", 0, p, 1, side), ["mid", "out"], rows)
            self.send(0, ("a", 0, p, 0, side), ["in", "mid", "out"], rows)

    def lines(self, p, r, rows):
        if r < 3:
            self.send(0, ("z", 1, p, r), ["in"], rows)
        if r == 2:
            self.send(1, ("z", 0, p, 0), ["out"], rows)

    def run(self, op):
        for role, keys in enumerate(self.waits(op)):
            self.clock[role] = max([self.clock[role]] + [self.message[key] for key in keys]) + 0.05
        kind, p = op[0], op[1]
        size, form = self.pieces[p]
        rows, wrows, mode = self.rows * size, self.wrows * size, self.modes[p]
        work = 0.0
        if kind == "SP":
            work = 0.13 * size * len(op[3]) * len(op[2])
        elif kind == "XS":
            for role in range(2):
                self.send(role, ("x", role, p, op[2]), [("x", role)], rows)
        elif kind == "XR":
            work = 0.03 * size
        elif kind == "FIN":
            work = 0.06 * size
        elif kind == "SOLVE":
            work = 0.6 + 0.06 * size
        elif kind in ("AGX", "AG"):
            work = 0.06 * size * (2 if kind == "AG" and mode == "C" else 1)
        self.clock = [c + (0.0 if kind in ("SOLVE", "AGX", "AG") else work) for c in self.clock]
        if kind == "XR" and form == "A":
            self.lines(p, op[2], rows)
        elif kind == "ZS":
            self.lines(p, op[2], rows * 2)
        elif kind == "ZI":
            both = rows * (2 if form == "B" else 1)
            if op[2] == 1:
                self.send(1, ("z", 1, p, 3), ["mid"], both)
            else:
                self.send(1, ("z", 0, p, 1), ["mid", "out"], both)
        elif kind == "SOLVE":
            self.clock = [c + 0.6 for c in self.clock]
            for role in range(2):
                self.send(role, ("ax", role, p), [("x", role)], wrows)
            if mode in "2YZ":
                self.column(p, 0, wrows, mode == "Y")
            work = work - 0.6
        elif kind == "AGX":
            if mode in "2C":
                self.column(p, 0 if mode == "C" else 1, wrows * (2 if mode == "C" else 1), mode == "C")
        elif kind == "RL":
            both = wrows * (2 if mode == "C" else 1)
            if op[2] == 2:
                self.send(1, ("a", 1, p, 0, 0), ["mid"], both)
            else:
                self.send(1, ("a", 0, p, op[2], 0), ["out"], both)
        elif kind == "AG" and mode in "YZ" and op[3] == 0:
            for role in range(2):
                self.send(role, ("a", role, p, op[2], 1), [("x", role)], wrows)
        if kind in ("SOLVE", "AGX", "AG"):
            self.clock = [c + work for c in self.clock]
        self.steps.append(op)

    def spectra_steps(self):
        lead = self.order[0]
        for p, (_, form) in enumerate(self.pieces):
            for group in GROUP_SETS:
                if (p, group[0]) == lead:
                    yield ("SP", p, (group[0],), (1,))
                    yield ("SP", p, (group[0],), (0,))
                    yield ("SP", p, group[1:], (1, 0))
                else:
                    yield ("SP", p, group, (1, 0))

    def needs(self):
        need, order = {}, self.order
        made = {}
        for op in self.spectra_steps():
            need[op] = []
            for r in op[2]:
                for side in op[3]:
                    made[op[1], r, side] = op
        for i, (p, r) in enumerate(order):
            back = [("XR",) + order[i - self.depth]] if i >= self.depth else []
            back += [("XS",) + order[i - 1]] if i else []
            chain = [("XR",) + order[i - 1]] if i else []
            if self.pieces[p][1] == "A":
                need["XS", p, r] = [made[p, r, 1]] + back
                need["XR", p, r] = [("XS", p, r), made[p, r, 0]] + chain
            else:
                need["XS", p, r] = [("FIN", p)] + back
                need["XR", p, r] = [("XS", p, r)] + chain
        for p, (_, form) in enumerate(self.pieces):
            kind = "XR" if form == "A" else "ZS"
            if form == "B":
                for r in range(3):
                    need["ZS", p, r] = [made[p, r, 0], made[p, r, 1]]
            for r in range(2):
                need["ZI", p, r] = [(kind, p, r)]
            need["FIN", p] = [("ZI", p, 0), ("ZI", p, 1), (kind, p, 2)]
            need["FIN", p] += [("XR", p, 3)] if form == "A" else [made[p, 3, 0], made[p, 3, 1]]
            need["SOLVE", p] = [("FIN", p) if form == "A" else ("XR", p, 3)]
            need["AGX", p] = [("SOLVE", p)]
            mode = self.modes[p]
            start = ("AGX", p) if mode == "C" else ("SOLVE", p)
            for slot in (2, 1, 0):
                if mode in "CY":
                    need["RL", p, slot] = [start]
                    need["AG", p, slot, 0] = [("RL", p, slot)]
                else:
                    need["AG", p, slot, 0] = [start]
                if mode in "YZ":
                    need["AG", p, slot, 1] = [("AG", p, slot, 0)]
                elif mode == "2":
                    need["AG", p, slot, 1] = [("AGX", p)]
        return need

    def plan(self):
        need = self.needs()
        place = {op: i for i, op in enumerate(need)}
        tick = {key: i for i, key in enumerate(self.order)}
        done = set()
        while len(done) < len(need):
            best = None
            for op in need:
                if op in done or any(other not in done for other in need[op]):
                    continue
                keys = self.waits(op)
                if any(key not in self.message for role in range(2) for key in keys[role]):
                    continue
                ready = max(max([self.clock[r]] + [self.message[key] for key in keys[r]]) for r in range(2))
                now = max(self.clock)
                urgent = -1.0
                if op[0] in ("SP", "ZS") and ready <= now + 1e-6:
                    form = self.pieces[op[1]][1]
                    r = op[2] if op[0] == "ZS" else op[2][0]
                    urgent = 2.5 + 0.1 * r if form == "B" else tick[op[1], r]
                key = (round(max(ready, now), 3), urgent, place[op])
                if best is None or key < best[0]:
                    best = (key, op)
            self.run(best[1])
            done.add(best[1])
        return self.steps


def line_kernel(sizes, mr_hbm, mi_hbm, hr_hbm, hi_hbm, valid_hbm, inter_hbm, cr_hbm, ci_hbm, est_ref, *scratch):
    n_seg, n_bin, segs, channels, detectors, nblk, pieces, modes, steps = sizes
    count = len(pieces)
    half = channels // 2
    groups = channels + 2 * detectors
    rows = groups * channels
    wrows = 2 * channels * detectors
    scratch = list(scratch)
    take = lambda n: [scratch.pop(0) for _ in range(n)]
    s_refs, x_refs, z_refs, w_refs = take(count), take(count), take(count), take(count)
    mr_ref, mi_ref, hr_ref, hi_ref, valid_ref, inter_ref, cr_ref, ci_ref = take(8)
    mfr_ref, mfi_ref, hfr_ref, hfi_ref, ebuf_ref, erecv_ref = take(6)
    x_send, x_recv, z_send, z_recv, a_send, a_recv, e_send, e_recv, in_sem, small_sem, out_sem = take(11)

    me = lax.axis_index("seg")
    my_bin = lax.axis_index("bin")
    x = lax.rem(me, 2)
    z = lax.div(me, 2)
    z_hi, z_lo = lax.div(z, 2), lax.rem(z, 2)
    mid = z_hi + z_lo - 2 * z_hi * z_lo
    is_mid, is_end = mid == 1, mid == 0
    sib = 2 * z_hi + 1 - z_lo
    far_mid = 2 - z_hi
    far_end = 3 - 3 * z_hi
    line = {3: z, 2: sib, 1: far_mid, 0: far_end}
    partner = (2 * z + 1 - x, my_bin)
    peers = [lax.rem(my_bin + d, n_bin) for d in range(1, n_bin)]

    def column(where):
        return (2 * line[where] + x, my_bin)

    def lanes_of(r, side):
        return 2 * line[r] + x + side - 2 * side * x

    barrier = pltpu.get_barrier_semaphore()
    for d in range(1, n_seg):
        pl.semaphore_signal(barrier, inc=1, device_id=(lax.rem(me + d, n_seg), my_bin), device_id_type=MESH)
    for peer in peers:
        pl.semaphore_signal(barrier, inc=1, device_id=(me, peer), device_id_type=MESH)

    small = [
        pltpu.make_async_copy(valid_hbm, valid_ref, small_sem.at[0]),
        pltpu.make_async_copy(inter_hbm, inter_ref, small_sem.at[1]),
    ]
    small[0].start()
    loads = {}
    for i, (r, side) in enumerate([(r, side) for r in range(4) for side in (1, 0)]):
        lanes = pl.ds(pl.multiple_of(lanes_of(r, side) * nblk * LANES, nblk * LANES), nblk * LANES)
        loads[r, side] = [
            pltpu.make_async_copy(src.at[:, :, lanes], dst.at[:, :, lanes], in_sem.at[i, j])
            for j, (src, dst) in enumerate(
                [(mr_hbm, mr_ref), (mi_hbm, mi_ref), (hr_hbm, hr_ref), (hi_hbm, hi_ref)]
            )
        ]
        for copy in loads[r, side]:
            copy.start()
    small[1].start()
    small[0].wait()

    first_block = [sum(size for size, _ in pieces[:p]) for p in range(count)]
    sub = lax.broadcasted_iota(jnp.int32, (channels, LANES), 0)
    loaded = set()

    def spectra(p, where, sides):
        size = pieces[p][0]
        for r in where:
            for side in sides:
                if (r, side) not in loaded:
                    loaded.add((r, side))
                    for copy in loads[r, side]:
                        copy.wait()

        def body(i, carry):
            r = where[0] + lax.div(i, size * len(sides))
            side = sides[0] if len(sides) == 1 else 1 - lax.rem(lax.div(i, size), 2)
            blk = lax.rem(i, size)
            if len(where) == 1:
                at = line[where[0]]
            else:
                at = line[where[0]] + (r - where[0]) * (line[where[1]] - line[where[0]])
            owner = 2 * at + x + side - 2 * side * x
            b = owner * nblk + first_block[p] + blk
            lanes = pl.ds(pl.multiple_of(b * LANES, LANES), LANES)
            acc = None
            for s in range(segs):
                mr = mr_ref[s, :, lanes].astype(jnp.float32)
                mi = mi_ref[s, :, lanes].astype(jnp.float32)
                hr = hr_ref[s, :, lanes].astype(jnp.float32)
                hi = hi_ref[s, :, lanes].astype(jnp.float32)
                mfr_ref[b, pl.ds(s * channels, channels), :] = mr
                mfi_ref[b, pl.ds(s * channels, channels), :] = mi
                hfr_ref[b, pl.ds(s * detectors, detectors), :] = hr
                hfi_ref[b, pl.ds(s * detectors, detectors), :] = hi
                v = valid_ref[s].astype(jnp.float32)
                kr, ki = mr * v, mi * v
                terms = [kr * mr + ki * mi]
                for turn in range(1, half + 1):
                    br = pltpu.roll(mr, channels - turn, 0)
                    bi = pltpu.roll(mi, channels - turn, 0)
                    terms.append(kr * br + ki * bi)
                    terms.append(ki * br - kr * bi)
                for k in range(detectors):
                    br = jnp.broadcast_to(hr[k : k + 1], (channels, LANES))
                    bi = jnp.broadcast_to(hi[k : k + 1], (channels, LANES))
                    terms.append(kr * br + ki * bi)
                    terms.append(ki * br - kr * bi)
                acc = terms if acc is None else [a + t for a, t in zip(acc, terms)]
            packed = jnp.where(sub < half, acc[channels - 1], acc[channels])
            out = acc[: channels - 1] + [packed] + acc[channels + 1 :]
            for g in range(groups):
                start = pl.multiple_of((g * size + blk) * channels, channels)
                s_refs[p][r, side, pl.ds(start, channels), :] = out[g]
            return carry

        lax.fori_loop(0, size * len(sides) * len(where), body, 0)

    def solve(p):
        size = pieces[p][0]
        ref = s_refs[p]

        def entry(g, row):
            start = g * size * channels + row
            if size == 1:
                return ref[3, 0, pl.ds(start, 1), :]
            return ref[3, 0, pl.ds(start, size, stride=channels), :]

        def above(a, b):
            r = b - a
            if r < half:
                return (entry(2 * r - 1, a), entry(2 * r, a))
            if r == half:
                return (entry(channels - 1, a), -entry(channels - 1, a + half))
            r = channels - r
            return (entry(2 * r - 1, b), -entry(2 * r, b))

        below = [[None] * channels for _ in range(channels)]
        for i in range(channels):
            for j in range(i):
                value = above(j, i)
                below[i][j] = (value[0], -value[1])
        diag = [entry(0, c) + 1.0 for c in range(channels)]
        right = [
            [(entry(channels + 2 * k, c), entry(channels + 2 * k + 1, c)) for k in range(detectors)]
            for c in range(channels)
        ]
        filt = wiener_solve(below, diag, right)
        for k in range(detectors):
            for c in range(channels):
                for part in range(2):
                    e = (k * channels + c) * 2 + part
                    w_refs[p][3, 0, pl.ds(e * size, size), :] = filt[k][c][part]

    def clean(p, r, sides):
        size = pieces[p][0]

        def body(i, carry):
            if len(sides) == 1:
                side, blk = sides[0], i
            else:
                side, blk = lax.div(i, size), lax.rem(i, size)
            b = lanes_of(r, side) * nblk + first_block[p] + blk
            lanes = pl.ds(pl.multiple_of(b * LANES, LANES), LANES)
            g = [
                (
                    hfr_ref[b, pl.ds(k, segs, stride=detectors), :],
                    hfi_ref[b, pl.ds(k, segs, stride=detectors), :],
                )
                for k in range(detectors)
            ]
            for c in range(channels):
                m = (
                    mfr_ref[b, pl.ds(c, segs, stride=channels), :],
                    mfi_ref[b, pl.ds(c, segs, stride=channels), :],
                )
                for k in range(detectors):
                    e = (k * channels + c) * 2
                    w = [w_refs[p][r, side, pl.ds(f * size + blk, 1), :] for f in (e, e + 1)]
                    g[k] = csub_conj_mul(g[k], w, m)
            real = g[0][0] * g[1][0] + g[0][1] * g[1][1]
            imag = g[0][1] * g[1][0] - g[0][0] * g[1][1]
            cr_ref[:, lanes] = real
            ci_ref[:, lanes] = imag
            ebuf_ref[pl.ds(0, segs), :] = ebuf_ref[pl.ds(0, segs), :] + real * inter_ref[pl.ds(b, 1), :]
            return carry

        if size * len(sides) == 1:
            body(0, 0)
        else:
            lax.fori_loop(0, size * len(sides), body, 0)

    started = []

    def remote(src, dst, send_sem, recv_sem, device):
        return pltpu.make_async_remote_copy(
            src_ref=src, dst_ref=dst, send_sem=send_sem, recv_sem=recv_sem,
            device_id=device, device_id_type=MESH,
        )

    def start(copy, when=None):
        started.append((when, copy))
        if when is None:
            copy.start()
        else:
            pl.when(when)(copy.start)

    def x_copy(p, r):
        src, dst = (s_refs[p].at[r, 1], x_refs[p].at[r]) if pieces[p][1] == "A" else (s_refs[p].at[3, 1], x_refs[p].at[0])
        return remote(src, dst, x_send.at[p, r], x_recv.at[p, r], partner)

    def part(p, r):
        return s_refs[p].at[r, 0] if pieces[p][1] == "A" else s_refs[p].at[r]

    def z_copy(p, r, slot, where):
        return remote(part(p, r), z_refs[p].at[slot], z_send.at[p, r], z_recv.at[p, slot], column(where))

    def send_in(p, r):
        if r < 3:
            start(z_copy(p, r, r, 2), is_end)
        if r == 2:
            start(z_copy(p, r, 0, 2), is_mid)

    def add(p, r, slot):
        ref = part(p, r)
        ref[...] = ref[...] + z_refs[p][slot]

    sends = [0] * count

    def a_copy(p, src, dst, slot_at, device):
        sends[p] += 1
        return remote(src, dst, a_send.at[p, sends[p] - 1], a_recv.at[p, slot_at[0], slot_at[1]], device)

    def a_wait(p, slot, side, both=False):
        ref = w_refs[p].at[slot] if both else w_refs[p].at[slot, side]
        remote(ref, ref, a_send.at[p, 0], a_recv.at[p, slot, side], partner).wait_recv()

    def spread(p, side, both, chain):
        src = w_refs[p].at[3] if both else w_refs[p].at[3, side]

        def to(slot, where, when=None):
            dst = w_refs[p].at[slot] if both else w_refs[p].at[slot, side]
            start(a_copy(p, src, dst, (slot, side), column(where)), when)

        to(2, 2)
        to(mid, 1, is_mid if chain else None)
        if not chain:
            to(mid, 0)

    def relay(p, slot):
        both = modes[p] == "C"
        pick = (lambda n: w_refs[p].at[n]) if both else (lambda n: w_refs[p].at[n, 0])
        to, where = (0, 1) if slot == 2 else (slot, 2)
        copy = a_copy(p, pick(slot), pick(to), (to, 0), column(where))
        started.append((is_mid, copy))

        @pl.when(is_mid)
        def _():
            a_wait(p, slot, 0, both)
            copy.start()

    ebuf_ref[pl.ds(0, segs), :] = jnp.zeros((segs, LANES), jnp.float32)
    entered = False
    for op in steps:
        kind, p = op[0], op[1]
        form, mode = pieces[p][1], modes[p]
        if kind == "SP":
            spectra(p, op[2], op[3])
            continue
        if not entered:
            pl.semaphore_wait(barrier, n_seg + n_bin - 2)
            entered = True
        if kind == "XS":
            start(x_copy(p, op[2]))
        elif kind == "XR":
            r = op[2]
            x_copy(p, r).wait_recv()
            if form == "A":
                s_refs[p][r, 0] = s_refs[p][r, 0] + x_refs[p][r]
                send_in(p, r)
            else:
                s_refs[p][3, 0] = s_refs[p][3, 0] + x_refs[p][0]
        elif kind == "ZS":
            send_in(p, op[2])
        elif kind == "ZI":
            r = op[2]
            copy = z_copy(p, r, 3, 1) if r == 1 else z_copy(p, r, 1, 0)
            started.append((is_mid, copy))

            @pl.when(is_mid)
            def _():
                z_copy(p, r, r, 2).wait_recv()
                add(p, r, r)
                copy.start()
        elif kind == "FIN":
            for when, slots in ((is_end, (0, 1)), (is_mid, (2, 3))):

                @pl.when(when)
                def _():
                    for slot in slots:
                        z_copy(p, 3, slot, 2).wait_recv()
                        add(p, 3, slot)
        elif kind == "SOLVE":
            solve(p)
            start(a_copy(p, w_refs[p].at[3, 0], w_refs[p].at[3, 1], (3, 1), partner))
            if mode in "2YZ":
                spread(p, 0, False, mode == "Y")
            if p == 0:
                small[1].wait()
                weight = inter_ref[...]
                weight = weight * weight
                total = weight[:segs]
                for i in range(1, weight.shape[0] // segs):
                    total = total + weight[i * segs : (i + 1) * segs]
                ebuf_ref[pl.ds(segs, segs), :] = total
            clean(p, 3, (0,))
        elif kind == "AGX":
            a_wait(p, 3, 1)
            if mode == "C":
                spread(p, 0, True, True)
            elif mode == "2":
                spread(p, 1, False, False)
            clean(p, 3, (1,))
        elif kind == "RL":
            relay(p, op[2])
        elif kind == "AG":
            slot, side = op[2], op[3]
            both = mode == "C"
            if mode in "CY" and side == 0:
                pl.when(is_end)(functools.partial(a_wait, p, slot, side, both))
            else:
                a_wait(p, slot, side)
            if mode in "YZ" and side == 0:
                start(a_copy(p, w_refs[p].at[slot, 0], w_refs[p].at[slot, 1], (slot, 1), partner))
            clean(p, slot, (0, 1) if both else (side,))

    def e_copy(d):
        return pltpu.make_async_remote_copy(
            src_ref=ebuf_ref,
            dst_ref=erecv_ref.at[d],
            send_sem=e_send.at[d],
            recv_sem=e_recv.at[d],
            device_id=(me, peers[d]),
            device_id_type=MESH,
        )

    for d in range(n_bin - 1):
        e_copy(d).start()
    outs = [
        pltpu.make_async_copy(cr_ref, cr_hbm, out_sem.at[0]),
        pltpu.make_async_copy(ci_ref, ci_hbm, out_sem.at[1]),
    ]
    for copy in outs:
        copy.start()
    for when, copy in started:
        if when is None:
            copy.wait_send()
    for when in (is_mid, is_end):

        @pl.when(when)
        def _():
            for other, copy in started:
                if other is when:
                    copy.wait_send()

    total = ebuf_ref[...]
    for d in range(n_bin - 1):
        e_copy(d).wait_recv()
        total = total + erecv_ref[d]
    number = jnp.sum(total[:segs], axis=1, keepdims=True)
    norm = jnp.sum(jnp.sum(total[segs:], axis=1, keepdims=True), axis=0, keepdims=True)
    est_ref[...] = jnp.broadcast_to(number / jnp.sqrt(norm), (segs, LANES))
    for d in range(n_bin - 1):
        e_copy(d).wait_send()
    for copy in outs:
        copy.wait()


def line_on_device(n_seg, n_bin, magnet_real, magnet_imag, detector_real, detector_imag, valid, intersection):
    segs, channels, bins = magnet_real.shape
    detectors = detector_real.shape[1]
    blocks = bins // LANES
    nblk = blocks // n_seg
    rows = (channels + 2 * detectors) * channels
    wrows = 2 * channels * detectors
    f32 = jnp.float32
    pieces = split_pieces(nblk)
    modes = ag_modes(len(pieces))
    steps = Planner(pieces, modes, tick_order(pieces), 4, rows, wrows).plan()
    sizes = (n_seg, n_bin, segs, channels, detectors, nblk, pieces, modes, steps)
    count = len(pieces)
    vmem = pl.BlockSpec(memory_space=pltpu.VMEM)
    hbm = pl.BlockSpec(memory_space=pl.ANY)
    scratch = [pltpu.VMEM((LINE, 2, rows * n, LANES), f32) for n, _ in pieces]
    scratch += [pltpu.VMEM((LINE if form == "A" else 1, rows * n, LANES), f32) for n, form in pieces]
    scratch += [pltpu.VMEM((LINE,) + (() if form == "A" else (2,)) + (rows * n, LANES), f32) for n, form in pieces]
    scratch += [pltpu.VMEM((LINE, 2, wrows * n, LANES), f32) for n, _ in pieces]
    scratch += [pltpu.VMEM(a.shape, a.dtype) for a in (magnet_real, magnet_imag, detector_real, detector_imag)]
    scratch += [
        pltpu.SMEM((segs,), jnp.int32),
        pltpu.VMEM((blocks, LANES), f32),
        pltpu.VMEM((segs, bins), f32),
        pltpu.VMEM((segs, bins), f32),
        pltpu.VMEM((blocks, segs * channels, LANES), f32),
        pltpu.VMEM((blocks, segs * channels, LANES), f32),
        pltpu.VMEM((blocks, segs * detectors, LANES), f32),
        pltpu.VMEM((blocks, segs * detectors, LANES), f32),
        pltpu.VMEM((2 * segs, LANES), f32),
        pltpu.VMEM((n_bin - 1, 2 * segs, LANES), f32),
    ]
    dma = pltpu.SemaphoreType.DMA
    scratch += [dma((count, LINE))] * 4 + [dma((count, 12)), dma((count, LINE, 2))]
    scratch += [dma((n_bin - 1,))] * 2 + [dma((2 * LINE, 4)), dma((2,)), dma((2,))]
    cleaned_real, cleaned_imag, estimate = pl.pallas_call(
        functools.partial(line_kernel, sizes),
        out_shape=(
            jax.ShapeDtypeStruct((segs, bins), f32),
            jax.ShapeDtypeStruct((segs, bins), f32),
            jax.ShapeDtypeStruct((segs, LANES), f32),
        ),
        in_specs=[hbm] * 6,
        out_specs=(hbm, hbm, vmem),
        scratch_shapes=scratch,
        compiler_params=pltpu.CompilerParams(
            collective_id=0, has_side_effects=True, vmem_limit_bytes=56 * 1024 * 1024
        ),
    )(
        magnet_real, magnet_imag, detector_real, detector_imag, valid,
        intersection.reshape(blocks, LANES),
    )
    return cleaned_real, cleaned_imag, estimate[:, 0]


def solution(mesh):
    placed = (
        P("seg", None, "bin"),
        P("seg", None, "bin"),
        P("seg", None, "bin"),
        P("seg", None, "bin"),
        P("seg"),
        P("bin"),
    )
    n_seg, n_bin = mesh.shape["seg"], mesh.shape["bin"]
    on_device = line_on_device if n_seg == 2 * LINE else halving_on_device
    return jax.shard_map(
        functools.partial(on_device, n_seg, n_bin),
        mesh=mesh,
        in_specs=placed,
        out_specs=(P("seg", "bin"), P("seg", "bin"), P("seg")),
        check_vma=False,
    )
```

```python
import functools
import heapq

import jax
import jax.numpy as jnp
from jax import lax
from jax.experimental import pallas as pl
from jax.experimental.pallas import tpu as pltpu
from jax.sharding import PartitionSpec as P

LANES = 128
MESH = pl.DeviceIdType.MESH
RS_WEIGHTS = [1.0, 1.0, 1.5]


def largest_divisor(value, limit):
    return max(d for d in range(1, limit + 1) if value % d == 0)


def cadd_mul_conj(acc, a, b):
    return (acc[0] - a[0] * b[0] - a[1] * b[1], acc[1] - a[1] * b[0] + a[0] * b[1])


def csub_mul(acc, a, b):
    return (acc[0] - a[0] * b[0] + a[1] * b[1], acc[1] - a[0] * b[1] - a[1] * b[0])


def csub_conj_mul(acc, a, b):
    return (acc[0] - a[0] * b[0] - a[1] * b[1], acc[1] - a[0] * b[1] + a[1] * b[0])


def wiener_solve(below, diag, right):
    channels = len(diag)
    detectors = len(right[0])
    diag = list(diag)
    inverse = [None] * channels
    low = [[None] * channels for _ in range(channels)]
    for j in range(channels):
        inverse[j] = 1.0 / diag[j]
        for i in range(j + 1, channels):
            low[i][j] = (below[i][j][0] * inverse[j], below[i][j][1] * inverse[j])
        for i in range(j + 1, channels):
            a, l = below[i][j], low[i][j]
            diag[i] = diag[i] - l[0] * a[0] - l[1] * a[1]
            for k in range(j + 1, i):
                below[i][k] = cadd_mul_conj(below[i][k], l, below[k][j])
    out = []
    for det in range(detectors):
        y = []
        for i in range(channels):
            run = right[i][det]
            for k in range(i):
                run = csub_mul(run, low[i][k], y[k])
            y.append(run)
        w = [None] * channels
        for i in reversed(range(channels)):
            run = (y[i][0] * inverse[i], y[i][1] * inverse[i])
            for k in range(i + 1, channels):
                run = csub_conj_mul(run, low[k][i], w[k])
            w[i] = run
        out.append(w)
    return out


def step_weights(stages):
    return RS_WEIGHTS if stages == len(RS_WEIGHTS) else [1.0] * stages


def flood_order(n, stages, parts, weights, gather):
    free = [0.0] * stages
    heap, order, count = [], [], {}

    def send(now, st, q, k):
        free[st] = max(now, free[st]) + weights[st]
        heapq.heappush(heap, (free[st] + 0.6, st, q, k))

    if gather:
        for k in range(parts):
            for st in range(stages):
                send(0.0, st, 0, k)
    else:
        for q in first_order(n, stages):
            for k in range(parts):
                send(0.0, 0, q, k)
    while heap:
        now, st, q, k = heapq.heappop(heap)
        order.append((st, q, k))
        bit = n >> (st + 1)
        if gather:
            for to in range(st):
                send(now, to, q + bit, k)
        else:
            d = q - bit
            count[d, k] = count.get((d, k), 0) + 1
            if d and count[d, k] == stages - d.bit_length():
                send(now, stages - d.bit_length(), d, k)
    return order


def first_order(n, stages):
    def key(q):
        return [q >> bit & 1 for bit in range(stages)]

    return sorted(range(n // 2, n), key=key, reverse=True)


def halving_kernel(
    sizes, mr_ref, mi_ref, hr_ref, hi_ref, valid_ref, inter_ref,
    cr_ref, ci_ref, est_ref,
    s_ref, recv_ref, w_ref, mfr_ref, mfi_ref, hfr_ref, hfi_ref, ebuf_ref, erecv_ref,
    rs_send, rs_recv, ag_send, ag_recv, e_send, e_recv,
):
    n_seg, n_bin, segs, channels, detectors, blocks, chunks, wchunks = sizes
    stages = n_seg.bit_length() - 1
    half = channels // 2
    nblk = blocks // n_seg
    groups = channels + 2 * detectors
    per = groups // chunks
    wrows = 2 * channels * detectors
    wper = wrows // wchunks

    me = lax.axis_index("seg")
    my_bin = lax.axis_index("bin")
    bits = [lax.rem(lax.div(me, 1 << st), 2) for st in range(stages)]
    partner = [me + (1 - 2 * bits[st]) * (1 << st) for st in range(stages)]
    peers = [lax.rem(my_bin + d, n_bin) for d in range(1, n_bin)]

    barrier = pltpu.get_barrier_semaphore()
    for st in range(stages):
        pl.semaphore_signal(barrier, inc=1, device_id=(partner[st], my_bin), device_id_type=MESH)
    for peer in peers:
        pl.semaphore_signal(barrier, inc=1, device_id=(me, peer), device_id_type=MESH)

    def position(q):
        pos = 0
        for st in range(stages):
            digit = lax.rem(lax.div(q, n_seg >> (st + 1)), 2)
            pos = pos + (bits[st] + digit - 2 * bits[st] * digit) * (n_seg >> (st + 1))
        return pos

    sub = lax.broadcasted_iota(jnp.int32, (channels, LANES), 0)

    def spectra(q):
        pos = position(q)

        def body(blk, carry):
            b = pos * nblk + blk
            lanes = pl.ds(pl.multiple_of(b * LANES, LANES), LANES)
            acc = None
            for s in range(segs):
                mr = mr_ref[s, :, lanes].astype(jnp.float32)
                mi = mi_ref[s, :, lanes].astype(jnp.float32)
                hr = hr_ref[s, :, lanes].astype(jnp.float32)
                hi = hi_ref[s, :, lanes].astype(jnp.float32)
                mfr_ref[b, pl.ds(s * channels, channels), :] = mr
                mfi_ref[b, pl.ds(s * channels, channels), :] = mi
                hfr_ref[b, pl.ds(s * detectors, detectors), :] = hr
                hfi_ref[b, pl.ds(s * detectors, detectors), :] = hi
                v = valid_ref[s].astype(jnp.float32)
                kr, ki = mr * v, mi * v
                terms = [kr * mr + ki * mi]
                for r in range(1, half + 1):
                    br = pltpu.roll(mr, channels - r, 0)
                    bi = pltpu.roll(mi, channels - r, 0)
                    terms.append(kr * br + ki * bi)
                    terms.append(ki * br - kr * bi)
                for k in range(detectors):
                    br = jnp.broadcast_to(hr[k : k + 1], (channels, LANES))
                    bi = jnp.broadcast_to(hi[k : k + 1], (channels, LANES))
                    terms.append(kr * br + ki * bi)
                    terms.append(ki * br - kr * bi)
                acc = terms if acc is None else [a + t for a, t in zip(acc, terms)]
            packed = jnp.where(sub < half, acc[channels - 1], acc[channels])
            rows = acc[: channels - 1] + [packed] + acc[channels + 1 :]
            for g in range(groups):
                at = pl.multiple_of((g % per) * nblk * channels + blk * channels, channels)
                s_ref[q, g // per, pl.ds(at, channels), :] = rows[g]
            return carry

        lax.fori_loop(0, nblk, body, 0)

    def rs_copy(st, q, k):
        return pltpu.make_async_remote_copy(
            src_ref=s_ref.at[q, k],
            dst_ref=recv_ref.at[q - 1, k],
            send_sem=rs_send.at[q - 1, k],
            recv_sem=rs_recv.at[q - 1, k],
            device_id=(partner[st], my_bin),
            device_id_type=MESH,
        )

    first = first_order(n_seg, stages)
    assert first[0] == n_seg - 1
    spectra(first[0])
    pl.semaphore_wait(barrier, stages + n_bin - 1)
    for k in range(chunks):
        rs_copy(0, first[0], k).start()

    def mirrored(i, low):
        q = 0 if low else n_seg // 2
        for bit in range(stages - 1):
            digit = 1 - lax.rem(lax.div(i, n_seg >> (bit + 2)), 2)
            q = q + digit * (1 << bit)
        return q

    def early(i, carry):
        q = mirrored(i, False)
        spectra(q)
        for k in range(chunks):
            rs_copy(0, q, k).start()
        return carry

    lax.fori_loop(1, n_seg // 2, early, 0)

    def late(i, carry):
        spectra(mirrored(i, True))
        return carry

    lax.fori_loop(0, n_seg // 2, late, 0)

    got = {}
    for st, q, k in flood_order(n_seg, stages, chunks, step_weights(stages), False):
        rs_copy(st, q, k).wait_recv()
        d = q - (n_seg >> (st + 1))
        s_ref[d, k] = s_ref[d, k] + recv_ref[q - 1, k]
        got[d, k] = got.get((d, k), 0) + 1
        if d and got[d, k] == stages - d.bit_length():
            rs_copy(stages - d.bit_length(), d, k).start()

    def entry(g, row):
        start = (g % per) * nblk * channels + row
        if nblk == 1:
            return s_ref[0, g // per, pl.ds(start, 1), :]
        return s_ref[0, g // per, pl.ds(start, nblk, stride=channels), :]

    def above(a, b):
        r = b - a
        if r < half:
            return (entry(2 * r - 1, a), entry(2 * r, a))
        if r == half:
            return (entry(channels - 1, a), -entry(channels - 1, a + half))
        r = channels - r
        return (entry(2 * r - 1, b), -entry(2 * r, b))

    below = [[None] * channels for _ in range(channels)]
    for i in range(channels):
        for j in range(i):
            value = above(j, i)
            below[i][j] = (value[0], -value[1])
    diag = [entry(0, c) + 1.0 for c in range(channels)]
    right = [
        [(entry(channels + 2 * k, c), entry(channels + 2 * k + 1, c)) for k in range(detectors)]
        for c in range(channels)
    ]
    filt = wiener_solve(below, diag, right)
    for k in range(detectors):
        for c in range(channels):
            for part in range(2):
                e = (k * channels + c) * 2 + part
                w_ref[0, e // wper, pl.ds((e % wper) * nblk, nblk), :] = filt[k][c][part]

    def ag_copy(st, q, k):
        to = q + (n_seg >> (st + 1))
        return pltpu.make_async_remote_copy(
            src_ref=w_ref.at[q, k],
            dst_ref=w_ref.at[to, k],
            send_sem=ag_send.at[to - 1, k],
            recv_sem=ag_recv.at[to - 1, k],
            device_id=(partner[st], my_bin),
            device_id_type=MESH,
        )

    def clean(q, carry):
        pos = position(q)

        def body(blk, carry):
            num, sq = carry
            b = pos * nblk + blk
            lanes = pl.ds(pl.multiple_of(b * LANES, LANES), LANES)
            g = [
                (
                    hfr_ref[b, pl.ds(k, segs, stride=detectors), :],
                    hfi_ref[b, pl.ds(k, segs, stride=detectors), :],
                )
                for k in range(detectors)
            ]
            for c in range(channels):
                m = (
                    mfr_ref[b, pl.ds(c, segs, stride=channels), :],
                    mfi_ref[b, pl.ds(c, segs, stride=channels), :],
                )
                for k in range(detectors):
                    e = (k * channels + c) * 2
                    w = [
                        w_ref[q, f // wper, pl.ds((f % wper) * nblk + blk, 1), :]
                        for f in (e, e + 1)
                    ]
                    g[k] = csub_conj_mul(g[k], w, m)
            real = g[0][0] * g[1][0] + g[0][1] * g[1][1]
            imag = g[0][1] * g[1][0] - g[0][0] * g[1][1]
            cr_ref[:, lanes] = real
            ci_ref[:, lanes] = imag
            weight = inter_ref[pl.ds(b, 1), :]
            return num + real * weight, sq + weight * weight

        return lax.fori_loop(0, nblk, body, carry)

    for k in range(wchunks):
        for st in range(stages):
            ag_copy(st, 0, k).start()
    sums = clean(0, (jnp.zeros((segs, LANES), jnp.float32), jnp.zeros((1, LANES), jnp.float32)))
    seen = {}
    for st, q, k in flood_order(n_seg, stages, wchunks, step_weights(stages), True):
        ag_copy(st, q, k).wait_recv()
        to = q + (n_seg >> (st + 1))
        for on in range(st):
            ag_copy(on, to, k).start()
        seen[to] = seen.get(to, 0) + 1
        if seen[to] == wchunks:
            sums = clean(to, sums)
    num, sq = sums
    ebuf_ref[pl.ds(0, segs), :] = num
    ebuf_ref[pl.ds(segs, segs), :] = jnp.broadcast_to(sq, (segs, LANES))

    def e_copy(d):
        return pltpu.make_async_remote_copy(
            src_ref=ebuf_ref,
            dst_ref=erecv_ref.at[d],
            send_sem=e_send.at[d],
            recv_sem=e_recv.at[d],
            device_id=(me, peers[d]),
            device_id_type=MESH,
        )

    for d in range(n_bin - 1):
        e_copy(d).start()
    for q in range(1, n_seg):
        st = stages - q.bit_length()
        for k in range(chunks):
            rs_copy(st, q, k).wait_send()
        for k in range(wchunks):
            ag_copy(st, q - (n_seg >> (st + 1)), k).wait_send()
    total = ebuf_ref[...]
    for d in range(n_bin - 1):
        e_copy(d).wait_recv()
        total = total + erecv_ref[d]
    total = jnp.sum(total, axis=1, keepdims=True)
    est_ref[...] = jnp.broadcast_to(total[:segs] / jnp.sqrt(total[segs:]), (segs, LANES))
    for d in range(n_bin - 1):
        e_copy(d).wait_send()


def halving_on_device(n_seg, n_bin, magnet_real, magnet_imag, detector_real, detector_imag, valid, intersection):
    segs, channels, bins = magnet_real.shape
    detectors = detector_real.shape[1]
    blocks = bins // LANES
    nblk = blocks // n_seg
    groups = channels + 2 * detectors
    chunks = largest_divisor(groups, 4)
    wrows = 2 * channels * detectors
    wchunks = largest_divisor(wrows, 2)
    rows = groups // chunks * nblk * channels
    f32 = jnp.float32
    sizes = (n_seg, n_bin, segs, channels, detectors, blocks, chunks, wchunks)
    vmem = pl.BlockSpec(memory_space=pltpu.VMEM)
    cleaned_real, cleaned_imag, estimate = pl.pallas_call(
        functools.partial(halving_kernel, sizes),
        out_shape=(
            jax.ShapeDtypeStruct((segs, bins), f32),
            jax.ShapeDtypeStruct((segs, bins), f32),
            jax.ShapeDtypeStruct((segs, LANES), f32),
        ),
        in_specs=[vmem] * 4 + [pl.BlockSpec(memory_space=pltpu.SMEM), vmem],
        out_specs=(vmem, vmem, vmem),
        scratch_shapes=[
            pltpu.VMEM((n_seg, chunks, rows, LANES), f32),
            pltpu.VMEM((n_seg - 1, chunks, rows, LANES), f32),
            pltpu.VMEM((n_seg, wchunks, wrows // wchunks * nblk, LANES), f32),
            pltpu.VMEM((blocks, segs * channels, LANES), f32),
            pltpu.VMEM((blocks, segs * channels, LANES), f32),
            pltpu.VMEM((blocks, segs * detectors, LANES), f32),
            pltpu.VMEM((blocks, segs * detectors, LANES), f32),
            pltpu.VMEM((2 * segs, LANES), f32),
            pltpu.VMEM((n_bin - 1, 2 * segs, LANES), f32),
        ]
        + [
            pltpu.SemaphoreType.DMA((n_seg - 1, chunks)),
            pltpu.SemaphoreType.DMA((n_seg - 1, chunks)),
            pltpu.SemaphoreType.DMA((n_seg - 1, wchunks)),
            pltpu.SemaphoreType.DMA((n_seg - 1, wchunks)),
            pltpu.SemaphoreType.DMA((n_bin - 1,)),
            pltpu.SemaphoreType.DMA((n_bin - 1,)),
        ],
        compiler_params=pltpu.CompilerParams(
            collective_id=0, has_side_effects=True, vmem_limit_bytes=56 * 1024 * 1024
        ),
    )(
        magnet_real, magnet_imag, detector_real, detector_imag, valid,
        intersection.reshape(blocks, LANES),
    )
    return cleaned_real, cleaned_imag, estimate[:, 0]


LINE = 4
GRANT = 24 * 1024 * 1024
ROW_US = 0.01128
HOP_US = (0.0, 2.6, 3.0, 3.4)
GROUP_SETS = ((0, 1), (2, 3))


def split_pieces(nblk):
    sizes = [1] * nblk
    return [(n, "A") for n in sizes[:-1]] + [(sizes[-1], "B")]


def ag_modes(count):
    direct = min(2, count - 1)
    return "".join("C" if p < 2 else "Y" if p < count - 1 - direct else "Z" for p in range(count - 1)) + "2"


def tick_order(pieces):
    first = [p for p, (_, kind) in enumerate(pieces) if kind == "A"]
    order = [(first[0], 0), (first[0], 1)]
    for p, nxt in zip(first, first[1:] + [None]):
        if nxt is not None:
            order += [(nxt, 0), (nxt, 1)]
        order += [(p, 2), (p, 3)]
    return order + [(p, 3) for p, (_, kind) in enumerate(pieces) if kind == "B"]


class Planner:
    def __init__(self, pieces, modes, order, depth, rows, wrows):
        self.pieces, self.modes, self.order, self.depth = pieces, modes, order, depth
        self.rows, self.wrows = rows, wrows
        self.clock = [2.0, 2.0]
        self.link, self.message, self.steps = {}, {}, []

    def send(self, role, key, path, rows):
        start = self.clock[role]
        for name in path:
            start = max(start, self.link.get(name, 0.0))
            self.link[name] = start + rows * ROW_US
        self.message[key] = start + rows * ROW_US + HOP_US[len(path)]

    def waits(self, op):
        kind, p = op[0], op[1]
        if kind == "XR":
            return [[("x", 0, p, op[2])], [("x", 1, p, op[2])]]
        if kind == "ZI":
            return [[], [("z", 1, p, op[2])]]
        if kind == "FIN":
            return [[("z", 0, p, 0), ("z", 0, p, 1)], [("z", 1, p, 2), ("z", 1, p, 3)]]
        if kind == "AGX":
            return [[("ax", 0, p)], [("ax", 1, p)]]
        if kind == "RL":
            return [[], [("a", 1, p, op[2], 0)]]
        if kind == "AG":
            both = [[("a", r, p, op[2], op[3])] for r in range(2)]
            if self.modes[p] in "CY" and op[3] == 0:
                both[1] = []
            return both
        return [[], []]

    def column(self, p, side, rows, chain):
        self.send(0, ("a", 1, p, 2, side), ["in"], rows)
        self.send(1, ("a", 0, p, 2, side), ["out"], rows)
        self.send(1, ("a", 1, p, 1, side), ["mid"], rows)
        if not chain:
            self.send(0, ("a", 1, p, 0, side), ["in", "mid"], rows)
            self.send(1, ("a", 0, p, 1, side), ["mid", "out"], rows)
            self.send(0, ("a", 0, p, 0, side), ["in", "mid", "out"], rows)

    def lines(self, p, r, rows):
        if r < 3:
            self.send(0, ("z", 1, p, r), ["in"], rows)
        if r == 2:
            self.send(1, ("z", 0, p, 0), ["out"], rows)

    def run(self, op):
        for role, keys in enumerate(self.waits(op)):
            self.clock[role] = max([self.clock[role]] + [self.message[key] for key in keys]) + 0.05
        kind, p = op[0], op[1]
        size, form = self.pieces[p]
        rows, wrows, mode = self.rows * size, self.wrows * size, self.modes[p]
        work = 0.0
        if kind == "SP":
            work = 0.13 * size * len(op[3]) * len(op[2])
        elif kind == "XS":
            for role in range(2):
                self.send(role, ("x", role, p, op[2]), [("x", role)], rows)
        elif kind == "XR":
            work = 0.03 * size
        elif kind == "FIN":
            work = 0.06 * size
        elif kind == "SOLVE":
            work = 0.6 + 0.06 * size
        elif kind in ("AGX", "AG"):
            work = 0.06 * size * (2 if kind == "AG" and mode == "C" else 1)
        self.clock = [c + (0.0 if kind in ("SOLVE", "AGX", "AG") else work) for c in self.clock]
        if kind == "XR" and form == "A":
            self.lines(p, op[2], rows)
        elif kind == "ZS":
            self.lines(p, op[2], rows * 2)
        elif kind == "ZI":
            both = rows * (2 if form == "B" else 1)
            if op[2] == 1:
                self.send(1, ("z", 1, p, 3), ["mid"], both)
            else:
                self.send(1, ("z", 0, p, 1), ["mid", "out"], both)
        elif kind == "SOLVE":
            self.clock = [c + 0.6 for c in self.clock]
            for role in range(2):
                self.send(role, ("ax", role, p), [("x", role)], wrows)
            if mode in "2YZ":
                self.column(p, 0, wrows, mode == "Y")
            work = work - 0.6
        elif kind == "AGX":
            if mode in "2C":
                self.column(p, 0 if mode == "C" else 1, wrows * (2 if mode == "C" else 1), mode == "C")
        elif kind == "RL":
            both = wrows * (2 if mode == "C" else 1)
            if op[2] == 2:
                self.send(1, ("a", 1, p, 0, 0), ["mid"], both)
            else:
                self.send(1, ("a", 0, p, op[2], 0), ["out"], both)
        elif kind == "AG" and mode in "YZ" and op[3] == 0:
            for role in range(2):
                self.send(role, ("a", role, p, op[2], 1), [("x", role)], wrows)
        if kind in ("SOLVE", "AGX", "AG"):
            self.clock = [c + work for c in self.clock]
        self.steps.append(op)

    def spectra_steps(self):
        lead = self.order[0]
        for p, (_, form) in enumerate(self.pieces):
            for group in GROUP_SETS:
                if (p, group[0]) == lead:
                    yield ("SP", p, (group[0],), (1,))
                    yield ("SP", p, (group[0],), (0,))
                    yield ("SP", p, group[1:], (1, 0))
                else:
                    yield ("SP", p, group, (1, 0))

    def needs(self):
        need, order = {}, self.order
        made = {}
        for op in self.spectra_steps():
            need[op] = []
            for r in op[2]:
                for side in op[3]:
                    made[op[1], r, side] = op
        for i, (p, r) in enumerate(order):
            back = [("XR",) + order[i - self.depth]] if i >= self.depth else []
            back += [("XS",) + order[i - 1]] if i else []
            chain = [("XR",) + order[i - 1]] if i else []
            if self.pieces[p][1] == "A":
                need["XS", p, r] = [made[p, r, 1]] + back
                need["XR", p, r] = [("XS", p, r), made[p, r, 0]] + chain
            else:
                need["XS", p, r] = [("FIN", p)] + back
                need["XR", p, r] = [("XS", p, r)] + chain
        for p, (_, form) in enumerate(self.pieces):
            kind = "XR" if form == "A" else "ZS"
            if form == "B":
                for r in range(3):
                    need["ZS", p, r] = [made[p, r, 0], made[p, r, 1]]
            for r in range(2):
                need["ZI", p, r] = [(kind, p, r)]
            need["FIN", p] = [("ZI", p, 0), ("ZI", p, 1), (kind, p, 2)]
            need["FIN", p] += [("XR", p, 3)] if form == "A" else [made[p, 3, 0], made[p, 3, 1]]
            need["SOLVE", p] = [("FIN", p) if form == "A" else ("XR", p, 3)]
            need["AGX", p] = [("SOLVE", p)]
            mode = self.modes[p]
            start = ("AGX", p) if mode == "C" else ("SOLVE", p)
            for slot in (2, 1, 0):
                if mode in "CY":
                    need["RL", p, slot] = [start]
                    need["AG", p, slot, 0] = [("RL", p, slot)]
                else:
                    need["AG", p, slot, 0] = [start]
                if mode in "YZ":
                    need["AG", p, slot, 1] = [("AG", p, slot, 0)]
                elif mode == "2":
                    need["AG", p, slot, 1] = [("AGX", p)]
        return need

    def plan(self):
        need = self.needs()
        place = {op: i for i, op in enumerate(need)}
        tick = {key: i for i, key in enumerate(self.order)}
        done = set()
        while len(done) < len(need):
            best = None
            for op in need:
                if op in done or any(other not in done for other in need[op]):
                    continue
                keys = self.waits(op)
                if any(key not in self.message for role in range(2) for key in keys[role]):
                    continue
                ready = max(max([self.clock[r]] + [self.message[key] for key in keys[r]]) for r in range(2))
                now = max(self.clock)
                urgent = -1.0
                if op[0] in ("SP", "ZS") and ready <= now + 1e-6:
                    form = self.pieces[op[1]][1]
                    r = op[2] if op[0] == "ZS" else op[2][0]
                    urgent = 2.5 + 0.1 * r if form == "B" else tick[op[1], r]
                key = (round(max(ready, now), 3), urgent, place[op])
                if best is None or key < best[0]:
                    best = (key, op)
            self.run(best[1])
            done.add(best[1])
        return self.steps


def line_kernel(sizes, mr_hbm, mi_hbm, hr_hbm, hi_hbm, valid_hbm, inter_hbm, cr_ref, ci_ref, est_ref, *scratch):
    n_seg, n_bin, segs, channels, detectors, nblk, pieces, modes, steps = sizes
    count = len(pieces)
    half = channels // 2
    groups = channels + 2 * detectors
    rows = groups * channels
    wrows = 2 * channels * detectors
    scratch = list(scratch)
    take = lambda n: [scratch.pop(0) for _ in range(n)]
    s_refs, x_refs, z_refs, w_refs = take(count), take(count), take(count), take(count)
    mr_ref, mi_ref, hr_ref, hi_ref, valid_ref, inter_ref = take(6)
    mfr_ref, mfi_ref, hfr_ref, hfi_ref, ebuf_ref, erecv_ref = take(6)
    x_send, x_recv, z_send, z_recv, a_send, a_recv, e_send, e_recv, in_sem, small_sem = take(10)

    me = lax.axis_index("seg")
    my_bin = lax.axis_index("bin")
    x = lax.rem(me, 2)
    z = lax.div(me, 2)
    z_hi, z_lo = lax.div(z, 2), lax.rem(z, 2)
    mid = z_hi + z_lo - 2 * z_hi * z_lo
    is_mid, is_end = mid == 1, mid == 0
    sib = 2 * z_hi + 1 - z_lo
    far_mid = 2 - z_hi
    far_end = 3 - 3 * z_hi
    line = {3: z, 2: sib, 1: far_mid, 0: far_end}
    partner = (2 * z + 1 - x, my_bin)
    peers = [lax.rem(my_bin + d, n_bin) for d in range(1, n_bin)]

    def column(where):
        return (2 * line[where] + x, my_bin)

    def lanes_of(r, side):
        return 2 * line[r] + x + side - 2 * side * x

    barrier = pltpu.get_barrier_semaphore()
    for d in range(1, n_seg):
        pl.semaphore_signal(barrier, inc=1, device_id=(lax.rem(me + d, n_seg), my_bin), device_id_type=MESH)
    for peer in peers:
        pl.semaphore_signal(barrier, inc=1, device_id=(me, peer), device_id_type=MESH)

    small = [
        pltpu.make_async_copy(valid_hbm, valid_ref, small_sem.at[0]),
        pltpu.make_async_copy(inter_hbm, inter_ref, small_sem.at[1]),
    ]
    small[0].start()
    loads = {}
    for i, (r, side) in enumerate([(r, side) for r in range(4) for side in (1, 0)]):
        lanes = pl.ds(pl.multiple_of(lanes_of(r, side) * nblk * LANES, nblk * LANES), nblk * LANES)
        loads[r, side] = [
            pltpu.make_async_copy(src.at[:, :, lanes], dst.at[:, :, lanes], in_sem.at[i, j])
            for j, (src, dst) in enumerate(
                [(mr_hbm, mr_ref), (mi_hbm, mi_ref), (hr_hbm, hr_ref), (hi_hbm, hi_ref)]
            )
        ]
        for copy in loads[r, side]:
            copy.start()
    small[1].start()
    small[0].wait()

    first_block = [sum(size for size, _ in pieces[:p]) for p in range(count)]
    sub = lax.broadcasted_iota(jnp.int32, (channels, LANES), 0)
    loaded = set()

    def spectra(p, where, sides):
        size = pieces[p][0]
        for r in where:
            for side in sides:
                if (r, side) not in loaded:
                    loaded.add((r, side))
                    for copy in loads[r, side]:
                        copy.wait()

        def body(i, carry):
            r = where[0] + lax.div(i, size * len(sides))
            side = sides[0] if len(sides) == 1 else 1 - lax.rem(lax.div(i, size), 2)
            blk = lax.rem(i, size)
            if len(where) == 1:
                at = line[where[0]]
            else:
                at = line[where[0]] + (r - where[0]) * (line[where[1]] - line[where[0]])
            owner = 2 * at + x + side - 2 * side * x
            b = owner * nblk + first_block[p] + blk
            lanes = pl.ds(pl.multiple_of(b * LANES, LANES), LANES)
            acc = None
            for s in range(segs):
                mr = mr_ref[s, :, lanes].astype(jnp.float32)
                mi = mi_ref[s, :, lanes].astype(jnp.float32)
                hr = hr_ref[s, :, lanes].astype(jnp.float32)
                hi = hi_ref[s, :, lanes].astype(jnp.float32)
                mfr_ref[b, pl.ds(s * channels, channels), :] = mr
                mfi_ref[b, pl.ds(s * channels, channels), :] = mi
                hfr_ref[b, pl.ds(s * detectors, detectors), :] = hr
                hfi_ref[b, pl.ds(s * detectors, detectors), :] = hi
                v = valid_ref[s].astype(jnp.float32)
                kr, ki = mr * v, mi * v
                terms = [kr * mr + ki * mi]
                for turn in range(1, half + 1):
                    br = pltpu.roll(mr, channels - turn, 0)
                    bi = pltpu.roll(mi, channels - turn, 0)
                    terms.append(kr * br + ki * bi)
                    terms.append(ki * br - kr * bi)
                for k in range(detectors):
                    br = jnp.broadcast_to(hr[k : k + 1], (channels, LANES))
                    bi = jnp.broadcast_to(hi[k : k + 1], (channels, LANES))
                    terms.append(kr * br + ki * bi)
                    terms.append(ki * br - kr * bi)
                acc = terms if acc is None else [a + t for a, t in zip(acc, terms)]
            packed = jnp.where(sub < half, acc[channels - 1], acc[channels])
            out = acc[: channels - 1] + [packed] + acc[channels + 1 :]
            for g in range(groups):
                start = pl.multiple_of((g * size + blk) * channels, channels)
                s_refs[p][r, side, pl.ds(start, channels), :] = out[g]
            return carry

        lax.fori_loop(0, size * len(sides) * len(where), body, 0)

    def solve(p):
        size = pieces[p][0]
        ref = s_refs[p]

        def entry(g, row):
            start = g * size * channels + row
            if size == 1:
                return ref[3, 0, pl.ds(start, 1), :]
            return ref[3, 0, pl.ds(start, size, stride=channels), :]

        def above(a, b):
            r = b - a
            if r < half:
                return (entry(2 * r - 1, a), entry(2 * r, a))
            if r == half:
                return (entry(channels - 1, a), -entry(channels - 1, a + half))
            r = channels - r
            return (entry(2 * r - 1, b), -entry(2 * r, b))

        below = [[None] * channels for _ in range(channels)]
        for i in range(channels):
            for j in range(i):
                value = above(j, i)
                below[i][j] = (value[0], -value[1])
        diag = [entry(0, c) + 1.0 for c in range(channels)]
        right = [
            [(entry(channels + 2 * k, c), entry(channels + 2 * k + 1, c)) for k in range(detectors)]
            for c in range(channels)
        ]
        filt = wiener_solve(below, diag, right)
        for k in range(detectors):
            for c in range(channels):
                for part in range(2):
                    e = (k * channels + c) * 2 + part
                    w_refs[p][3, 0, pl.ds(e * size, size), :] = filt[k][c][part]

    def clean(p, r, sides):
        size = pieces[p][0]

        def body(i, carry):
            if len(sides) == 1:
                side, blk = sides[0], i
            else:
                side, blk = lax.div(i, size), lax.rem(i, size)
            b = lanes_of(r, side) * nblk + first_block[p] + blk
            lanes = pl.ds(pl.multiple_of(b * LANES, LANES), LANES)
            g = [
                (
                    hfr_ref[b, pl.ds(k, segs, stride=detectors), :],
                    hfi_ref[b, pl.ds(k, segs, stride=detectors), :],
                )
                for k in range(detectors)
            ]
            for c in range(channels):
                m = (
                    mfr_ref[b, pl.ds(c, segs, stride=channels), :],
                    mfi_ref[b, pl.ds(c, segs, stride=channels), :],
                )
                for k in range(detectors):
                    e = (k * channels + c) * 2
                    w = [w_refs[p][r, side, pl.ds(f * size + blk, 1), :] for f in (e, e + 1)]
                    g[k] = csub_conj_mul(g[k], w, m)
            real = g[0][0] * g[1][0] + g[0][1] * g[1][1]
            imag = g[0][1] * g[1][0] - g[0][0] * g[1][1]
            cr_ref[:, lanes] = real
            ci_ref[:, lanes] = imag
            ebuf_ref[pl.ds(0, segs), :] = ebuf_ref[pl.ds(0, segs), :] + real * inter_ref[pl.ds(b, 1), :]
            return carry

        if size * len(sides) == 1:
            body(0, 0)
        else:
            lax.fori_loop(0, size * len(sides), body, 0)

    started = []

    def remote(src, dst, send_sem, recv_sem, device):
        return pltpu.make_async_remote_copy(
            src_ref=src, dst_ref=dst, send_sem=send_sem, recv_sem=recv_sem,
            device_id=device, device_id_type=MESH,
        )

    def start(copy, when=None):
        started.append((when, copy))
        if when is None:
            copy.start()
        else:
            pl.when(when)(copy.start)

    def x_copy(p, r):
        src, dst = (s_refs[p].at[r, 1], x_refs[p].at[r]) if pieces[p][1] == "A" else (s_refs[p].at[3, 1], x_refs[p].at[0])
        return remote(src, dst, x_send.at[p, r], x_recv.at[p, r], partner)

    def part(p, r):
        return s_refs[p].at[r, 0] if pieces[p][1] == "A" else s_refs[p].at[r]

    def z_copy(p, r, slot, where):
        return remote(part(p, r), z_refs[p].at[slot], z_send.at[p, r], z_recv.at[p, slot], column(where))

    def send_in(p, r):
        if r < 3:
            start(z_copy(p, r, r, 2), is_end)
        if r == 2:
            start(z_copy(p, r, 0, 2), is_mid)

    def add(p, r, slot):
        ref = part(p, r)
        ref[...] = ref[...] + z_refs[p][slot]

    sends = [0] * count

    def a_copy(p, src, dst, slot_at, device):
        sends[p] += 1
        return remote(src, dst, a_send.at[p, sends[p] - 1], a_recv.at[p, slot_at[0], slot_at[1]], device)

    def a_wait(p, slot, side, both=False):
        ref = w_refs[p].at[slot] if both else w_refs[p].at[slot, side]
        remote(ref, ref, a_send.at[p, 0], a_recv.at[p, slot, side], partner).wait_recv()

    def spread(p, side, both, chain):
        src = w_refs[p].at[3] if both else w_refs[p].at[3, side]

        def to(slot, where, when=None):
            dst = w_refs[p].at[slot] if both else w_refs[p].at[slot, side]
            start(a_copy(p, src, dst, (slot, side), column(where)), when)

        to(2, 2)
        to(mid, 1, is_mid if chain else None)
        if not chain:
            to(mid, 0)

    def relay(p, slot):
        both = modes[p] == "C"
        pick = (lambda n: w_refs[p].at[n]) if both else (lambda n: w_refs[p].at[n, 0])
        to, where = (0, 1) if slot == 2 else (slot, 2)
        copy = a_copy(p, pick(slot), pick(to), (to, 0), column(where))
        started.append((is_mid, copy))

        @pl.when(is_mid)
        def _():
            a_wait(p, slot, 0, both)
            copy.start()

    ebuf_ref[pl.ds(0, segs), :] = jnp.zeros((segs, LANES), jnp.float32)
    entered = False
    for op in steps:
        kind, p = op[0], op[1]
        form, mode = pieces[p][1], modes[p]
        if kind == "SP":
            spectra(p, op[2], op[3])
            continue
        if not entered:
            pl.semaphore_wait(barrier, n_seg + n_bin - 2)
            entered = True
        if kind == "XS":
            start(x_copy(p, op[2]))
        elif kind == "XR":
            r = op[2]
            x_copy(p, r).wait_recv()
            if form == "A":
                s_refs[p][r, 0] = s_refs[p][r, 0] + x_refs[p][r]
                send_in(p, r)
            else:
                s_refs[p][3, 0] = s_refs[p][3, 0] + x_refs[p][0]
        elif kind == "ZS":
            send_in(p, op[2])
        elif kind == "ZI":
            r = op[2]
            copy = z_copy(p, r, 3, 1) if r == 1 else z_copy(p, r, 1, 0)
            started.append((is_mid, copy))

            @pl.when(is_mid)
            def _():
                z_copy(p, r, r, 2).wait_recv()
                add(p, r, r)
                copy.start()
        elif kind == "FIN":
            for when, slots in ((is_end, (0, 1)), (is_mid, (2, 3))):

                @pl.when(when)
                def _():
                    for slot in slots:
                        z_copy(p, 3, slot, 2).wait_recv()
                        add(p, 3, slot)
        elif kind == "SOLVE":
            solve(p)
            start(a_copy(p, w_refs[p].at[3, 0], w_refs[p].at[3, 1], (3, 1), partner))
            if mode in "2YZ":
                spread(p, 0, False, mode == "Y")
            if p == 0:
                small[1].wait()
                weight = inter_ref[...]
                weight = weight * weight
                total = weight[:segs]
                for i in range(1, weight.shape[0] // segs):
                    total = total + weight[i * segs : (i + 1) * segs]
                ebuf_ref[pl.ds(segs, segs), :] = total
            clean(p, 3, (0,))
        elif kind == "AGX":
            a_wait(p, 3, 1)
            if mode == "C":
                spread(p, 0, True, True)
            elif mode == "2":
                spread(p, 1, False, False)
            clean(p, 3, (1,))
        elif kind == "RL":
            relay(p, op[2])
        elif kind == "AG":
            slot, side = op[2], op[3]
            both = mode == "C"
            if mode in "CY" and side == 0:
                pl.when(is_end)(functools.partial(a_wait, p, slot, side, both))
            else:
                a_wait(p, slot, side)
            if mode in "YZ" and side == 0:
                start(a_copy(p, w_refs[p].at[slot, 0], w_refs[p].at[slot, 1], (slot, 1), partner))
            clean(p, slot, (0, 1) if both else (side,))

    def e_copy(d):
        return pltpu.make_async_remote_copy(
            src_ref=ebuf_ref,
            dst_ref=erecv_ref.at[d],
            send_sem=e_send.at[d],
            recv_sem=e_recv.at[d],
            device_id=(me, peers[d]),
            device_id_type=MESH,
        )

    for d in range(n_bin - 1):
        e_copy(d).start()
    for when, copy in started:
        if when is None:
            copy.wait_send()
    for when in (is_mid, is_end):

        @pl.when(when)
        def _():
            for other, copy in started:
                if other is when:
                    copy.wait_send()

    total = ebuf_ref[...]
    for d in range(n_bin - 1):
        e_copy(d).wait_recv()
        total = total + erecv_ref[d]
    number = jnp.sum(total[:segs], axis=1, keepdims=True)
    norm = jnp.sum(jnp.sum(total[segs:], axis=1, keepdims=True), axis=0, keepdims=True)
    own = lax.broadcasted_iota(jnp.int32, (segs, LANES), 0) == lax.broadcasted_iota(jnp.int32, (segs, LANES), 1)
    est_ref[...] = jnp.sum(jnp.where(own, number / jnp.sqrt(norm), 0.0), axis=0, keepdims=True)
    for d in range(n_bin - 1):
        e_copy(d).wait_send()


def store_kernel(cr_ref, ci_ref, est_ref, cr_hbm, ci_hbm, est_out, sems):
    copies = [pltpu.make_async_copy(cr_ref, cr_hbm, sems.at[0]), pltpu.make_async_copy(ci_ref, ci_hbm, sems.at[1])]
    for copy in copies:
        copy.start()
    est_out[...] = est_ref[0, : est_out.shape[0]]
    for copy in copies:
        copy.wait()


def line_on_device(n_seg, n_bin, magnet_real, magnet_imag, detector_real, detector_imag, valid, intersection):
    segs, channels, bins = magnet_real.shape
    detectors = detector_real.shape[1]
    blocks = bins // LANES
    nblk = blocks // n_seg
    rows = (channels + 2 * detectors) * channels
    wrows = 2 * channels * detectors
    f32 = jnp.float32
    pieces = split_pieces(nblk)
    modes = ag_modes(len(pieces))
    steps = Planner(pieces, modes, tick_order(pieces), 4, rows, wrows).plan()
    sizes = (n_seg, n_bin, segs, channels, detectors, nblk, pieces, modes, steps)
    count = len(pieces)
    vmem = pl.BlockSpec(memory_space=pltpu.VMEM)
    hbm = pl.BlockSpec(memory_space=pltpu.HBM)
    scratch = [pltpu.VMEM((LINE, 2, rows * n, LANES), f32) for n, _ in pieces]
    scratch += [pltpu.VMEM((LINE if form == "A" else 1, rows * n, LANES), f32) for n, form in pieces]
    scratch += [pltpu.VMEM((LINE,) + (() if form == "A" else (2,)) + (rows * n, LANES), f32) for n, form in pieces]
    scratch += [pltpu.VMEM((LINE, 2, wrows * n, LANES), f32) for n, _ in pieces]
    scratch += [pltpu.VMEM(a.shape, a.dtype) for a in (magnet_real, magnet_imag, detector_real, detector_imag)]
    scratch += [
        pltpu.SMEM((segs,), jnp.int32),
        pltpu.VMEM((blocks, LANES), f32),
        pltpu.VMEM((blocks, segs * channels, LANES), f32),
        pltpu.VMEM((blocks, segs * channels, LANES), f32),
        pltpu.VMEM((blocks, segs * detectors, LANES), f32),
        pltpu.VMEM((blocks, segs * detectors, LANES), f32),
        pltpu.VMEM((2 * segs, LANES), f32),
        pltpu.VMEM((n_bin - 1, 2 * segs, LANES), f32),
    ]
    dma = pltpu.SemaphoreType.DMA
    scratch += [dma((count, LINE))] * 4 + [dma((count, 12)), dma((count, LINE, 2))]
    scratch += [dma((n_bin - 1,))] * 2 + [dma((2 * LINE, 4)), dma((2,))]
    operands = [magnet_real, magnet_imag, detector_real, detector_imag, valid, intersection.reshape(blocks, LANES)]
    cleaned_real, cleaned_imag, estimate = pl.pallas_call(
        functools.partial(line_kernel, sizes),
        out_shape=(
            pltpu.VMEM((segs, bins), f32),
            pltpu.VMEM((segs, bins), f32),
            pltpu.VMEM((1, LANES), f32),
        ),
        in_specs=[hbm] * 6,
        out_specs=(vmem, vmem, vmem),
        scratch_shapes=scratch,
        compiler_params=pltpu.CompilerParams(
            collective_id=0, has_side_effects=True, vmem_limit_bytes=GRANT
        ),
    )(*[pltpu.with_memory_space_constraint(a, pltpu.HBM) for a in operands])
    return pl.pallas_call(
        store_kernel,
        out_shape=(
            jax.ShapeDtypeStruct((segs, bins), f32),
            jax.ShapeDtypeStruct((segs, bins), f32),
            jax.ShapeDtypeStruct((segs,), f32),
        ),
        in_specs=[vmem] * 3,
        out_specs=(hbm, hbm, vmem),
        scratch_shapes=[dma((2,))],
        compiler_params=pltpu.CompilerParams(vmem_limit_bytes=4 * 1024 * 1024),
    )(cleaned_real, cleaned_imag, estimate)


def solution(mesh):
    placed = (
        P("seg", None, "bin"),
        P("seg", None, "bin"),
        P("seg", None, "bin"),
        P("seg", None, "bin"),
        P("seg"),
        P("bin"),
    )
    n_seg, n_bin = mesh.shape["seg"], mesh.shape["bin"]
    on_device = line_on_device if n_seg == 2 * LINE else halving_on_device
    return jax.shard_map(
        functools.partial(on_device, n_seg, n_bin),
        mesh=mesh,
        in_specs=placed,
        out_specs=(P("seg", "bin"), P("seg", "bin"), P("seg")),
        check_vma=False,
    )
```

```python
import functools
import heapq

import jax
import jax.numpy as jnp
from jax import lax
from jax.experimental import pallas as pl
from jax.experimental.pallas import tpu as pltpu
from jax.sharding import PartitionSpec as P

LANES = 128
MESH = pl.DeviceIdType.MESH
RS_WEIGHTS = [1.0, 1.0, 1.5]


def largest_divisor(value, limit):
    return max(d for d in range(1, limit + 1) if value % d == 0)


def cadd_mul_conj(acc, a, b):
    return (acc[0] - a[0] * b[0] - a[1] * b[1], acc[1] - a[1] * b[0] + a[0] * b[1])


def csub_mul(acc, a, b):
    return (acc[0] - a[0] * b[0] + a[1] * b[1], acc[1] - a[0] * b[1] - a[1] * b[0])


def csub_conj_mul(acc, a, b):
    return (acc[0] - a[0] * b[0] - a[1] * b[1], acc[1] - a[0] * b[1] + a[1] * b[0])


def wiener_solve(below, diag, right):
    channels = len(diag)
    detectors = len(right[0])
    diag = list(diag)
    inverse = [None] * channels
    low = [[None] * channels for _ in range(channels)]
    for j in range(channels):
        inverse[j] = 1.0 / diag[j]
        for i in range(j + 1, channels):
            low[i][j] = (below[i][j][0] * inverse[j], below[i][j][1] * inverse[j])
        for i in range(j + 1, channels):
            a, l = below[i][j], low[i][j]
            diag[i] = diag[i] - l[0] * a[0] - l[1] * a[1]
            for k in range(j + 1, i):
                below[i][k] = cadd_mul_conj(below[i][k], l, below[k][j])
    out = []
    for det in range(detectors):
        y = []
        for i in range(channels):
            run = right[i][det]
            for k in range(i):
                run = csub_mul(run, low[i][k], y[k])
            y.append(run)
        w = [None] * channels
        for i in reversed(range(channels)):
            run = (y[i][0] * inverse[i], y[i][1] * inverse[i])
            for k in range(i + 1, channels):
                run = csub_conj_mul(run, low[k][i], w[k])
            w[i] = run
        out.append(w)
    return out


def step_weights(stages):
    return RS_WEIGHTS if stages == len(RS_WEIGHTS) else [1.0] * stages


def flood_order(n, stages, parts, weights, gather):
    free = [0.0] * stages
    heap, order, count = [], [], {}

    def send(now, st, q, k):
        free[st] = max(now, free[st]) + weights[st]
        heapq.heappush(heap, (free[st] + 0.6, st, q, k))

    if gather:
        for k in range(parts):
            for st in range(stages):
                send(0.0, st, 0, k)
    else:
        for q in first_order(n, stages):
            for k in range(parts):
                send(0.0, 0, q, k)
    while heap:
        now, st, q, k = heapq.heappop(heap)
        order.append((st, q, k))
        bit = n >> (st + 1)
        if gather:
            for to in range(st):
                send(now, to, q + bit, k)
        else:
            d = q - bit
            count[d, k] = count.get((d, k), 0) + 1
            if d and count[d, k] == stages - d.bit_length():
                send(now, stages - d.bit_length(), d, k)
    return order


def first_order(n, stages):
    def key(q):
        return [q >> bit & 1 for bit in range(stages)]

    return sorted(range(n // 2, n), key=key, reverse=True)


def halving_kernel(
    sizes, mr_ref, mi_ref, hr_ref, hi_ref, valid_ref, inter_ref,
    cr_ref, ci_ref, est_ref,
    s_ref, recv_ref, w_ref, mfr_ref, mfi_ref, hfr_ref, hfi_ref, ebuf_ref, erecv_ref,
    rs_send, rs_recv, ag_send, ag_recv, e_send, e_recv,
):
    n_seg, n_bin, segs, channels, detectors, blocks, chunks, wchunks = sizes
    stages = n_seg.bit_length() - 1
    half = channels // 2
    nblk = blocks // n_seg
    groups = channels + 2 * detectors
    per = groups // chunks
    wrows = 2 * channels * detectors
    wper = wrows // wchunks

    me = lax.axis_index("seg")
    my_bin = lax.axis_index("bin")
    bits = [lax.rem(lax.div(me, 1 << st), 2) for st in range(stages)]
    partner = [me + (1 - 2 * bits[st]) * (1 << st) for st in range(stages)]
    peers = [lax.rem(my_bin + d, n_bin) for d in range(1, n_bin)]

    barrier = pltpu.get_barrier_semaphore()
    for st in range(stages):
        pl.semaphore_signal(barrier, inc=1, device_id=(partner[st], my_bin), device_id_type=MESH)
    for peer in peers:
        pl.semaphore_signal(barrier, inc=1, device_id=(me, peer), device_id_type=MESH)

    def position(q):
        pos = 0
        for st in range(stages):
            digit = lax.rem(lax.div(q, n_seg >> (st + 1)), 2)
            pos = pos + (bits[st] + digit - 2 * bits[st] * digit) * (n_seg >> (st + 1))
        return pos

    sub = lax.broadcasted_iota(jnp.int32, (channels, LANES), 0)

    def spectra(q):
        pos = position(q)

        def body(blk, carry):
            b = pos * nblk + blk
            lanes = pl.ds(pl.multiple_of(b * LANES, LANES), LANES)
            acc = None
            for s in range(segs):
                mr = mr_ref[s, :, lanes].astype(jnp.float32)
                mi = mi_ref[s, :, lanes].astype(jnp.float32)
                hr = hr_ref[s, :, lanes].astype(jnp.float32)
                hi = hi_ref[s, :, lanes].astype(jnp.float32)
                mfr_ref[b, pl.ds(s * channels, channels), :] = mr
                mfi_ref[b, pl.ds(s * channels, channels), :] = mi
                hfr_ref[b, pl.ds(s * detectors, detectors), :] = hr
                hfi_ref[b, pl.ds(s * detectors, detectors), :] = hi
                v = valid_ref[s].astype(jnp.float32)
                kr, ki = mr * v, mi * v
                terms = [kr * mr + ki * mi]
                for r in range(1, half + 1):
                    br = pltpu.roll(mr, channels - r, 0)
                    bi = pltpu.roll(mi, channels - r, 0)
                    terms.append(kr * br + ki * bi)
                    terms.append(ki * br - kr * bi)
                for k in range(detectors):
                    br = jnp.broadcast_to(hr[k : k + 1], (channels, LANES))
                    bi = jnp.broadcast_to(hi[k : k + 1], (channels, LANES))
                    terms.append(kr * br + ki * bi)
                    terms.append(ki * br - kr * bi)
                acc = terms if acc is None else [a + t for a, t in zip(acc, terms)]
            packed = jnp.where(sub < half, acc[channels - 1], acc[channels])
            rows = acc[: channels - 1] + [packed] + acc[channels + 1 :]
            for g in range(groups):
                at = pl.multiple_of((g % per) * nblk * channels + blk * channels, channels)
                s_ref[q, g // per, pl.ds(at, channels), :] = rows[g]
            return carry

        lax.fori_loop(0, nblk, body, 0)

    def rs_copy(st, q, k):
        return pltpu.make_async_remote_copy(
            src_ref=s_ref.at[q, k],
            dst_ref=recv_ref.at[q - 1, k],
            send_sem=rs_send.at[q - 1, k],
            recv_sem=rs_recv.at[q - 1, k],
            device_id=(partner[st], my_bin),
            device_id_type=MESH,
        )

    first = first_order(n_seg, stages)
    assert first[0] == n_seg - 1
    spectra(first[0])
    pl.semaphore_wait(barrier, stages + n_bin - 1)
    for k in range(chunks):
        rs_copy(0, first[0], k).start()

    def mirrored(i, low):
        q = 0 if low else n_seg // 2
        for bit in range(stages - 1):
            digit = 1 - lax.rem(lax.div(i, n_seg >> (bit + 2)), 2)
            q = q + digit * (1 << bit)
        return q

    def early(i, carry):
        q = mirrored(i, False)
        spectra(q)
        for k in range(chunks):
            rs_copy(0, q, k).start()
        return carry

    lax.fori_loop(1, n_seg // 2, early, 0)

    def late(i, carry):
        spectra(mirrored(i, True))
        return carry

    lax.fori_loop(0, n_seg // 2, late, 0)

    got = {}
    for st, q, k in flood_order(n_seg, stages, chunks, step_weights(stages), False):
        rs_copy(st, q, k).wait_recv()
        d = q - (n_seg >> (st + 1))
        s_ref[d, k] = s_ref[d, k] + recv_ref[q - 1, k]
        got[d, k] = got.get((d, k), 0) + 1
        if d and got[d, k] == stages - d.bit_length():
            rs_copy(stages - d.bit_length(), d, k).start()

    def entry(g, row):
        start = (g % per) * nblk * channels + row
        if nblk == 1:
            return s_ref[0, g // per, pl.ds(start, 1), :]
        return s_ref[0, g // per, pl.ds(start, nblk, stride=channels), :]

    def above(a, b):
        r = b - a
        if r < half:
            return (entry(2 * r - 1, a), entry(2 * r, a))
        if r == half:
            return (entry(channels - 1, a), -entry(channels - 1, a + half))
        r = channels - r
        return (entry(2 * r - 1, b), -entry(2 * r, b))

    below = [[None] * channels for _ in range(channels)]
    for i in range(channels):
        for j in range(i):
            value = above(j, i)
            below[i][j] = (value[0], -value[1])
    diag = [entry(0, c) + 1.0 for c in range(channels)]
    right = [
        [(entry(channels + 2 * k, c), entry(channels + 2 * k + 1, c)) for k in range(detectors)]
        for c in range(channels)
    ]
    filt = wiener_solve(below, diag, right)
    for k in range(detectors):
        for c in range(channels):
            for part in range(2):
                e = (k * channels + c) * 2 + part
                w_ref[0, e // wper, pl.ds((e % wper) * nblk, nblk), :] = filt[k][c][part]

    def ag_copy(st, q, k):
        to = q + (n_seg >> (st + 1))
        return pltpu.make_async_remote_copy(
            src_ref=w_ref.at[q, k],
            dst_ref=w_ref.at[to, k],
            send_sem=ag_send.at[to - 1, k],
            recv_sem=ag_recv.at[to - 1, k],
            device_id=(partner[st], my_bin),
            device_id_type=MESH,
        )

    def clean(q, carry):
        pos = position(q)

        def body(blk, carry):
            num, sq = carry
            b = pos * nblk + blk
            lanes = pl.ds(pl.multiple_of(b * LANES, LANES), LANES)
            g = [
                (
                    hfr_ref[b, pl.ds(k, segs, stride=detectors), :],
                    hfi_ref[b, pl.ds(k, segs, stride=detectors), :],
                )
                for k in range(detectors)
            ]
            for c in range(channels):
                m = (
                    mfr_ref[b, pl.ds(c, segs, stride=channels), :],
                    mfi_ref[b, pl.ds(c, segs, stride=channels), :],
                )
                for k in range(detectors):
                    e = (k * channels + c) * 2
                    w = [
                        w_ref[q, f // wper, pl.ds((f % wper) * nblk + blk, 1), :]
                        for f in (e, e + 1)
                    ]
                    g[k] = csub_conj_mul(g[k], w, m)
            real = g[0][0] * g[1][0] + g[0][1] * g[1][1]
            imag = g[0][1] * g[1][0] - g[0][0] * g[1][1]
            cr_ref[:, lanes] = real
            ci_ref[:, lanes] = imag
            weight = inter_ref[pl.ds(b, 1), :]
            return num + real * weight, sq + weight * weight

        return lax.fori_loop(0, nblk, body, carry)

    for k in range(wchunks):
        for st in range(stages):
            ag_copy(st, 0, k).start()
    sums = clean(0, (jnp.zeros((segs, LANES), jnp.float32), jnp.zeros((1, LANES), jnp.float32)))
    seen = {}
    for st, q, k in flood_order(n_seg, stages, wchunks, step_weights(stages), True):
        ag_copy(st, q, k).wait_recv()
        to = q + (n_seg >> (st + 1))
        for on in range(st):
            ag_copy(on, to, k).start()
        seen[to] = seen.get(to, 0) + 1
        if seen[to] == wchunks:
            sums = clean(to, sums)
    num, sq = sums
    ebuf_ref[pl.ds(0, segs), :] = num
    ebuf_ref[pl.ds(segs, segs), :] = jnp.broadcast_to(sq, (segs, LANES))

    def e_copy(d):
        return pltpu.make_async_remote_copy(
            src_ref=ebuf_ref,
            dst_ref=erecv_ref.at[d],
            send_sem=e_send.at[d],
            recv_sem=e_recv.at[d],
            device_id=(me, peers[d]),
            device_id_type=MESH,
        )

    for d in range(n_bin - 1):
        e_copy(d).start()
    for q in range(1, n_seg):
        st = stages - q.bit_length()
        for k in range(chunks):
            rs_copy(st, q, k).wait_send()
        for k in range(wchunks):
            ag_copy(st, q - (n_seg >> (st + 1)), k).wait_send()
    total = ebuf_ref[...]
    for d in range(n_bin - 1):
        e_copy(d).wait_recv()
        total = total + erecv_ref[d]
    total = jnp.sum(total, axis=1, keepdims=True)
    est_ref[...] = jnp.broadcast_to(total[:segs] / jnp.sqrt(total[segs:]), (segs, LANES))
    for d in range(n_bin - 1):
        e_copy(d).wait_send()


def halving_on_device(n_seg, n_bin, magnet_real, magnet_imag, detector_real, detector_imag, valid, intersection):
    segs, channels, bins = magnet_real.shape
    detectors = detector_real.shape[1]
    blocks = bins // LANES
    nblk = blocks // n_seg
    groups = channels + 2 * detectors
    chunks = largest_divisor(groups, 4)
    wrows = 2 * channels * detectors
    wchunks = largest_divisor(wrows, 2)
    rows = groups // chunks * nblk * channels
    f32 = jnp.float32
    sizes = (n_seg, n_bin, segs, channels, detectors, blocks, chunks, wchunks)
    vmem = pl.BlockSpec(memory_space=pltpu.VMEM)
    cleaned_real, cleaned_imag, estimate = pl.pallas_call(
        functools.partial(halving_kernel, sizes),
        out_shape=(
            jax.ShapeDtypeStruct((segs, bins), f32),
            jax.ShapeDtypeStruct((segs, bins), f32),
            jax.ShapeDtypeStruct((segs, LANES), f32),
        ),
        in_specs=[vmem] * 4 + [pl.BlockSpec(memory_space=pltpu.SMEM), vmem],
        out_specs=(vmem, vmem, vmem),
        scratch_shapes=[
            pltpu.VMEM((n_seg, chunks, rows, LANES), f32),
            pltpu.VMEM((n_seg - 1, chunks, rows, LANES), f32),
            pltpu.VMEM((n_seg, wchunks, wrows // wchunks * nblk, LANES), f32),
            pltpu.VMEM((blocks, segs * channels, LANES), f32),
            pltpu.VMEM((blocks, segs * channels, LANES), f32),
            pltpu.VMEM((blocks, segs * detectors, LANES), f32),
            pltpu.VMEM((blocks, segs * detectors, LANES), f32),
            pltpu.VMEM((2 * segs, LANES), f32),
            pltpu.VMEM((n_bin - 1, 2 * segs, LANES), f32),
        ]
        + [
            pltpu.SemaphoreType.DMA((n_seg - 1, chunks)),
            pltpu.SemaphoreType.DMA((n_seg - 1, chunks)),
            pltpu.SemaphoreType.DMA((n_seg - 1, wchunks)),
            pltpu.SemaphoreType.DMA((n_seg - 1, wchunks)),
            pltpu.SemaphoreType.DMA((n_bin - 1,)),
            pltpu.SemaphoreType.DMA((n_bin - 1,)),
        ],
        compiler_params=pltpu.CompilerParams(
            collective_id=0, has_side_effects=True, vmem_limit_bytes=56 * 1024 * 1024
        ),
    )(
        magnet_real, magnet_imag, detector_real, detector_imag, valid,
        intersection.reshape(blocks, LANES),
    )
    return cleaned_real, cleaned_imag, estimate[:, 0]


LINE = 4
DEPTH = 3
GRANT = 24 * 1024 * 1024
ROW_US = 0.01128
HOP_US = (0.0, 2.6, 3.0, 3.4, 3.8)
GROUP_SETS = ((0, 1), (2, 3))


TUNED = {
    8: (
        (2, 3, 2, 1),
        "2YZY",
        ((1, 0), (0, 1), (1, 1), (0, 0), (2, 0), (1, 2), (2, 1), (1, 3), (3, 3), (2, 2), (0, 2), (2, 3), (0, 3)),
    ),
}


def schedule(nblk):
    if nblk in TUNED:
        sizes, modes, order = TUNED[nblk]
        pieces = [(n, "A") for n in sizes[:-1]] + [(sizes[-1], "B")]
        return pieces, modes, list(order)
    pieces = [(n, "A") for n in [1] * (nblk - 1)] + [(1, "B")] if nblk > 1 else [(nblk, "A")]
    return pieces, "Y" * len(pieces), tick_order(pieces)


def tick_order(pieces):
    first = [p for p, (_, kind) in enumerate(pieces) if kind == "A"]
    order = [(first[0], 0), (first[0], 1)]
    for p, nxt in zip(first, first[1:] + [None]):
        if nxt is not None:
            order += [(nxt, 0), (nxt, 1)]
        order += [(p, 2), (p, 3)]
    return order + [(p, 3) for p, (_, kind) in enumerate(pieces) if kind == "B"]


class Planner:
    def __init__(self, pieces, modes, order, depth, rows, wrows):
        self.pieces, self.modes, self.order, self.depth = pieces, modes, order, depth
        self.rows, self.wrows = rows, wrows
        self.clock = [2.0, 2.0]
        self.link, self.message, self.steps = {}, {}, []

    def send(self, role, key, path, rows):
        start = self.clock[role]
        for name in path:
            start = max(start, self.link.get(name, 0.0))
            self.link[name] = start + rows * ROW_US
        self.message[key] = start + rows * ROW_US + HOP_US[len(path)]

    def waits(self, op):
        kind, p = op[0], op[1]
        if kind == "XR":
            return [[("x", 0, p, op[2])], [("x", 1, p, op[2])]]
        if kind == "ZI":
            return [[], [("z", 1, p, op[2])]]
        if kind == "FIN":
            return [[("z", 0, p, 0), ("z", 0, p, 1)], [("z", 1, p, 2), ("z", 1, p, 3)]]
        if kind == "AGX":
            return [[("ax", 0, p)], [("ax", 1, p)]]
        if kind == "RL":
            return [[], [("a", 1, p, op[2], 0)]]
        if kind == "AG":
            both = [[("a", r, p, op[2], op[3])] for r in range(2)]
            if self.modes[p] in "CY" and op[3] == 0:
                both[1] = []
            return both
        return [[], []]

    def column(self, p, side, rows, chain):
        self.send(0, ("a", 1, p, 2, side), ["in"], rows)
        self.send(1, ("a", 0, p, 2, side), ["out"], rows)
        self.send(1, ("a", 1, p, 1, side), ["mid"], rows)
        if not chain:
            self.send(0, ("a", 1, p, 0, side), ["in", "mid"], rows)
            self.send(1, ("a", 0, p, 1, side), ["mid", "out"], rows)
            self.send(0, ("a", 0, p, 0, side), ["in", "mid", "out"], rows)

    def diagonal(self, p, rows):
        self.send(0, ("a", 1, p, 2, 1), [("x", 0), "in"], rows)
        self.send(1, ("a", 0, p, 2, 1), [("x", 1), "out"], rows)
        self.send(1, ("a", 1, p, 1, 1), [("x", 1), "mid"], rows)
        self.send(0, ("a", 1, p, 0, 1), [("x", 0), "in", "mid"], rows)
        self.send(1, ("a", 0, p, 1, 1), [("x", 1), "mid", "out"], rows)
        self.send(0, ("a", 0, p, 0, 1), [("x", 0), "in", "mid", "out"], rows)

    def lines(self, p, r, rows):
        if r < 3:
            self.send(0, ("z", 1, p, r), ["in"], rows)
        if r == 2:
            self.send(1, ("z", 0, p, 0), ["out"], rows)

    def run(self, op):
        for role, keys in enumerate(self.waits(op)):
            self.clock[role] = max([self.clock[role]] + [self.message[key] for key in keys]) + 0.05
        kind, p = op[0], op[1]
        size, form = self.pieces[p]
        rows, wrows, mode = self.rows * size, self.wrows * size, self.modes[p]
        work = 0.0
        if kind == "SP":
            work = 0.13 * size * len(op[3]) * len(op[2])
        elif kind == "XS":
            for role in range(2):
                self.send(role, ("x", role, p, op[2]), [("x", role)], rows)
        elif kind == "XR":
            work = 0.03 * size
        elif kind == "FIN":
            work = 0.06 * size
        elif kind == "SOLVE":
            work = 0.6 + 0.06 * size
        elif kind in ("AGX", "AG"):
            work = 0.06 * size * (2 if kind == "AG" and mode == "C" else 1)
        self.clock = [c + (0.0 if kind in ("SOLVE", "AGX", "AG") else work) for c in self.clock]
        if kind == "XR" and form == "A":
            self.lines(p, op[2], rows)
        elif kind == "ZS":
            self.lines(p, op[2], rows * 2)
        elif kind == "ZI":
            both = rows * (2 if form == "B" else 1)
            if op[2] == 1:
                self.send(1, ("z", 1, p, 3), ["mid"], both)
            else:
                self.send(1, ("z", 0, p, 1), ["mid", "out"], both)
        elif kind == "SOLVE":
            self.clock = [c + 0.6 for c in self.clock]
            for role in range(2):
                self.send(role, ("ax", role, p), [("x", role)], wrows)
            if mode in "2DYZ":
                self.column(p, 0, wrows, mode == "Y")
            if mode == "D":
                self.diagonal(p, wrows)
            work = work - 0.6
        elif kind == "AGX":
            if mode in "2C":
                self.column(p, 0 if mode == "C" else 1, wrows * (2 if mode == "C" else 1), mode == "C")
        elif kind == "RL":
            both = wrows * (2 if mode == "C" else 1)
            if op[2] == 2:
                self.send(1, ("a", 1, p, 0, 0), ["mid"], both)
            else:
                self.send(1, ("a", 0, p, op[2], 0), ["out"], both)
        elif kind == "AG" and mode in "YZ" and op[3] == 0:
            for role in range(2):
                self.send(role, ("a", role, p, op[2], 1), [("x", role)], wrows)
        if kind in ("SOLVE", "AGX", "AG"):
            self.clock = [c + work for c in self.clock]
        self.steps.append(op)

    def spectra_steps(self):
        lead = self.order[0]
        for p, (_, form) in enumerate(self.pieces):
            for group in GROUP_SETS:
                if (p, group[0]) == lead:
                    yield ("SP", p, (group[0],), (1,))
                    yield ("SP", p, (group[0],), (0,))
                    yield ("SP", p, group[1:], (1, 0))
                else:
                    yield ("SP", p, group, (1, 0))

    def needs(self):
        need, order = {}, self.order
        made = {}
        for op in self.spectra_steps():
            need[op] = []
            for r in op[2]:
                for side in op[3]:
                    made[op[1], r, side] = op
        for i, (p, r) in enumerate(order):
            back = [("XR",) + order[i - self.depth]] if i >= self.depth else []
            back += [("XS",) + order[i - 1]] if i else []
            chain = [("XR",) + order[i - 1]] if i else []
            if self.pieces[p][1] == "A":
                need["XS", p, r] = [made[p, r, 1]] + back
                need["XR", p, r] = [("XS", p, r), made[p, r, 0]] + chain
            else:
                need["XS", p, r] = [("FIN", p)] + back
                need["XR", p, r] = [("XS", p, r)] + chain
        for p, (_, form) in enumerate(self.pieces):
            kind = "XR" if form == "A" else "ZS"
            if form == "B":
                for r in range(3):
                    need["ZS", p, r] = [made[p, r, 0], made[p, r, 1]]
            for r in range(2):
                need["ZI", p, r] = [(kind, p, r)]
            need["FIN", p] = [("ZI", p, 0), ("ZI", p, 1), (kind, p, 2)]
            need["FIN", p] += [("XR", p, 3)] if form == "A" else [made[p, 3, 0], made[p, 3, 1]]
            need["SOLVE", p] = [("FIN", p) if form == "A" else ("XR", p, 3)]
            need["AGX", p] = [("SOLVE", p)]
            mode = self.modes[p]
            start = ("AGX", p) if mode == "C" else ("SOLVE", p)
            for slot in (2, 1, 0):
                if mode in "CY":
                    need["RL", p, slot] = [start]
                    need["AG", p, slot, 0] = [("RL", p, slot)]
                else:
                    need["AG", p, slot, 0] = [start]
                if mode in "YZ":
                    need["AG", p, slot, 1] = [("AG", p, slot, 0)]
                elif mode in "2D":
                    need["AG", p, slot, 1] = [("AGX", p) if mode == "2" else start]
        return need

    def plan(self):
        need = self.needs()
        place = {op: i for i, op in enumerate(need)}
        tick = {key: i for i, key in enumerate(self.order)}
        done = set()
        while len(done) < len(need):
            best = None
            for op in need:
                if op in done or any(other not in done for other in need[op]):
                    continue
                keys = self.waits(op)
                if any(key not in self.message for role in range(2) for key in keys[role]):
                    continue
                ready = max(max([self.clock[r]] + [self.message[key] for key in keys[r]]) for r in range(2))
                now = max(self.clock)
                urgent = -1.0
                if op[0] in ("SP", "ZS") and ready <= now + 1e-6:
                    form = self.pieces[op[1]][1]
                    r = op[2] if op[0] == "ZS" else op[2][0]
                    urgent = 2.5 + 0.1 * r if form == "B" else tick[op[1], r]
                key = (round(max(ready, now), 3), urgent, place[op])
                if best is None or key < best[0]:
                    best = (key, op)
            self.run(best[1])
            done.add(best[1])
        return self.steps


def line_kernel(sizes, mr_hbm, mi_hbm, hr_hbm, hi_hbm, valid_hbm, inter_hbm, cr_ref, ci_ref, est_ref, *scratch):
    n_seg, n_bin, segs, channels, detectors, nblk, pieces, modes, steps = sizes
    count = len(pieces)
    half = channels // 2
    groups = channels + 2 * detectors
    rows = groups * channels
    wrows = 2 * channels * detectors
    scratch = list(scratch)
    take = lambda n: [scratch.pop(0) for _ in range(n)]
    s_refs, x_refs, z_refs, w_refs = take(count), take(count), take(count), take(count)
    mr_ref, mi_ref, hr_ref, hi_ref, valid_ref, inter_ref = take(6)
    mfr_ref, mfi_ref, hfr_ref, hfi_ref, ebuf_ref, erecv_ref = take(6)
    x_send, x_recv, z_send, z_recv, a_send, a_recv, e_send, e_recv, in_sem, small_sem = take(10)

    me = lax.axis_index("seg")
    my_bin = lax.axis_index("bin")
    x = lax.rem(me, 2)
    z = lax.div(me, 2)
    z_hi, z_lo = lax.div(z, 2), lax.rem(z, 2)
    mid = z_hi + z_lo - 2 * z_hi * z_lo
    is_mid, is_end = mid == 1, mid == 0
    sib = 2 * z_hi + 1 - z_lo
    far_mid = 2 - z_hi
    far_end = 3 - 3 * z_hi
    line = {3: z, 2: sib, 1: far_mid, 0: far_end}
    partner = (2 * z + 1 - x, my_bin)
    peers = [lax.rem(my_bin + d, n_bin) for d in range(1, n_bin)]

    def column(where):
        return (2 * line[where] + x, my_bin)

    def lanes_of(r, side):
        return 2 * line[r] + x + side - 2 * side * x

    barrier = pltpu.get_barrier_semaphore()
    for d in range(1, n_seg):
        pl.semaphore_signal(barrier, inc=1, device_id=(lax.rem(me + d, n_seg), my_bin), device_id_type=MESH)
    for peer in peers:
        pl.semaphore_signal(barrier, inc=1, device_id=(me, peer), device_id_type=MESH)

    small = [
        pltpu.make_async_copy(valid_hbm, valid_ref, small_sem.at[0]),
        pltpu.make_async_copy(inter_hbm, inter_ref, small_sem.at[1]),
    ]
    small[0].start()
    loads = {}
    for i, (r, side) in enumerate([(r, side) for r in range(4) for side in (1, 0)]):
        lanes = pl.ds(pl.multiple_of(lanes_of(r, side) * nblk * LANES, nblk * LANES), nblk * LANES)
        loads[r, side] = [
            pltpu.make_async_copy(src.at[:, :, lanes], dst.at[:, :, lanes], in_sem.at[i, j])
            for j, (src, dst) in enumerate(
                [(mr_hbm, mr_ref), (mi_hbm, mi_ref), (hr_hbm, hr_ref), (hi_hbm, hi_ref)]
            )
        ]
        for copy in loads[r, side]:
            copy.start()
    small[1].start()
    small[0].wait()

    first_block = [sum(size for size, _ in pieces[:p]) for p in range(count)]
    sub = lax.broadcasted_iota(jnp.int32, (channels, LANES), 0)
    loaded = set()

    def spectra(p, where, sides):
        size = pieces[p][0]
        for r in where:
            for side in sides:
                if (r, side) not in loaded:
                    loaded.add((r, side))
                    for copy in loads[r, side]:
                        copy.wait()

        def body(i, carry):
            r = where[0] + lax.div(i, size * len(sides))
            side = sides[0] if len(sides) == 1 else 1 - lax.rem(lax.div(i, size), 2)
            blk = lax.rem(i, size)
            if len(where) == 1:
                at = line[where[0]]
            else:
                at = line[where[0]] + (r - where[0]) * (line[where[1]] - line[where[0]])
            owner = 2 * at + x + side - 2 * side * x
            b = owner * nblk + first_block[p] + blk
            lanes = pl.ds(pl.multiple_of(b * LANES, LANES), LANES)
            acc = None
            for s in range(segs):
                mr = mr_ref[s, :, lanes].astype(jnp.float32)
                mi = mi_ref[s, :, lanes].astype(jnp.float32)
                hr = hr_ref[s, :, lanes].astype(jnp.float32)
                hi = hi_ref[s, :, lanes].astype(jnp.float32)
                mfr_ref[b, pl.ds(s * channels, channels), :] = mr
                mfi_ref[b, pl.ds(s * channels, channels), :] = mi
                hfr_ref[b, pl.ds(s * detectors, detectors), :] = hr
                hfi_ref[b, pl.ds(s * detectors, detectors), :] = hi
                v = valid_ref[s].astype(jnp.float32)
                kr, ki = mr * v, mi * v
                terms = [kr * mr + ki * mi]
                for turn in range(1, half + 1):
                    br = pltpu.roll(mr, channels - turn, 0)
                    bi = pltpu.roll(mi, channels - turn, 0)
                    terms.append(kr * br + ki * bi)
                    terms.append(ki * br - kr * bi)
                for k in range(detectors):
                    br = jnp.broadcast_to(hr[k : k + 1], (channels, LANES))
                    bi = jnp.broadcast_to(hi[k : k + 1], (channels, LANES))
                    terms.append(kr * br + ki * bi)
                    terms.append(ki * br - kr * bi)
                acc = terms if acc is None else [a + t for a, t in zip(acc, terms)]
            packed = jnp.where(sub < half, acc[channels - 1], acc[channels])
            out = acc[: channels - 1] + [packed] + acc[channels + 1 :]
            for g in range(groups):
                start = pl.multiple_of((g * size + blk) * channels, channels)
                s_refs[p][r, side, pl.ds(start, channels), :] = out[g]
            return carry

        lax.fori_loop(0, size * len(sides) * len(where), body, 0)

    def solve(p):
        size = pieces[p][0]
        ref = s_refs[p]

        def entry(g, row):
            start = g * size * channels + row
            if size == 1:
                return ref[3, 0, pl.ds(start, 1), :]
            return ref[3, 0, pl.ds(start, size, stride=channels), :]

        def above(a, b):
            r = b - a
            if r < half:
                return (entry(2 * r - 1, a), entry(2 * r, a))
            if r == half:
                return (entry(channels - 1, a), -entry(channels - 1, a + half))
            r = channels - r
            return (entry(2 * r - 1, b), -entry(2 * r, b))

        below = [[None] * channels for _ in range(channels)]
        for i in range(channels):
            for j in range(i):
                value = above(j, i)
                below[i][j] = (value[0], -value[1])
        diag = [entry(0, c) + 1.0 for c in range(channels)]
        right = [
            [(entry(channels + 2 * k, c), entry(channels + 2 * k + 1, c)) for k in range(detectors)]
            for c in range(channels)
        ]
        filt = wiener_solve(below, diag, right)
        for k in range(detectors):
            for c in range(channels):
                for part in range(2):
                    e = (k * channels + c) * 2 + part
                    w_refs[p][3, 0, pl.ds(e * size, size), :] = filt[k][c][part]

    def clean(p, r, sides):
        size = pieces[p][0]

        def body(i, carry):
            if len(sides) == 1:
                side, blk = sides[0], i
            else:
                side, blk = lax.div(i, size), lax.rem(i, size)
            b = lanes_of(r, side) * nblk + first_block[p] + blk
            lanes = pl.ds(pl.multiple_of(b * LANES, LANES), LANES)
            g = [
                (
                    hfr_ref[b, pl.ds(k, segs, stride=detectors), :],
                    hfi_ref[b, pl.ds(k, segs, stride=detectors), :],
                )
                for k in range(detectors)
            ]
            for c in range(channels):
                m = (
                    mfr_ref[b, pl.ds(c, segs, stride=channels), :],
                    mfi_ref[b, pl.ds(c, segs, stride=channels), :],
                )
                for k in range(detectors):
                    e = (k * channels + c) * 2
                    w = [w_refs[p][r, side, pl.ds(f * size + blk, 1), :] for f in (e, e + 1)]
                    g[k] = csub_conj_mul(g[k], w, m)
            real = g[0][0] * g[1][0] + g[0][1] * g[1][1]
            imag = g[0][1] * g[1][0] - g[0][0] * g[1][1]
            cr_ref[:, lanes] = real
            ci_ref[:, lanes] = imag
            ebuf_ref[pl.ds(0, segs), :] = ebuf_ref[pl.ds(0, segs), :] + real * inter_ref[pl.ds(b, 1), :]
            return carry

        if size * len(sides) == 1:
            body(0, 0)
        else:
            lax.fori_loop(0, size * len(sides), body, 0)

    started = []

    def remote(src, dst, send_sem, recv_sem, device):
        return pltpu.make_async_remote_copy(
            src_ref=src, dst_ref=dst, send_sem=send_sem, recv_sem=recv_sem,
            device_id=device, device_id_type=MESH,
        )

    def start(copy, when=None):
        started.append((when, copy))
        if when is None:
            copy.start()
        else:
            pl.when(when)(copy.start)

    def x_copy(p, r):
        src, dst = (s_refs[p].at[r, 1], x_refs[p].at[r]) if pieces[p][1] == "A" else (s_refs[p].at[3, 1], x_refs[p].at[0])
        return remote(src, dst, x_send.at[p, r], x_recv.at[p, r], partner)

    def part(p, r):
        return s_refs[p].at[r, 0] if pieces[p][1] == "A" else s_refs[p].at[r]

    def z_copy(p, r, slot, where):
        return remote(part(p, r), z_refs[p].at[slot], z_send.at[p, r], z_recv.at[p, slot], column(where))

    def send_in(p, r):
        if r < 3:
            start(z_copy(p, r, r, 2), is_end)
        if r == 2:
            start(z_copy(p, r, 0, 2), is_mid)

    def add(p, r, slot):
        ref = part(p, r)
        ref[...] = ref[...] + z_refs[p][slot]

    sends = [0] * count

    def a_copy(p, src, dst, slot_at, device):
        sends[p] += 1
        return remote(src, dst, a_send.at[p, sends[p] - 1], a_recv.at[p, slot_at[0], slot_at[1]], device)

    def a_wait(p, slot, side, both=False):
        ref = w_refs[p].at[slot] if both else w_refs[p].at[slot, side]
        remote(ref, ref, a_send.at[p, 0], a_recv.at[p, slot, side], partner).wait_recv()

    def spread(p, side, both, chain):
        src = w_refs[p].at[3] if both else w_refs[p].at[3, side]

        def to(slot, where, when=None):
            dst = w_refs[p].at[slot] if both else w_refs[p].at[slot, side]
            start(a_copy(p, src, dst, (slot, side), column(where)), when)

        to(2, 2)
        to(mid, 1, is_mid if chain else None)
        if not chain:
            to(mid, 0)

    def relay(p, slot):
        both = modes[p] == "C"
        pick = (lambda n: w_refs[p].at[n]) if both else (lambda n: w_refs[p].at[n, 0])
        to, where = (0, 1) if slot == 2 else (slot, 2)
        copy = a_copy(p, pick(slot), pick(to), (to, 0), column(where))
        started.append((is_mid, copy))

        @pl.when(is_mid)
        def _():
            a_wait(p, slot, 0, both)
            copy.start()

    ebuf_ref[pl.ds(0, segs), :] = jnp.zeros((segs, LANES), jnp.float32)
    entered = weighed = False
    for op in steps:
        kind, p = op[0], op[1]
        form, mode = pieces[p][1], modes[p]
        if kind == "SP":
            spectra(p, op[2], op[3])
            continue
        if not entered:
            pl.semaphore_wait(barrier, n_seg + n_bin - 2)
            entered = True
        if kind == "XS":
            start(x_copy(p, op[2]))
        elif kind == "XR":
            r = op[2]
            x_copy(p, r).wait_recv()
            if form == "A":
                s_refs[p][r, 0] = s_refs[p][r, 0] + x_refs[p][r]
                send_in(p, r)
            else:
                s_refs[p][3, 0] = s_refs[p][3, 0] + x_refs[p][0]
        elif kind == "ZS":
            send_in(p, op[2])
        elif kind == "ZI":
            r = op[2]
            copy = z_copy(p, r, 3, 1) if r == 1 else z_copy(p, r, 1, 0)
            started.append((is_mid, copy))

            @pl.when(is_mid)
            def _():
                z_copy(p, r, r, 2).wait_recv()
                add(p, r, r)
                copy.start()
        elif kind == "FIN":
            for when, slots in ((is_end, (0, 1)), (is_mid, (2, 3))):

                @pl.when(when)
                def _():
                    for slot in slots:
                        z_copy(p, 3, slot, 2).wait_recv()
                        add(p, 3, slot)
        elif kind == "SOLVE":
            solve(p)
            start(a_copy(p, w_refs[p].at[3, 0], w_refs[p].at[3, 1], (3, 1), partner))
            if mode in "2DYZ":
                spread(p, 0, False, mode == "Y")
            if mode == "D":
                for slot, where in ((2, 2), (mid, 1), (mid, 0)):
                    device = (2 * line[where] + 1 - x, my_bin)
                    start(a_copy(p, w_refs[p].at[3, 0], w_refs[p].at[slot, 1], (slot, 1), device))
            if not weighed:
                weighed = True
                small[1].wait()
                weight = inter_ref[...]
                weight = weight * weight
                total = weight[:segs]
                for i in range(1, weight.shape[0] // segs):
                    total = total + weight[i * segs : (i + 1) * segs]
                ebuf_ref[pl.ds(segs, segs), :] = total
            clean(p, 3, (0,))
        elif kind == "AGX":
            a_wait(p, 3, 1)
            if mode == "C":
                spread(p, 0, True, True)
            elif mode == "2":
                spread(p, 1, False, False)
            clean(p, 3, (1,))
        elif kind == "RL":
            relay(p, op[2])
        elif kind == "AG":
            slot, side = op[2], op[3]
            both = mode == "C"
            if mode in "CY" and side == 0:
                pl.when(is_end)(functools.partial(a_wait, p, slot, side, both))
            else:
                a_wait(p, slot, side)
            if mode in "YZ" and side == 0:
                start(a_copy(p, w_refs[p].at[slot, 0], w_refs[p].at[slot, 1], (slot, 1), partner))
            clean(p, slot, (0, 1) if both else (side,))

    def e_copy(d):
        return pltpu.make_async_remote_copy(
            src_ref=ebuf_ref,
            dst_ref=erecv_ref.at[d],
            send_sem=e_send.at[d],
            recv_sem=e_recv.at[d],
            device_id=(me, peers[d]),
            device_id_type=MESH,
        )

    for d in range(n_bin - 1):
        e_copy(d).start()
    for when, copy in started:
        if when is None:
            copy.wait_send()
    for when in (is_mid, is_end):

        @pl.when(when)
        def _():
            for other, copy in started:
                if other is when:
                    copy.wait_send()

    total = ebuf_ref[...]
    for d in range(n_bin - 1):
        e_copy(d).wait_recv()
        total = total + erecv_ref[d]
    number = jnp.sum(total[:segs], axis=1, keepdims=True)
    norm = jnp.sum(jnp.sum(total[segs:], axis=1, keepdims=True), axis=0, keepdims=True)
    own = lax.broadcasted_iota(jnp.int32, (segs, LANES), 0) == lax.broadcasted_iota(jnp.int32, (segs, LANES), 1)
    est_ref[...] = jnp.sum(jnp.where(own, number / jnp.sqrt(norm), 0.0), axis=0, keepdims=True)
    for d in range(n_bin - 1):
        e_copy(d).wait_send()


def store_kernel(cr_ref, ci_ref, est_ref, cr_hbm, ci_hbm, est_out, sems):
    copies = [pltpu.make_async_copy(cr_ref, cr_hbm, sems.at[0]), pltpu.make_async_copy(ci_ref, ci_hbm, sems.at[1])]
    for copy in copies:
        copy.start()
    est_out[...] = est_ref[0, : est_out.shape[0]]
    for copy in copies:
        copy.wait()


def line_on_device(n_seg, n_bin, magnet_real, magnet_imag, detector_real, detector_imag, valid, intersection):
    segs, channels, bins = magnet_real.shape
    detectors = detector_real.shape[1]
    blocks = bins // LANES
    nblk = blocks // n_seg
    rows = (channels + 2 * detectors) * channels
    wrows = 2 * channels * detectors
    f32 = jnp.float32
    pieces, modes, order = schedule(nblk)
    steps = Planner(pieces, modes, order, DEPTH, rows, wrows).plan()
    sizes = (n_seg, n_bin, segs, channels, detectors, nblk, pieces, modes, steps)
    count = len(pieces)
    vmem = pl.BlockSpec(memory_space=pltpu.VMEM)
    hbm = pl.BlockSpec(memory_space=pltpu.HBM)
    scratch = [pltpu.VMEM((LINE, 2, rows * n, LANES), f32) for n, _ in pieces]
    scratch += [pltpu.VMEM((LINE if form == "A" else 1, rows * n, LANES), f32) for n, form in pieces]
    scratch += [pltpu.VMEM((LINE,) + (() if form == "A" else (2,)) + (rows * n, LANES), f32) for n, form in pieces]
    scratch += [pltpu.VMEM((LINE, 2, wrows * n, LANES), f32) for n, _ in pieces]
    scratch += [pltpu.VMEM(a.shape, a.dtype) for a in (magnet_real, magnet_imag, detector_real, detector_imag)]
    scratch += [
        pltpu.SMEM((segs,), jnp.int32),
        pltpu.VMEM((blocks, LANES), f32),
        pltpu.VMEM((blocks, segs * channels, LANES), f32),
        pltpu.VMEM((blocks, segs * channels, LANES), f32),
        pltpu.VMEM((blocks, segs * detectors, LANES), f32),
        pltpu.VMEM((blocks, segs * detectors, LANES), f32),
        pltpu.VMEM((2 * segs, LANES), f32),
        pltpu.VMEM((n_bin - 1, 2 * segs, LANES), f32),
    ]
    dma = pltpu.SemaphoreType.DMA
    scratch += [dma((count, LINE))] * 4 + [dma((count, 12)), dma((count, LINE, 2))]
    scratch += [dma((n_bin - 1,))] * 2 + [dma((2 * LINE, 4)), dma((2,))]
    operands = [magnet_real, magnet_imag, detector_real, detector_imag, valid, intersection.reshape(blocks, LANES)]
    cleaned_real, cleaned_imag, estimate = pl.pallas_call(
        functools.partial(line_kernel, sizes),
        out_shape=(
            pltpu.VMEM((segs, bins), f32),
            pltpu.VMEM((segs, bins), f32),
            pltpu.VMEM((1, LANES), f32),
        ),
        in_specs=[hbm] * 6,
        out_specs=(vmem, vmem, vmem),
        scratch_shapes=scratch,
        compiler_params=pltpu.CompilerParams(
            collective_id=0, has_side_effects=True, vmem_limit_bytes=GRANT
        ),
    )(*[pltpu.with_memory_space_constraint(a, pltpu.HBM) for a in operands])
    return pl.pallas_call(
        store_kernel,
        out_shape=(
            jax.ShapeDtypeStruct((segs, bins), f32),
            jax.ShapeDtypeStruct((segs, bins), f32),
            jax.ShapeDtypeStruct((segs,), f32),
        ),
        in_specs=[vmem] * 3,
        out_specs=(hbm, hbm, vmem),
        scratch_shapes=[dma((2,))],
        compiler_params=pltpu.CompilerParams(vmem_limit_bytes=4 * 1024 * 1024),
    )(cleaned_real, cleaned_imag, estimate)


def solution(mesh):
    placed = (
        P("seg", None, "bin"),
        P("seg", None, "bin"),
        P("seg", None, "bin"),
        P("seg", None, "bin"),
        P("seg"),
        P("bin"),
    )
    n_seg, n_bin = mesh.shape["seg"], mesh.shape["bin"]
    on_device = line_on_device if n_seg == 2 * LINE else halving_on_device
    return jax.shard_map(
        functools.partial(on_device, n_seg, n_bin),
        mesh=mesh,
        in_specs=placed,
        out_specs=(P("seg", "bin"), P("seg", "bin"), P("seg")),
        check_vma=False,
    )
```

```python
import functools
import heapq

import jax
import jax.numpy as jnp
from jax import lax
from jax.experimental import pallas as pl
from jax.experimental.pallas import tpu as pltpu
from jax.sharding import PartitionSpec as P

LANES = 128
MESH = pl.DeviceIdType.MESH
RS_WEIGHTS = [1.0, 1.0, 1.5]


def largest_divisor(value, limit):
    return max(d for d in range(1, limit + 1) if value % d == 0)


def cadd_mul_conj(acc, a, b):
    return (acc[0] - a[0] * b[0] - a[1] * b[1], acc[1] - a[1] * b[0] + a[0] * b[1])


def csub_mul(acc, a, b):
    return (acc[0] - a[0] * b[0] + a[1] * b[1], acc[1] - a[0] * b[1] - a[1] * b[0])


def csub_conj_mul(acc, a, b):
    return (acc[0] - a[0] * b[0] - a[1] * b[1], acc[1] - a[0] * b[1] + a[1] * b[0])


def wiener_solve(below, diag, right):
    channels = len(diag)
    detectors = len(right[0])
    diag = list(diag)
    inverse = [None] * channels
    low = [[None] * channels for _ in range(channels)]
    for j in range(channels):
        inverse[j] = 1.0 / diag[j]
        for i in range(j + 1, channels):
            low[i][j] = (below[i][j][0] * inverse[j], below[i][j][1] * inverse[j])
        for i in range(j + 1, channels):
            a, l = below[i][j], low[i][j]
            diag[i] = diag[i] - l[0] * a[0] - l[1] * a[1]
            for k in range(j + 1, i):
                below[i][k] = cadd_mul_conj(below[i][k], l, below[k][j])
    out = []
    for det in range(detectors):
        y = []
        for i in range(channels):
            run = right[i][det]
            for k in range(i):
                run = csub_mul(run, low[i][k], y[k])
            y.append(run)
        w = [None] * channels
        for i in reversed(range(channels)):
            run = (y[i][0] * inverse[i], y[i][1] * inverse[i])
            for k in range(i + 1, channels):
                run = csub_conj_mul(run, low[k][i], w[k])
            w[i] = run
        out.append(w)
    return out


def step_weights(stages):
    return RS_WEIGHTS if stages == len(RS_WEIGHTS) else [1.0] * stages


def flood_order(n, stages, parts, weights, gather):
    free = [0.0] * stages
    heap, order, count = [], [], {}

    def send(now, st, q, k):
        free[st] = max(now, free[st]) + weights[st]
        heapq.heappush(heap, (free[st] + 0.6, st, q, k))

    if gather:
        for k in range(parts):
            for st in range(stages):
                send(0.0, st, 0, k)
    else:
        for q in first_order(n, stages):
            for k in range(parts):
                send(0.0, 0, q, k)
    while heap:
        now, st, q, k = heapq.heappop(heap)
        order.append((st, q, k))
        bit = n >> (st + 1)
        if gather:
            for to in range(st):
                send(now, to, q + bit, k)
        else:
            d = q - bit
            count[d, k] = count.get((d, k), 0) + 1
            if d and count[d, k] == stages - d.bit_length():
                send(now, stages - d.bit_length(), d, k)
    return order


def first_order(n, stages):
    def key(q):
        return [q >> bit & 1 for bit in range(stages)]

    return sorted(range(n // 2, n), key=key, reverse=True)


def halving_kernel(
    sizes, mr_ref, mi_ref, hr_ref, hi_ref, valid_ref, inter_ref,
    cr_ref, ci_ref, est_ref,
    s_ref, recv_ref, w_ref, mfr_ref, mfi_ref, hfr_ref, hfi_ref, ebuf_ref, erecv_ref,
    rs_send, rs_recv, ag_send, ag_recv, e_send, e_recv,
):
    n_seg, n_bin, segs, channels, detectors, blocks, chunks, wchunks = sizes
    stages = n_seg.bit_length() - 1
    half = channels // 2
    nblk = blocks // n_seg
    groups = channels + 2 * detectors
    per = groups // chunks
    wrows = 2 * channels * detectors
    wper = wrows // wchunks

    me = lax.axis_index("seg")
    my_bin = lax.axis_index("bin")
    bits = [lax.rem(lax.div(me, 1 << st), 2) for st in range(stages)]
    partner = [me + (1 - 2 * bits[st]) * (1 << st) for st in range(stages)]
    peers = [lax.rem(my_bin + d, n_bin) for d in range(1, n_bin)]

    barrier = pltpu.get_barrier_semaphore()
    for st in range(stages):
        pl.semaphore_signal(barrier, inc=1, device_id=(partner[st], my_bin), device_id_type=MESH)
    for peer in peers:
        pl.semaphore_signal(barrier, inc=1, device_id=(me, peer), device_id_type=MESH)

    def position(q):
        pos = 0
        for st in range(stages):
            digit = lax.rem(lax.div(q, n_seg >> (st + 1)), 2)
            pos = pos + (bits[st] + digit - 2 * bits[st] * digit) * (n_seg >> (st + 1))
        return pos

    sub = lax.broadcasted_iota(jnp.int32, (channels, LANES), 0)

    def spectra(q):
        pos = position(q)

        def body(blk, carry):
            b = pos * nblk + blk
            lanes = pl.ds(pl.multiple_of(b * LANES, LANES), LANES)
            acc = None
            for s in range(segs):
                mr = mr_ref[s, :, lanes].astype(jnp.float32)
                mi = mi_ref[s, :, lanes].astype(jnp.float32)
                hr = hr_ref[s, :, lanes].astype(jnp.float32)
                hi = hi_ref[s, :, lanes].astype(jnp.float32)
                mfr_ref[b, pl.ds(s * channels, channels), :] = mr
                mfi_ref[b, pl.ds(s * channels, channels), :] = mi
                hfr_ref[b, pl.ds(s * detectors, detectors), :] = hr
                hfi_ref[b, pl.ds(s * detectors, detectors), :] = hi
                v = valid_ref[s].astype(jnp.float32)
                kr, ki = mr * v, mi * v
                terms = [kr * mr + ki * mi]
                for r in range(1, half + 1):
                    br = pltpu.roll(mr, channels - r, 0)
                    bi = pltpu.roll(mi, channels - r, 0)
                    terms.append(kr * br + ki * bi)
                    terms.append(ki * br - kr * bi)
                for k in range(detectors):
                    br = jnp.broadcast_to(hr[k : k + 1], (channels, LANES))
                    bi = jnp.broadcast_to(hi[k : k + 1], (channels, LANES))
                    terms.append(kr * br + ki * bi)
                    terms.append(ki * br - kr * bi)
                acc = terms if acc is None else [a + t for a, t in zip(acc, terms)]
            packed = jnp.where(sub < half, acc[channels - 1], acc[channels])
            rows = acc[: channels - 1] + [packed] + acc[channels + 1 :]
            for g in range(groups):
                at = pl.multiple_of((g % per) * nblk * channels + blk * channels, channels)
                s_ref[q, g // per, pl.ds(at, channels), :] = rows[g]
            return carry

        lax.fori_loop(0, nblk, body, 0)

    def rs_copy(st, q, k):
        return pltpu.make_async_remote_copy(
            src_ref=s_ref.at[q, k],
            dst_ref=recv_ref.at[q - 1, k],
            send_sem=rs_send.at[q - 1, k],
            recv_sem=rs_recv.at[q - 1, k],
            device_id=(partner[st], my_bin),
            device_id_type=MESH,
        )

    first = first_order(n_seg, stages)
    assert first[0] == n_seg - 1
    spectra(first[0])
    pl.semaphore_wait(barrier, stages + n_bin - 1)
    for k in range(chunks):
        rs_copy(0, first[0], k).start()

    def mirrored(i, low):
        q = 0 if low else n_seg // 2
        for bit in range(stages - 1):
            digit = 1 - lax.rem(lax.div(i, n_seg >> (bit + 2)), 2)
            q = q + digit * (1 << bit)
        return q

    def early(i, carry):
        q = mirrored(i, False)
        spectra(q)
        for k in range(chunks):
            rs_copy(0, q, k).start()
        return carry

    lax.fori_loop(1, n_seg // 2, early, 0)

    def late(i, carry):
        spectra(mirrored(i, True))
        return carry

    lax.fori_loop(0, n_seg // 2, late, 0)

    got = {}
    for st, q, k in flood_order(n_seg, stages, chunks, step_weights(stages), False):
        rs_copy(st, q, k).wait_recv()
        d = q - (n_seg >> (st + 1))
        s_ref[d, k] = s_ref[d, k] + recv_ref[q - 1, k]
        got[d, k] = got.get((d, k), 0) + 1
        if d and got[d, k] == stages - d.bit_length():
            rs_copy(stages - d.bit_length(), d, k).start()

    def entry(g, row):
        start = (g % per) * nblk * channels + row
        if nblk == 1:
            return s_ref[0, g // per, pl.ds(start, 1), :]
        return s_ref[0, g // per, pl.ds(start, nblk, stride=channels), :]

    def above(a, b):
        r = b - a
        if r < half:
            return (entry(2 * r - 1, a), entry(2 * r, a))
        if r == half:
            return (entry(channels - 1, a), -entry(channels - 1, a + half))
        r = channels - r
        return (entry(2 * r - 1, b), -entry(2 * r, b))

    below = [[None] * channels for _ in range(channels)]
    for i in range(channels):
        for j in range(i):
            value = above(j, i)
            below[i][j] = (value[0], -value[1])
    diag = [entry(0, c) + 1.0 for c in range(channels)]
    right = [
        [(entry(channels + 2 * k, c), entry(channels + 2 * k + 1, c)) for k in range(detectors)]
        for c in range(channels)
    ]
    filt = wiener_solve(below, diag, right)
    for k in range(detectors):
        for c in range(channels):
            for part in range(2):
                e = (k * channels + c) * 2 + part
                w_ref[0, e // wper, pl.ds((e % wper) * nblk, nblk), :] = filt[k][c][part]

    def ag_copy(st, q, k):
        to = q + (n_seg >> (st + 1))
        return pltpu.make_async_remote_copy(
            src_ref=w_ref.at[q, k],
            dst_ref=w_ref.at[to, k],
            send_sem=ag_send.at[to - 1, k],
            recv_sem=ag_recv.at[to - 1, k],
            device_id=(partner[st], my_bin),
            device_id_type=MESH,
        )

    def clean(q, carry):
        pos = position(q)

        def body(blk, carry):
            num, sq = carry
            b = pos * nblk + blk
            lanes = pl.ds(pl.multiple_of(b * LANES, LANES), LANES)
            g = [
                (
                    hfr_ref[b, pl.ds(k, segs, stride=detectors), :],
                    hfi_ref[b, pl.ds(k, segs, stride=detectors), :],
                )
                for k in range(detectors)
            ]
            for c in range(channels):
                m = (
                    mfr_ref[b, pl.ds(c, segs, stride=channels), :],
                    mfi_ref[b, pl.ds(c, segs, stride=channels), :],
                )
                for k in range(detectors):
                    e = (k * channels + c) * 2
                    w = [
                        w_ref[q, f // wper, pl.ds((f % wper) * nblk + blk, 1), :]
                        for f in (e, e + 1)
                    ]
                    g[k] = csub_conj_mul(g[k], w, m)
            real = g[0][0] * g[1][0] + g[0][1] * g[1][1]
            imag = g[0][1] * g[1][0] - g[0][0] * g[1][1]
            cr_ref[:, lanes] = real
            ci_ref[:, lanes] = imag
            weight = inter_ref[pl.ds(b, 1), :]
            return num + real * weight, sq + weight * weight

        return lax.fori_loop(0, nblk, body, carry)

    for k in range(wchunks):
        for st in range(stages):
            ag_copy(st, 0, k).start()
    sums = clean(0, (jnp.zeros((segs, LANES), jnp.float32), jnp.zeros((1, LANES), jnp.float32)))
    seen = {}
    for st, q, k in flood_order(n_seg, stages, wchunks, step_weights(stages), True):
        ag_copy(st, q, k).wait_recv()
        to = q + (n_seg >> (st + 1))
        for on in range(st):
            ag_copy(on, to, k).start()
        seen[to] = seen.get(to, 0) + 1
        if seen[to] == wchunks:
            sums = clean(to, sums)
    num, sq = sums
    ebuf_ref[pl.ds(0, segs), :] = num
    ebuf_ref[pl.ds(segs, segs), :] = jnp.broadcast_to(sq, (segs, LANES))

    def e_copy(d):
        return pltpu.make_async_remote_copy(
            src_ref=ebuf_ref,
            dst_ref=erecv_ref.at[d],
            send_sem=e_send.at[d],
            recv_sem=e_recv.at[d],
            device_id=(me, peers[d]),
            device_id_type=MESH,
        )

    for d in range(n_bin - 1):
        e_copy(d).start()
    for q in range(1, n_seg):
        st = stages - q.bit_length()
        for k in range(chunks):
            rs_copy(st, q, k).wait_send()
        for k in range(wchunks):
            ag_copy(st, q - (n_seg >> (st + 1)), k).wait_send()
    total = ebuf_ref[...]
    for d in range(n_bin - 1):
        e_copy(d).wait_recv()
        total = total + erecv_ref[d]
    total = jnp.sum(total, axis=1, keepdims=True)
    est_ref[...] = jnp.broadcast_to(total[:segs] / jnp.sqrt(total[segs:]), (segs, LANES))
    for d in range(n_bin - 1):
        e_copy(d).wait_send()


def halving_on_device(n_seg, n_bin, magnet_real, magnet_imag, detector_real, detector_imag, valid, intersection):
    segs, channels, bins = magnet_real.shape
    detectors = detector_real.shape[1]
    blocks = bins // LANES
    nblk = blocks // n_seg
    groups = channels + 2 * detectors
    chunks = largest_divisor(groups, 4)
    wrows = 2 * channels * detectors
    wchunks = largest_divisor(wrows, 2)
    rows = groups // chunks * nblk * channels
    f32 = jnp.float32
    sizes = (n_seg, n_bin, segs, channels, detectors, blocks, chunks, wchunks)
    vmem = pl.BlockSpec(memory_space=pltpu.VMEM)
    cleaned_real, cleaned_imag, estimate = pl.pallas_call(
        functools.partial(halving_kernel, sizes),
        out_shape=(
            jax.ShapeDtypeStruct((segs, bins), f32),
            jax.ShapeDtypeStruct((segs, bins), f32),
            jax.ShapeDtypeStruct((segs, LANES), f32),
        ),
        in_specs=[vmem] * 4 + [pl.BlockSpec(memory_space=pltpu.SMEM), vmem],
        out_specs=(vmem, vmem, vmem),
        scratch_shapes=[
            pltpu.VMEM((n_seg, chunks, rows, LANES), f32),
            pltpu.VMEM((n_seg - 1, chunks, rows, LANES), f32),
            pltpu.VMEM((n_seg, wchunks, wrows // wchunks * nblk, LANES), f32),
            pltpu.VMEM((blocks, segs * channels, LANES), f32),
            pltpu.VMEM((blocks, segs * channels, LANES), f32),
            pltpu.VMEM((blocks, segs * detectors, LANES), f32),
            pltpu.VMEM((blocks, segs * detectors, LANES), f32),
            pltpu.VMEM((2 * segs, LANES), f32),
            pltpu.VMEM((n_bin - 1, 2 * segs, LANES), f32),
        ]
        + [
            pltpu.SemaphoreType.DMA((n_seg - 1, chunks)),
            pltpu.SemaphoreType.DMA((n_seg - 1, chunks)),
            pltpu.SemaphoreType.DMA((n_seg - 1, wchunks)),
            pltpu.SemaphoreType.DMA((n_seg - 1, wchunks)),
            pltpu.SemaphoreType.DMA((n_bin - 1,)),
            pltpu.SemaphoreType.DMA((n_bin - 1,)),
        ],
        compiler_params=pltpu.CompilerParams(
            collective_id=0, has_side_effects=True, vmem_limit_bytes=56 * 1024 * 1024
        ),
    )(
        magnet_real, magnet_imag, detector_real, detector_imag, valid,
        intersection.reshape(blocks, LANES),
    )
    return cleaned_real, cleaned_imag, estimate[:, 0]


LINE = 4
DEPTH = 4
GRANT = 24 * 1024 * 1024
ROW_US = 0.01128
HOP_US = (0.0, 2.6, 3.0, 3.4, 3.8)
GROUP_SETS = ((0, 1), (2, 3))


TUNED = {
    8: (
        (3, 2, 2, 1),
        "Y2ZY",
        ((0, 0), (2, 1), (0, 1), (2, 0), (1, 0), (0, 2), (3, 3), (1, 1), (0, 3), (2, 2), (1, 2), (2, 3), (1, 3)),
    ),
}


def schedule(nblk):
    if nblk in TUNED:
        sizes, modes, order = TUNED[nblk]
        pieces = [(n, "A") for n in sizes[:-1]] + [(sizes[-1], "B")]
        return pieces, modes, list(order)
    pieces = [(n, "A") for n in [1] * (nblk - 1)] + [(1, "B")] if nblk > 1 else [(nblk, "A")]
    return pieces, "Y" * len(pieces), tick_order(pieces)


def tick_order(pieces):
    first = [p for p, (_, kind) in enumerate(pieces) if kind == "A"]
    order = [(first[0], 0), (first[0], 1)]
    for p, nxt in zip(first, first[1:] + [None]):
        if nxt is not None:
            order += [(nxt, 0), (nxt, 1)]
        order += [(p, 2), (p, 3)]
    return order + [(p, 3) for p, (_, kind) in enumerate(pieces) if kind == "B"]


class Planner:
    def __init__(self, pieces, modes, order, depth, rows, wrows):
        self.pieces, self.modes, self.order, self.depth = pieces, modes, order, depth
        self.rows, self.wrows = rows, wrows
        self.clock = [2.0, 2.0]
        self.link, self.message, self.steps = {}, {}, []

    def send(self, role, key, path, rows):
        start = self.clock[role]
        for name in path:
            start = max(start, self.link.get(name, 0.0))
            self.link[name] = start + rows * ROW_US
        self.message[key] = start + rows * ROW_US + HOP_US[len(path)]

    def waits(self, op):
        kind, p = op[0], op[1]
        if kind == "XR":
            return [[("x", 0, p, op[2])], [("x", 1, p, op[2])]]
        if kind == "ZI":
            return [[], [("z", 1, p, op[2])]]
        if kind == "FIN":
            return [[("z", 0, p, 0), ("z", 0, p, 1)], [("z", 1, p, 2), ("z", 1, p, 3)]]
        if kind == "AGX":
            return [[("ax", 0, p)], [("ax", 1, p)]]
        if kind == "RL":
            return [[], [("a", 1, p, op[2], 0)]]
        if kind == "AG":
            both = [[("a", r, p, op[2], op[3])] for r in range(2)]
            if self.modes[p] in "CY" and op[3] == 0:
                both[1] = []
            return both
        return [[], []]

    def column(self, p, side, rows, chain):
        self.send(0, ("a", 1, p, 2, side), ["in"], rows)
        self.send(1, ("a", 0, p, 2, side), ["out"], rows)
        self.send(1, ("a", 1, p, 1, side), ["mid"], rows)
        if not chain:
            self.send(0, ("a", 1, p, 0, side), ["in", "mid"], rows)
            self.send(1, ("a", 0, p, 1, side), ["mid", "out"], rows)
            self.send(0, ("a", 0, p, 0, side), ["in", "mid", "out"], rows)

    def diagonal(self, p, rows):
        self.send(0, ("a", 1, p, 2, 1), [("x", 0), "in"], rows)
        self.send(1, ("a", 0, p, 2, 1), [("x", 1), "out"], rows)
        self.send(1, ("a", 1, p, 1, 1), [("x", 1), "mid"], rows)
        self.send(0, ("a", 1, p, 0, 1), [("x", 0), "in", "mid"], rows)
        self.send(1, ("a", 0, p, 1, 1), [("x", 1), "mid", "out"], rows)
        self.send(0, ("a", 0, p, 0, 1), [("x", 0), "in", "mid", "out"], rows)

    def lines(self, p, r, rows):
        if r < 3:
            self.send(0, ("z", 1, p, r), ["in"], rows)
        if r == 2:
            self.send(1, ("z", 0, p, 0), ["out"], rows)

    def run(self, op):
        for role, keys in enumerate(self.waits(op)):
            self.clock[role] = max([self.clock[role]] + [self.message[key] for key in keys]) + 0.05
        kind, p = op[0], op[1]
        size, form = self.pieces[p]
        rows, wrows, mode = self.rows * size, self.wrows * size, self.modes[p]
        work = 0.0
        if kind == "SP":
            work = 0.13 * size * len(op[3]) * len(op[2])
        elif kind == "XS":
            for role in range(2):
                self.send(role, ("x", role, p, op[2]), [("x", role)], rows)
        elif kind == "XR":
            work = 0.03 * size
        elif kind == "FIN":
            work = 0.06 * size
        elif kind == "SOLVE":
            work = 0.6 + 0.06 * size
        elif kind in ("AGX", "AG"):
            work = 0.06 * size * (2 if kind == "AG" and mode == "C" else 1)
        self.clock = [c + (0.0 if kind in ("SOLVE", "AGX", "AG") else work) for c in self.clock]
        if kind == "XR" and form == "A":
            self.lines(p, op[2], rows)
        elif kind == "ZS":
            self.lines(p, op[2], rows * 2)
        elif kind == "ZI":
            both = rows * (2 if form == "B" else 1)
            if op[2] == 1:
                self.send(1, ("z", 1, p, 3), ["mid"], both)
            else:
                self.send(1, ("z", 0, p, 1), ["mid", "out"], both)
        elif kind == "SOLVE":
            self.clock = [c + 0.6 for c in self.clock]
            for role in range(2):
                self.send(role, ("ax", role, p), [("x", role)], wrows)
            if mode in "2DYZ":
                self.column(p, 0, wrows, mode == "Y")
            if mode == "D":
                self.diagonal(p, wrows)
            work = work - 0.6
        elif kind == "AGX":
            if mode in "2C":
                self.column(p, 0 if mode == "C" else 1, wrows * (2 if mode == "C" else 1), mode == "C")
        elif kind == "RL":
            both = wrows * (2 if mode == "C" else 1)
            if op[2] == 2:
                self.send(1, ("a", 1, p, 0, 0), ["mid"], both)
            else:
                self.send(1, ("a", 0, p, op[2], 0), ["out"], both)
        elif kind == "AG" and mode in "YZ" and op[3] == 0:
            for role in range(2):
                self.send(role, ("a", role, p, op[2], 1), [("x", role)], wrows)
        if kind in ("SOLVE", "AGX", "AG"):
            self.clock = [c + work for c in self.clock]
        self.steps.append(op)

    def spectra_steps(self):
        lead = self.order[0]
        for p, (_, form) in enumerate(self.pieces):
            for group in GROUP_SETS:
                if (p, group[0]) == lead:
                    yield ("SP", p, (group[0],), (1,))
                    yield ("SP", p, (group[0],), (0,))
                    yield ("SP", p, group[1:], (1, 0))
                else:
                    yield ("SP", p, group, (1, 0))

    def needs(self):
        need, order = {}, self.order
        made = {}
        for op in self.spectra_steps():
            need[op] = []
            for r in op[2]:
                for side in op[3]:
                    made[op[1], r, side] = op
        for i, (p, r) in enumerate(order):
            back = [("XR",) + order[i - self.depth]] if i >= self.depth else []
            back += [("XS",) + order[i - 1]] if i else []
            chain = [("XR",) + order[i - 1]] if i else []
            if self.pieces[p][1] == "A":
                need["XS", p, r] = [made[p, r, 1]] + back
                need["XR", p, r] = [("XS", p, r), made[p, r, 0]] + chain
            else:
                need["XS", p, r] = [("FIN", p)] + back
                need["XR", p, r] = [("XS", p, r)] + chain
        for p, (_, form) in enumerate(self.pieces):
            kind = "XR" if form == "A" else "ZS"
            if form == "B":
                for r in range(3):
                    need["ZS", p, r] = [made[p, r, 0], made[p, r, 1]]
            for r in range(2):
                need["ZI", p, r] = [(kind, p, r)]
            need["FIN", p] = [("ZI", p, 0), ("ZI", p, 1), (kind, p, 2)]
            need["FIN", p] += [("XR", p, 3)] if form == "A" else [made[p, 3, 0], made[p, 3, 1]]
            need["SOLVE", p] = [("FIN", p) if form == "A" else ("XR", p, 3)]
            need["AGX", p] = [("SOLVE", p)]
            mode = self.modes[p]
            start = ("AGX", p) if mode == "C" else ("SOLVE", p)
            for slot in (2, 1, 0):
                if mode in "CY":
                    need["RL", p, slot] = [start]
                    need["AG", p, slot, 0] = [("RL", p, slot)]
                else:
                    need["AG", p, slot, 0] = [start]
                if mode in "YZ":
                    need["AG", p, slot, 1] = [("AG", p, slot, 0)]
                elif mode in "2D":
                    need["AG", p, slot, 1] = [("AGX", p) if mode == "2" else start]
        return need

    def plan(self):
        need = self.needs()
        place = {op: i for i, op in enumerate(need)}
        tick = {key: i for i, key in enumerate(self.order)}
        done = set()
        while len(done) < len(need):
            best = None
            for op in need:
                if op in done or any(other not in done for other in need[op]):
                    continue
                keys = self.waits(op)
                if any(key not in self.message for role in range(2) for key in keys[role]):
                    continue
                ready = max(max([self.clock[r]] + [self.message[key] for key in keys[r]]) for r in range(2))
                now = max(self.clock)
                urgent = -1.0
                if op[0] in ("SP", "ZS") and ready <= now + 1e-6:
                    form = self.pieces[op[1]][1]
                    r = op[2] if op[0] == "ZS" else op[2][0]
                    urgent = 2.5 + 0.1 * r if form == "B" else tick[op[1], r]
                key = (round(max(ready, now), 3), urgent, place[op])
                if best is None or key < best[0]:
                    best = (key, op)
            self.run(best[1])
            done.add(best[1])
        return self.steps


def line_kernel(sizes, mr_hbm, mi_hbm, hr_hbm, hi_hbm, valid_hbm, inter_hbm, cr_ref, ci_ref, est_ref, *scratch):
    n_seg, n_bin, segs, channels, detectors, nblk, pieces, modes, steps = sizes
    count = len(pieces)
    half = channels // 2
    groups = channels + 2 * detectors
    rows = groups * channels
    wrows = 2 * channels * detectors
    scratch = list(scratch)
    take = lambda n: [scratch.pop(0) for _ in range(n)]
    s_refs, x_refs, z_refs, w_refs = take(count), take(count), take(count), take(count)
    mr_ref, mi_ref, hr_ref, hi_ref, valid_ref, inter_ref = take(6)
    mfr_ref, mfi_ref, hfr_ref, hfi_ref, ebuf_ref, erecv_ref = take(6)
    x_send, x_recv, z_send, z_recv, a_send, a_recv, e_send, e_recv, in_sem, small_sem = take(10)

    me = lax.axis_index("seg")
    my_bin = lax.axis_index("bin")
    x = lax.rem(me, 2)
    z = lax.div(me, 2)
    z_hi, z_lo = lax.div(z, 2), lax.rem(z, 2)
    mid = z_hi + z_lo - 2 * z_hi * z_lo
    is_mid, is_end = mid == 1, mid == 0
    sib = 2 * z_hi + 1 - z_lo
    far_mid = 2 - z_hi
    far_end = 3 - 3 * z_hi
    line = {3: z, 2: sib, 1: far_mid, 0: far_end}
    partner = (2 * z + 1 - x, my_bin)
    peers = [lax.rem(my_bin + d, n_bin) for d in range(1, n_bin)]

    def column(where):
        return (2 * line[where] + x, my_bin)

    def lanes_of(r, side):
        return 2 * line[r] + x + side - 2 * side * x

    barrier = pltpu.get_barrier_semaphore()
    for d in range(1, n_seg):
        pl.semaphore_signal(barrier, inc=1, device_id=(lax.rem(me + d, n_seg), my_bin), device_id_type=MESH)
    for peer in peers:
        pl.semaphore_signal(barrier, inc=1, device_id=(me, peer), device_id_type=MESH)

    small = [
        pltpu.make_async_copy(valid_hbm, valid_ref, small_sem.at[0]),
        pltpu.make_async_copy(inter_hbm, inter_ref, small_sem.at[1]),
    ]
    small[0].start()
    loads = {}
    for i, (r, side) in enumerate([(r, side) for r in range(4) for side in (1, 0)]):
        lanes = pl.ds(pl.multiple_of(lanes_of(r, side) * nblk * LANES, nblk * LANES), nblk * LANES)
        loads[r, side] = [
            pltpu.make_async_copy(src.at[:, :, lanes], dst.at[:, :, lanes], in_sem.at[i, j])
            for j, (src, dst) in enumerate(
                [(mr_hbm, mr_ref), (mi_hbm, mi_ref), (hr_hbm, hr_ref), (hi_hbm, hi_ref)]
            )
        ]
        for copy in loads[r, side]:
            copy.start()
    small[1].start()
    small[0].wait()

    first_block = [sum(size for size, _ in pieces[:p]) for p in range(count)]
    sub = lax.broadcasted_iota(jnp.int32, (channels, LANES), 0)
    loaded = set()

    def spectra(p, where, sides):
        size = pieces[p][0]
        for r in where:
            for side in sides:
                if (r, side) not in loaded:
                    loaded.add((r, side))
                    for copy in loads[r, side]:
                        copy.wait()

        def body(i, carry):
            r = where[0] + lax.div(i, size * len(sides))
            side = sides[0] if len(sides) == 1 else 1 - lax.rem(lax.div(i, size), 2)
            blk = lax.rem(i, size)
            if len(where) == 1:
                at = line[where[0]]
            else:
                at = line[where[0]] + (r - where[0]) * (line[where[1]] - line[where[0]])
            owner = 2 * at + x + side - 2 * side * x
            b = owner * nblk + first_block[p] + blk
            lanes = pl.ds(pl.multiple_of(b * LANES, LANES), LANES)
            acc = None
            for s in range(segs):
                mr = mr_ref[s, :, lanes].astype(jnp.float32)
                mi = mi_ref[s, :, lanes].astype(jnp.float32)
                hr = hr_ref[s, :, lanes].astype(jnp.float32)
                hi = hi_ref[s, :, lanes].astype(jnp.float32)
                mfr_ref[b, pl.ds(s * channels, channels), :] = mr
                mfi_ref[b, pl.ds(s * channels, channels), :] = mi
                hfr_ref[b, pl.ds(s * detectors, detectors), :] = hr
                hfi_ref[b, pl.ds(s * detectors, detectors), :] = hi
                v = valid_ref[s].astype(jnp.float32)
                kr, ki = mr * v, mi * v
                terms = [kr * mr + ki * mi]
                for turn in range(1, half + 1):
                    br = pltpu.roll(mr, channels - turn, 0)
                    bi = pltpu.roll(mi, channels - turn, 0)
                    terms.append(kr * br + ki * bi)
                    terms.append(ki * br - kr * bi)
                for k in range(detectors):
                    br = jnp.broadcast_to(hr[k : k + 1], (channels, LANES))
                    bi = jnp.broadcast_to(hi[k : k + 1], (channels, LANES))
                    terms.append(kr * br + ki * bi)
                    terms.append(ki * br - kr * bi)
                acc = terms if acc is None else [a + t for a, t in zip(acc, terms)]
            packed = jnp.where(sub < half, acc[channels - 1], acc[channels])
            out = acc[: channels - 1] + [packed] + acc[channels + 1 :]
            for g in range(groups):
                start = pl.multiple_of((g * size + blk) * channels, channels)
                s_refs[p][r, side, pl.ds(start, channels), :] = out[g]
            return carry

        lax.fori_loop(0, size * len(sides) * len(where), body, 0)

    def solve(p):
        size = pieces[p][0]
        ref = s_refs[p]

        def entry(g, row):
            start = g * size * channels + row
            if size == 1:
                return ref[3, 0, pl.ds(start, 1), :]
            return ref[3, 0, pl.ds(start, size, stride=channels), :]

        def above(a, b):
            r = b - a
            if r < half:
                return (entry(2 * r - 1, a), entry(2 * r, a))
            if r == half:
                return (entry(channels - 1, a), -entry(channels - 1, a + half))
            r = channels - r
            return (entry(2 * r - 1, b), -entry(2 * r, b))

        below = [[None] * channels for _ in range(channels)]
        for i in range(channels):
            for j in range(i):
                value = above(j, i)
                below[i][j] = (value[0], -value[1])
        diag = [entry(0, c) + 1.0 for c in range(channels)]
        right = [
            [(entry(channels + 2 * k, c), entry(channels + 2 * k + 1, c)) for k in range(detectors)]
            for c in range(channels)
        ]
        filt = wiener_solve(below, diag, right)
        for k in range(detectors):
            for c in range(channels):
                for part in range(2):
                    e = (k * channels + c) * 2 + part
                    w_refs[p][3, 0, pl.ds(e * size, size), :] = filt[k][c][part]

    def clean(p, r, sides):
        size = pieces[p][0]

        def body(i, carry):
            if len(sides) == 1:
                side, blk = sides[0], i
            else:
                side, blk = lax.div(i, size), lax.rem(i, size)
            b = lanes_of(r, side) * nblk + first_block[p] + blk
            lanes = pl.ds(pl.multiple_of(b * LANES, LANES), LANES)
            g = [
                (
                    hfr_ref[b, pl.ds(k, segs, stride=detectors), :],
                    hfi_ref[b, pl.ds(k, segs, stride=detectors), :],
                )
                for k in range(detectors)
            ]
            for c in range(channels):
                m = (
                    mfr_ref[b, pl.ds(c, segs, stride=channels), :],
                    mfi_ref[b, pl.ds(c, segs, stride=channels), :],
                )
                for k in range(detectors):
                    e = (k * channels + c) * 2
                    w = [w_refs[p][r, side, pl.ds(f * size + blk, 1), :] for f in (e, e + 1)]
                    g[k] = csub_conj_mul(g[k], w, m)
            real = g[0][0] * g[1][0] + g[0][1] * g[1][1]
            imag = g[0][1] * g[1][0] - g[0][0] * g[1][1]
            cr_ref[:, lanes] = real
            ci_ref[:, lanes] = imag
            ebuf_ref[pl.ds(0, segs), :] = ebuf_ref[pl.ds(0, segs), :] + real * inter_ref[pl.ds(b, 1), :]
            return carry

        if size * len(sides) == 1:
            body(0, 0)
        else:
            lax.fori_loop(0, size * len(sides), body, 0)

    started = []

    def remote(src, dst, send_sem, recv_sem, device):
        return pltpu.make_async_remote_copy(
            src_ref=src, dst_ref=dst, send_sem=send_sem, recv_sem=recv_sem,
            device_id=device, device_id_type=MESH,
        )

    def start(copy, when=None):
        started.append((when, copy))
        if when is None:
            copy.start()
        else:
            pl.when(when)(copy.start)

    def x_copy(p, r):
        src, dst = (s_refs[p].at[r, 1], x_refs[p].at[r]) if pieces[p][1] == "A" else (s_refs[p].at[3, 1], x_refs[p].at[0])
        return remote(src, dst, x_send.at[p, r], x_recv.at[p, r], partner)

    def part(p, r):
        return s_refs[p].at[r, 0] if pieces[p][1] == "A" else s_refs[p].at[r]

    def z_copy(p, r, slot, where):
        return remote(part(p, r), z_refs[p].at[slot], z_send.at[p, r], z_recv.at[p, slot], column(where))

    def send_in(p, r):
        if r < 3:
            start(z_copy(p, r, r, 2), is_end)
        if r == 2:
            start(z_copy(p, r, 0, 2), is_mid)

    def add(p, r, slot):
        ref = part(p, r)
        ref[...] = ref[...] + z_refs[p][slot]

    sends = [0] * count

    def a_copy(p, src, dst, slot_at, device):
        sends[p] += 1
        return remote(src, dst, a_send.at[p, sends[p] - 1], a_recv.at[p, slot_at[0], slot_at[1]], device)

    def a_wait(p, slot, side, both=False):
        ref = w_refs[p].at[slot] if both else w_refs[p].at[slot, side]
        remote(ref, ref, a_send.at[p, 0], a_recv.at[p, slot, side], partner).wait_recv()

    def spread(p, side, both, chain):
        src = w_refs[p].at[3] if both else w_refs[p].at[3, side]

        def to(slot, where, when=None):
            dst = w_refs[p].at[slot] if both else w_refs[p].at[slot, side]
            start(a_copy(p, src, dst, (slot, side), column(where)), when)

        to(2, 2)
        to(mid, 1, is_mid if chain else None)
        if not chain:
            to(mid, 0)

    def relay(p, slot):
        both = modes[p] == "C"
        pick = (lambda n: w_refs[p].at[n]) if both else (lambda n: w_refs[p].at[n, 0])
        to, where = (0, 1) if slot == 2 else (slot, 2)
        copy = a_copy(p, pick(slot), pick(to), (to, 0), column(where))
        started.append((is_mid, copy))

        @pl.when(is_mid)
        def _():
            a_wait(p, slot, 0, both)
            copy.start()

    ebuf_ref[pl.ds(0, segs), :] = jnp.zeros((segs, LANES), jnp.float32)
    entered = weighed = False
    for op in steps:
        kind, p = op[0], op[1]
        form, mode = pieces[p][1], modes[p]
        if kind == "SP":
            spectra(p, op[2], op[3])
            continue
        if not entered:
            pl.semaphore_wait(barrier, n_seg + n_bin - 2)
            entered = True
        if kind == "XS":
            start(x_copy(p, op[2]))
        elif kind == "XR":
            r = op[2]
            x_copy(p, r).wait_recv()
            if form == "A":
                s_refs[p][r, 0] = s_refs[p][r, 0] + x_refs[p][r]
                send_in(p, r)
            else:
                s_refs[p][3, 0] = s_refs[p][3, 0] + x_refs[p][0]
        elif kind == "ZS":
            send_in(p, op[2])
        elif kind == "ZI":
            r = op[2]
            copy = z_copy(p, r, 3, 1) if r == 1 else z_copy(p, r, 1, 0)
            started.append((is_mid, copy))

            @pl.when(is_mid)
            def _():
                z_copy(p, r, r, 2).wait_recv()
                add(p, r, r)
                copy.start()
        elif kind == "FIN":
            for when, slots in ((is_end, (0, 1)), (is_mid, (2, 3))):

                @pl.when(when)
                def _():
                    for slot in slots:
                        z_copy(p, 3, slot, 2).wait_recv()
                        add(p, 3, slot)
        elif kind == "SOLVE":
            solve(p)
            start(a_copy(p, w_refs[p].at[3, 0], w_refs[p].at[3, 1], (3, 1), partner))
            if mode in "2DYZ":
                spread(p, 0, False, mode == "Y")
            if mode == "D":
                for slot, where in ((2, 2), (mid, 1), (mid, 0)):
                    device = (2 * line[where] + 1 - x, my_bin)
                    start(a_copy(p, w_refs[p].at[3, 0], w_refs[p].at[slot, 1], (slot, 1), device))
            if not weighed:
                weighed = True
                small[1].wait()
                weight = inter_ref[...]
                weight = weight * weight
                total = weight[:segs]
                for i in range(1, weight.shape[0] // segs):
                    total = total + weight[i * segs : (i + 1) * segs]
                ebuf_ref[pl.ds(segs, segs), :] = total
            clean(p, 3, (0,))
        elif kind == "AGX":
            a_wait(p, 3, 1)
            if mode == "C":
                spread(p, 0, True, True)
            elif mode == "2":
                spread(p, 1, False, False)
            clean(p, 3, (1,))
        elif kind == "RL":
            relay(p, op[2])
        elif kind == "AG":
            slot, side = op[2], op[3]
            both = mode == "C"
            if mode in "CY" and side == 0:
                pl.when(is_end)(functools.partial(a_wait, p, slot, side, both))
            else:
                a_wait(p, slot, side)
            if mode in "YZ" and side == 0:
                start(a_copy(p, w_refs[p].at[slot, 0], w_refs[p].at[slot, 1], (slot, 1), partner))
            clean(p, slot, (0, 1) if both else (side,))

    def e_copy(d):
        return pltpu.make_async_remote_copy(
            src_ref=ebuf_ref,
            dst_ref=erecv_ref.at[d],
            send_sem=e_send.at[d],
            recv_sem=e_recv.at[d],
            device_id=(me, peers[d]),
            device_id_type=MESH,
        )

    for d in range(n_bin - 1):
        e_copy(d).start()
    for when, copy in started:
        if when is None:
            copy.wait_send()
    for when in (is_mid, is_end):

        @pl.when(when)
        def _():
            for other, copy in started:
                if other is when:
                    copy.wait_send()

    total = ebuf_ref[...]
    for d in range(n_bin - 1):
        e_copy(d).wait_recv()
        total = total + erecv_ref[d]
    number = jnp.sum(total[:segs], axis=1, keepdims=True)
    norm = jnp.sum(jnp.sum(total[segs:], axis=1, keepdims=True), axis=0, keepdims=True)
    own = lax.broadcasted_iota(jnp.int32, (segs, LANES), 0) == lax.broadcasted_iota(jnp.int32, (segs, LANES), 1)
    est_ref[...] = jnp.sum(jnp.where(own, number / jnp.sqrt(norm), 0.0), axis=0, keepdims=True)
    for d in range(n_bin - 1):
        e_copy(d).wait_send()


def store_kernel(cr_ref, ci_ref, est_ref, cr_hbm, ci_hbm, est_out, sems):
    copies = [pltpu.make_async_copy(cr_ref, cr_hbm, sems.at[0]), pltpu.make_async_copy(ci_ref, ci_hbm, sems.at[1])]
    for copy in copies:
        copy.start()
    est_out[...] = est_ref[0, : est_out.shape[0]]
    for copy in copies:
        copy.wait()


def line_on_device(n_seg, n_bin, magnet_real, magnet_imag, detector_real, detector_imag, valid, intersection):
    segs, channels, bins = magnet_real.shape
    detectors = detector_real.shape[1]
    blocks = bins // LANES
    nblk = blocks // n_seg
    rows = (channels + 2 * detectors) * channels
    wrows = 2 * channels * detectors
    f32 = jnp.float32
    pieces, modes, order = schedule(nblk)
    steps = Planner(pieces, modes, order, DEPTH, rows, wrows).plan()
    sizes = (n_seg, n_bin, segs, channels, detectors, nblk, pieces, modes, steps)
    count = len(pieces)
    vmem = pl.BlockSpec(memory_space=pltpu.VMEM)
    hbm = pl.BlockSpec(memory_space=pltpu.HBM)
    scratch = [pltpu.VMEM((LINE, 2, rows * n, LANES), f32) for n, _ in pieces]
    scratch += [pltpu.VMEM((LINE if form == "A" else 1, rows * n, LANES), f32) for n, form in pieces]
    scratch += [pltpu.VMEM((LINE,) + (() if form == "A" else (2,)) + (rows * n, LANES), f32) for n, form in pieces]
    scratch += [pltpu.VMEM((LINE, 2, wrows * n, LANES), f32) for n, _ in pieces]
    scratch += [pltpu.VMEM(a.shape, a.dtype) for a in (magnet_real, magnet_imag, detector_real, detector_imag)]
    scratch += [
        pltpu.SMEM((segs,), jnp.int32),
        pltpu.VMEM((blocks, LANES), f32),
        pltpu.VMEM((blocks, segs * channels, LANES), f32),
        pltpu.VMEM((blocks, segs * channels, LANES), f32),
        pltpu.VMEM((blocks, segs * detectors, LANES), f32),
        pltpu.VMEM((blocks, segs * detectors, LANES), f32),
        pltpu.VMEM((2 * segs, LANES), f32),
        pltpu.VMEM((n_bin - 1, 2 * segs, LANES), f32),
    ]
    dma = pltpu.SemaphoreType.DMA
    scratch += [dma((count, LINE))] * 4 + [dma((count, 9)), dma((count, LINE, 2))]
    scratch += [dma((n_bin - 1,))] * 2 + [dma((2 * LINE, 4)), dma((2,))]
    operands = [magnet_real, magnet_imag, detector_real, detector_imag, valid, intersection.reshape(blocks, LANES)]
    cleaned_real, cleaned_imag, estimate = pl.pallas_call(
        functools.partial(line_kernel, sizes),
        out_shape=(
            pltpu.VMEM((segs, bins), f32),
            pltpu.VMEM((segs, bins), f32),
            pltpu.VMEM((1, LANES), f32),
        ),
        in_specs=[hbm] * 6,
        out_specs=(vmem, vmem, vmem),
        scratch_shapes=scratch,
        compiler_params=pltpu.CompilerParams(
            collective_id=0, has_side_effects=True, vmem_limit_bytes=GRANT
        ),
    )(*[pltpu.with_memory_space_constraint(a, pltpu.HBM) for a in operands])
    return pl.pallas_call(
        store_kernel,
        out_shape=(
            jax.ShapeDtypeStruct((segs, bins), f32),
            jax.ShapeDtypeStruct((segs, bins), f32),
            jax.ShapeDtypeStruct((segs,), f32),
        ),
        in_specs=[vmem] * 3,
        out_specs=(hbm, hbm, vmem),
        scratch_shapes=[dma((2,))],
        compiler_params=pltpu.CompilerParams(vmem_limit_bytes=4 * 1024 * 1024),
    )(cleaned_real, cleaned_imag, estimate)


def solution(mesh):
    placed = (
        P("seg", None, "bin"),
        P("seg", None, "bin"),
        P("seg", None, "bin"),
        P("seg", None, "bin"),
        P("seg"),
        P("bin"),
    )
    n_seg, n_bin = mesh.shape["seg"], mesh.shape["bin"]
    on_device = line_on_device if n_seg == 2 * LINE else halving_on_device
    return jax.shard_map(
        functools.partial(on_device, n_seg, n_bin),
        mesh=mesh,
        in_specs=placed,
        out_specs=(P("seg", "bin"), P("seg", "bin"), P("seg")),
        check_vma=False,
    )
```

```python
import functools
import heapq

import jax
import jax.numpy as jnp
from jax import lax
from jax.experimental import pallas as pl
from jax.experimental.pallas import tpu as pltpu
from jax.sharding import PartitionSpec as P

LANES = 128
MESH = pl.DeviceIdType.MESH
RS_WEIGHTS = [1.0, 1.0, 1.5]


def largest_divisor(value, limit):
    return max(d for d in range(1, limit + 1) if value % d == 0)


def cadd_mul_conj(acc, a, b):
    return (acc[0] - a[0] * b[0] - a[1] * b[1], acc[1] - a[1] * b[0] + a[0] * b[1])


def csub_mul(acc, a, b):
    return (acc[0] - a[0] * b[0] + a[1] * b[1], acc[1] - a[0] * b[1] - a[1] * b[0])


def csub_conj_mul(acc, a, b):
    return (acc[0] - a[0] * b[0] - a[1] * b[1], acc[1] - a[0] * b[1] + a[1] * b[0])


def wiener_solve(below, diag, right):
    channels = len(diag)
    detectors = len(right[0])
    diag = list(diag)
    inverse = [None] * channels
    low = [[None] * channels for _ in range(channels)]
    for j in range(channels):
        inverse[j] = 1.0 / diag[j]
        for i in range(j + 1, channels):
            low[i][j] = (below[i][j][0] * inverse[j], below[i][j][1] * inverse[j])
        for i in range(j + 1, channels):
            a, l = below[i][j], low[i][j]
            diag[i] = diag[i] - l[0] * a[0] - l[1] * a[1]
            for k in range(j + 1, i):
                below[i][k] = cadd_mul_conj(below[i][k], l, below[k][j])
    out = []
    for det in range(detectors):
        y = []
        for i in range(channels):
            run = right[i][det]
            for k in range(i):
                run = csub_mul(run, low[i][k], y[k])
            y.append(run)
        w = [None] * channels
        for i in reversed(range(channels)):
            run = (y[i][0] * inverse[i], y[i][1] * inverse[i])
            for k in range(i + 1, channels):
                run = csub_conj_mul(run, low[k][i], w[k])
            w[i] = run
        out.append(w)
    return out


def step_weights(stages):
    return RS_WEIGHTS if stages == len(RS_WEIGHTS) else [1.0] * stages


def flood_order(n, stages, parts, weights, gather):
    free = [0.0] * stages
    heap, order, count = [], [], {}

    def send(now, st, q, k):
        free[st] = max(now, free[st]) + weights[st]
        heapq.heappush(heap, (free[st] + 0.6, st, q, k))

    if gather:
        for k in range(parts):
            for st in range(stages):
                send(0.0, st, 0, k)
    else:
        for q in first_order(n, stages):
            for k in range(parts):
                send(0.0, 0, q, k)
    while heap:
        now, st, q, k = heapq.heappop(heap)
        order.append((st, q, k))
        bit = n >> (st + 1)
        if gather:
            for to in range(st):
                send(now, to, q + bit, k)
        else:
            d = q - bit
            count[d, k] = count.get((d, k), 0) + 1
            if d and count[d, k] == stages - d.bit_length():
                send(now, stages - d.bit_length(), d, k)
    return order


def first_order(n, stages):
    def key(q):
        return [q >> bit & 1 for bit in range(stages)]

    return sorted(range(n // 2, n), key=key, reverse=True)


def halving_kernel(
    sizes, mr_ref, mi_ref, hr_ref, hi_ref, valid_ref, inter_ref,
    cr_ref, ci_ref, est_ref,
    s_ref, recv_ref, w_ref, mfr_ref, mfi_ref, hfr_ref, hfi_ref, ebuf_ref, erecv_ref,
    rs_send, rs_recv, ag_send, ag_recv, e_send, e_recv,
):
    n_seg, n_bin, segs, channels, detectors, blocks, chunks, wchunks = sizes
    stages = n_seg.bit_length() - 1
    half = channels // 2
    nblk = blocks // n_seg
    groups = channels + 2 * detectors
    per = groups // chunks
    wrows = 2 * channels * detectors
    wper = wrows // wchunks

    me = lax.axis_index("seg")
    my_bin = lax.axis_index("bin")
    bits = [lax.rem(lax.div(me, 1 << st), 2) for st in range(stages)]
    partner = [me + (1 - 2 * bits[st]) * (1 << st) for st in range(stages)]
    peers = [lax.rem(my_bin + d, n_bin) for d in range(1, n_bin)]

    barrier = pltpu.get_barrier_semaphore()
    for st in range(stages):
        pl.semaphore_signal(barrier, inc=1, device_id=(partner[st], my_bin), device_id_type=MESH)
    for peer in peers:
        pl.semaphore_signal(barrier, inc=1, device_id=(me, peer), device_id_type=MESH)

    def position(q):
        pos = 0
        for st in range(stages):
            digit = lax.rem(lax.div(q, n_seg >> (st + 1)), 2)
            pos = pos + (bits[st] + digit - 2 * bits[st] * digit) * (n_seg >> (st + 1))
        return pos

    sub = lax.broadcasted_iota(jnp.int32, (channels, LANES), 0)

    def spectra(q):
        pos = position(q)

        def body(blk, carry):
            b = pos * nblk + blk
            lanes = pl.ds(pl.multiple_of(b * LANES, LANES), LANES)
            acc = None
            for s in range(segs):
                mr = mr_ref[s, :, lanes].astype(jnp.float32)
                mi = mi_ref[s, :, lanes].astype(jnp.float32)
                hr = hr_ref[s, :, lanes].astype(jnp.float32)
                hi = hi_ref[s, :, lanes].astype(jnp.float32)
                mfr_ref[b, pl.ds(s * channels, channels), :] = mr
                mfi_ref[b, pl.ds(s * channels, channels), :] = mi
                hfr_ref[b, pl.ds(s * detectors, detectors), :] = hr
                hfi_ref[b, pl.ds(s * detectors, detectors), :] = hi
                v = valid_ref[s].astype(jnp.float32)
                kr, ki = mr * v, mi * v
                terms = [kr * mr + ki * mi]
                for r in range(1, half + 1):
                    br = pltpu.roll(mr, channels - r, 0)
                    bi = pltpu.roll(mi, channels - r, 0)
                    terms.append(kr * br + ki * bi)
                    terms.append(ki * br - kr * bi)
                for k in range(detectors):
                    br = jnp.broadcast_to(hr[k : k + 1], (channels, LANES))
                    bi = jnp.broadcast_to(hi[k : k + 1], (channels, LANES))
                    terms.append(kr * br + ki * bi)
                    terms.append(ki * br - kr * bi)
                acc = terms if acc is None else [a + t for a, t in zip(acc, terms)]
            packed = jnp.where(sub < half, acc[channels - 1], acc[channels])
            rows = acc[: channels - 1] + [packed] + acc[channels + 1 :]
            for g in range(groups):
                at = pl.multiple_of((g % per) * nblk * channels + blk * channels, channels)
                s_ref[q, g // per, pl.ds(at, channels), :] = rows[g]
            return carry

        lax.fori_loop(0, nblk, body, 0)

    def rs_copy(st, q, k):
        return pltpu.make_async_remote_copy(
            src_ref=s_ref.at[q, k],
            dst_ref=recv_ref.at[q - 1, k],
            send_sem=rs_send.at[q - 1, k],
            recv_sem=rs_recv.at[q - 1, k],
            device_id=(partner[st], my_bin),
            device_id_type=MESH,
        )

    first = first_order(n_seg, stages)
    assert first[0] == n_seg - 1
    spectra(first[0])
    pl.semaphore_wait(barrier, stages + n_bin - 1)
    for k in range(chunks):
        rs_copy(0, first[0], k).start()

    def mirrored(i, low):
        q = 0 if low else n_seg // 2
        for bit in range(stages - 1):
            digit = 1 - lax.rem(lax.div(i, n_seg >> (bit + 2)), 2)
            q = q + digit * (1 << bit)
        return q

    def early(i, carry):
        q = mirrored(i, False)
        spectra(q)
        for k in range(chunks):
            rs_copy(0, q, k).start()
        return carry

    lax.fori_loop(1, n_seg // 2, early, 0)

    def late(i, carry):
        spectra(mirrored(i, True))
        return carry

    lax.fori_loop(0, n_seg // 2, late, 0)

    got = {}
    for st, q, k in flood_order(n_seg, stages, chunks, step_weights(stages), False):
        rs_copy(st, q, k).wait_recv()
        d = q - (n_seg >> (st + 1))
        s_ref[d, k] = s_ref[d, k] + recv_ref[q - 1, k]
        got[d, k] = got.get((d, k), 0) + 1
        if d and got[d, k] == stages - d.bit_length():
            rs_copy(stages - d.bit_length(), d, k).start()

    def entry(g, row):
        start = (g % per) * nblk * channels + row
        if nblk == 1:
            return s_ref[0, g // per, pl.ds(start, 1), :]
        return s_ref[0, g // per, pl.ds(start, nblk, stride=channels), :]

    def above(a, b):
        r = b - a
        if r < half:
            return (entry(2 * r - 1, a), entry(2 * r, a))
        if r == half:
            return (entry(channels - 1, a), -entry(channels - 1, a + half))
        r = channels - r
        return (entry(2 * r - 1, b), -entry(2 * r, b))

    below = [[None] * channels for _ in range(channels)]
    for i in range(channels):
        for j in range(i):
            value = above(j, i)
            below[i][j] = (value[0], -value[1])
    diag = [entry(0, c) + 1.0 for c in range(channels)]
    right = [
        [(entry(channels + 2 * k, c), entry(channels + 2 * k + 1, c)) for k in range(detectors)]
        for c in range(channels)
    ]
    filt = wiener_solve(below, diag, right)
    for k in range(detectors):
        for c in range(channels):
            for part in range(2):
                e = (k * channels + c) * 2 + part
                w_ref[0, e // wper, pl.ds((e % wper) * nblk, nblk), :] = filt[k][c][part]

    def ag_copy(st, q, k):
        to = q + (n_seg >> (st + 1))
        return pltpu.make_async_remote_copy(
            src_ref=w_ref.at[q, k],
            dst_ref=w_ref.at[to, k],
            send_sem=ag_send.at[to - 1, k],
            recv_sem=ag_recv.at[to - 1, k],
            device_id=(partner[st], my_bin),
            device_id_type=MESH,
        )

    def clean(q, carry):
        pos = position(q)

        def body(blk, carry):
            num, sq = carry
            b = pos * nblk + blk
            lanes = pl.ds(pl.multiple_of(b * LANES, LANES), LANES)
            g = [
                (
                    hfr_ref[b, pl.ds(k, segs, stride=detectors), :],
                    hfi_ref[b, pl.ds(k, segs, stride=detectors), :],
                )
                for k in range(detectors)
            ]
            for c in range(channels):
                m = (
                    mfr_ref[b, pl.ds(c, segs, stride=channels), :],
                    mfi_ref[b, pl.ds(c, segs, stride=channels), :],
                )
                for k in range(detectors):
                    e = (k * channels + c) * 2
                    w = [
                        w_ref[q, f // wper, pl.ds((f % wper) * nblk + blk, 1), :]
                        for f in (e, e + 1)
                    ]
                    g[k] = csub_conj_mul(g[k], w, m)
            real = g[0][0] * g[1][0] + g[0][1] * g[1][1]
            imag = g[0][1] * g[1][0] - g[0][0] * g[1][1]
            cr_ref[:, lanes] = real
            ci_ref[:, lanes] = imag
            weight = inter_ref[pl.ds(b, 1), :]
            return num + real * weight, sq + weight * weight

        return lax.fori_loop(0, nblk, body, carry)

    for k in range(wchunks):
        for st in range(stages):
            ag_copy(st, 0, k).start()
    sums = clean(0, (jnp.zeros((segs, LANES), jnp.float32), jnp.zeros((1, LANES), jnp.float32)))
    seen = {}
    for st, q, k in flood_order(n_seg, stages, wchunks, step_weights(stages), True):
        ag_copy(st, q, k).wait_recv()
        to = q + (n_seg >> (st + 1))
        for on in range(st):
            ag_copy(on, to, k).start()
        seen[to] = seen.get(to, 0) + 1
        if seen[to] == wchunks:
            sums = clean(to, sums)
    num, sq = sums
    ebuf_ref[pl.ds(0, segs), :] = num
    ebuf_ref[pl.ds(segs, segs), :] = jnp.broadcast_to(sq, (segs, LANES))

    def e_copy(d):
        return pltpu.make_async_remote_copy(
            src_ref=ebuf_ref,
            dst_ref=erecv_ref.at[d],
            send_sem=e_send.at[d],
            recv_sem=e_recv.at[d],
            device_id=(me, peers[d]),
            device_id_type=MESH,
        )

    for d in range(n_bin - 1):
        e_copy(d).start()
    for q in range(1, n_seg):
        st = stages - q.bit_length()
        for k in range(chunks):
            rs_copy(st, q, k).wait_send()
        for k in range(wchunks):
            ag_copy(st, q - (n_seg >> (st + 1)), k).wait_send()
    total = ebuf_ref[...]
    for d in range(n_bin - 1):
        e_copy(d).wait_recv()
        total = total + erecv_ref[d]
    total = jnp.sum(total, axis=1, keepdims=True)
    est_ref[...] = jnp.broadcast_to(total[:segs] / jnp.sqrt(total[segs:]), (segs, LANES))
    for d in range(n_bin - 1):
        e_copy(d).wait_send()


def halving_on_device(n_seg, n_bin, magnet_real, magnet_imag, detector_real, detector_imag, valid, intersection):
    segs, channels, bins = magnet_real.shape
    detectors = detector_real.shape[1]
    blocks = bins // LANES
    nblk = blocks // n_seg
    groups = channels + 2 * detectors
    chunks = largest_divisor(groups, 4)
    wrows = 2 * channels * detectors
    wchunks = largest_divisor(wrows, 2)
    rows = groups // chunks * nblk * channels
    f32 = jnp.float32
    sizes = (n_seg, n_bin, segs, channels, detectors, blocks, chunks, wchunks)
    vmem = pl.BlockSpec(memory_space=pltpu.VMEM)
    cleaned_real, cleaned_imag, estimate = pl.pallas_call(
        functools.partial(halving_kernel, sizes),
        out_shape=(
            jax.ShapeDtypeStruct((segs, bins), f32),
            jax.ShapeDtypeStruct((segs, bins), f32),
            jax.ShapeDtypeStruct((segs, LANES), f32),
        ),
        in_specs=[vmem] * 4 + [pl.BlockSpec(memory_space=pltpu.SMEM), vmem],
        out_specs=(vmem, vmem, vmem),
        scratch_shapes=[
            pltpu.VMEM((n_seg, chunks, rows, LANES), f32),
            pltpu.VMEM((n_seg - 1, chunks, rows, LANES), f32),
            pltpu.VMEM((n_seg, wchunks, wrows // wchunks * nblk, LANES), f32),
            pltpu.VMEM((blocks, segs * channels, LANES), f32),
            pltpu.VMEM((blocks, segs * channels, LANES), f32),
            pltpu.VMEM((blocks, segs * detectors, LANES), f32),
            pltpu.VMEM((blocks, segs * detectors, LANES), f32),
            pltpu.VMEM((2 * segs, LANES), f32),
            pltpu.VMEM((n_bin - 1, 2 * segs, LANES), f32),
        ]
        + [
            pltpu.SemaphoreType.DMA((n_seg - 1, chunks)),
            pltpu.SemaphoreType.DMA((n_seg - 1, chunks)),
            pltpu.SemaphoreType.DMA((n_seg - 1, wchunks)),
            pltpu.SemaphoreType.DMA((n_seg - 1, wchunks)),
            pltpu.SemaphoreType.DMA((n_bin - 1,)),
            pltpu.SemaphoreType.DMA((n_bin - 1,)),
        ],
        compiler_params=pltpu.CompilerParams(
            collective_id=0, has_side_effects=True, vmem_limit_bytes=56 * 1024 * 1024
        ),
    )(
        magnet_real, magnet_imag, detector_real, detector_imag, valid,
        intersection.reshape(blocks, LANES),
    )
    return cleaned_real, cleaned_imag, estimate[:, 0]


LINE = 4
DEPTH = 4
GRANT = 24 * 1024 * 1024
ROW_US = 0.01128
HOP_US = (0.0, 2.3, 2.7, 3.1, 3.5)
STEP_US = 0.08
WORK = 0.7
GROUP_SETS = ((0, 1), (2, 3))


TUNED = {
    8: (
        (3, 2, 2, 1),
        "Y2ZY",
        ((0, 0), (2, 1), (0, 1), (2, 0), (1, 0), (0, 2), (3, 3), (1, 1), (0, 3), (2, 2), (1, 2), (2, 3), (1, 3)),
    ),
}


def schedule(nblk):
    if nblk in TUNED:
        sizes, modes, order = TUNED[nblk]
        pieces = [(n, "A") for n in sizes[:-1]] + [(sizes[-1], "B")]
        return pieces, modes, list(order)
    pieces = [(n, "A") for n in [1] * (nblk - 1)] + [(1, "B")] if nblk > 1 else [(nblk, "A")]
    return pieces, "Y" * len(pieces), tick_order(pieces)


def tick_order(pieces):
    first = [p for p, (_, kind) in enumerate(pieces) if kind == "A"]
    order = [(first[0], 0), (first[0], 1)]
    for p, nxt in zip(first, first[1:] + [None]):
        if nxt is not None:
            order += [(nxt, 0), (nxt, 1)]
        order += [(p, 2), (p, 3)]
    return order + [(p, 3) for p, (_, kind) in enumerate(pieces) if kind == "B"]


class Planner:
    def __init__(self, pieces, modes, order, depth, rows, wrows):
        self.pieces, self.modes, self.order, self.depth = pieces, modes, order, depth
        self.rows, self.wrows = rows, wrows
        self.clock = [2.0, 2.0]
        self.link, self.message, self.steps = {}, {}, []

    def send(self, role, key, path, rows):
        start = self.clock[role]
        for name in path:
            start = max(start, self.link.get(name, 0.0))
            self.link[name] = start + rows * ROW_US
        self.message[key] = start + rows * ROW_US + HOP_US[len(path)]

    def waits(self, op):
        kind, p = op[0], op[1]
        if kind == "XR":
            return [[("x", 0, p, op[2])], [("x", 1, p, op[2])]]
        if kind == "ZI":
            return [[], [("z", 1, p, op[2])]]
        if kind == "FIN":
            return [[("z", 0, p, 0), ("z", 0, p, 1)], [("z", 1, p, 2), ("z", 1, p, 3)]]
        if kind == "AGX":
            return [[("ax", 0, p)], [("ax", 1, p)]]
        if kind == "RL":
            return [[], [("a", 1, p, op[2], 0)]]
        if kind == "AG":
            both = [[("a", r, p, op[2], op[3])] for r in range(2)]
            if self.modes[p] in "CY" and op[3] == 0:
                both[1] = []
            return both
        return [[], []]

    def column(self, p, side, rows, chain):
        self.send(0, ("a", 1, p, 2, side), ["in"], rows)
        self.send(1, ("a", 0, p, 2, side), ["out"], rows)
        self.send(1, ("a", 1, p, 1, side), ["mid"], rows)
        if not chain:
            self.send(0, ("a", 1, p, 0, side), ["in", "mid"], rows)
            self.send(1, ("a", 0, p, 1, side), ["mid", "out"], rows)
            self.send(0, ("a", 0, p, 0, side), ["in", "mid", "out"], rows)

    def diagonal(self, p, rows):
        self.send(0, ("a", 1, p, 2, 1), [("x", 0), "in"], rows)
        self.send(1, ("a", 0, p, 2, 1), [("x", 1), "out"], rows)
        self.send(1, ("a", 1, p, 1, 1), [("x", 1), "mid"], rows)
        self.send(0, ("a", 1, p, 0, 1), [("x", 0), "in", "mid"], rows)
        self.send(1, ("a", 0, p, 1, 1), [("x", 1), "mid", "out"], rows)
        self.send(0, ("a", 0, p, 0, 1), [("x", 0), "in", "mid", "out"], rows)

    def lines(self, p, r, rows):
        if r < 3:
            self.send(0, ("z", 1, p, r), ["in"], rows)
        if r == 2:
            self.send(1, ("z", 0, p, 0), ["out"], rows)

    def run(self, op):
        for role, keys in enumerate(self.waits(op)):
            self.clock[role] = max([self.clock[role]] + [self.message[key] for key in keys]) + STEP_US
        kind, p = op[0], op[1]
        size, form = self.pieces[p]
        rows, wrows, mode = self.rows * size, self.wrows * size, self.modes[p]
        work = 0.0
        if kind == "SP":
            work = 0.13 * size * len(op[3]) * len(op[2])
        elif kind == "XS":
            for role in range(2):
                self.send(role, ("x", role, p, op[2]), [("x", role)], rows)
        elif kind == "XR":
            work = 0.03 * size
        elif kind == "FIN":
            work = 0.06 * size
        elif kind == "SOLVE":
            work = 0.6 + 0.06 * size
        elif kind in ("AGX", "AG"):
            work = 0.06 * size * (2 if kind == "AG" and mode == "C" else 1)
        work = work * WORK
        self.clock = [c + (0.0 if kind in ("SOLVE", "AGX", "AG") else work) for c in self.clock]
        if kind == "XR" and form == "A":
            self.lines(p, op[2], rows)
        elif kind == "ZS":
            self.lines(p, op[2], rows * 2)
        elif kind == "ZI":
            both = rows * (2 if form == "B" else 1)
            if op[2] == 1:
                self.send(1, ("z", 1, p, 3), ["mid"], both)
            else:
                self.send(1, ("z", 0, p, 1), ["mid", "out"], both)
        elif kind == "SOLVE":
            self.clock = [c + 0.6 * WORK for c in self.clock]
            for role in range(2):
                self.send(role, ("ax", role, p), [("x", role)], wrows)
            if mode in "2DYZ":
                self.column(p, 0, wrows, mode == "Y")
            if mode == "D":
                self.diagonal(p, wrows)
            work = work - 0.6 * WORK
        elif kind == "AGX":
            if mode in "2C":
                self.column(p, 0 if mode == "C" else 1, wrows * (2 if mode == "C" else 1), mode == "C")
        elif kind == "RL":
            both = wrows * (2 if mode == "C" else 1)
            if op[2] == 2:
                self.send(1, ("a", 1, p, 0, 0), ["mid"], both)
            else:
                self.send(1, ("a", 0, p, op[2], 0), ["out"], both)
        elif kind == "AG" and mode in "YZ" and op[3] == 0:
            for role in range(2):
                self.send(role, ("a", role, p, op[2], 1), [("x", role)], wrows)
        if kind in ("SOLVE", "AGX", "AG"):
            self.clock = [c + work for c in self.clock]
        self.steps.append(op)

    def spectra_steps(self):
        lead = self.order[0]
        for p, (_, form) in enumerate(self.pieces):
            for group in GROUP_SETS:
                if (p, group[0]) == lead:
                    yield ("SP", p, (group[0],), (1,))
                    yield ("SP", p, (group[0],), (0,))
                    yield ("SP", p, group[1:], (1, 0))
                else:
                    yield ("SP", p, group, (1, 0))

    def needs(self):
        need, order = {}, self.order
        made = {}
        for op in self.spectra_steps():
            need[op] = []
            for r in op[2]:
                for side in op[3]:
                    made[op[1], r, side] = op
        for i, (p, r) in enumerate(order):
            back = [("XR",) + order[i - self.depth]] if i >= self.depth else []
            back += [("XS",) + order[i - 1]] if i else []
            chain = [("XR",) + order[i - 1]] if i else []
            if self.pieces[p][1] == "A":
                need["XS", p, r] = [made[p, r, 1]] + back
                need["XR", p, r] = [("XS", p, r), made[p, r, 0]] + chain
            else:
                need["XS", p, r] = [("FIN", p)] + back
                need["XR", p, r] = [("XS", p, r)] + chain
        for p, (_, form) in enumerate(self.pieces):
            kind = "XR" if form == "A" else "ZS"
            if form == "B":
                for r in range(3):
                    need["ZS", p, r] = [made[p, r, 0], made[p, r, 1]]
            for r in range(2):
                need["ZI", p, r] = [(kind, p, r)]
            need["FIN", p] = [("ZI", p, 0), ("ZI", p, 1), (kind, p, 2)]
            need["FIN", p] += [("XR", p, 3)] if form == "A" else [made[p, 3, 0], made[p, 3, 1]]
            need["SOLVE", p] = [("FIN", p) if form == "A" else ("XR", p, 3)]
            need["AGX", p] = [("SOLVE", p)]
            mode = self.modes[p]
            start = ("AGX", p) if mode == "C" else ("SOLVE", p)
            for slot in (2, 1, 0):
                if mode in "CY":
                    need["RL", p, slot] = [start]
                    need["AG", p, slot, 0] = [("RL", p, slot)]
                else:
                    need["AG", p, slot, 0] = [start]
                if mode in "YZ":
                    need["AG", p, slot, 1] = [("AG", p, slot, 0)]
                elif mode in "2D":
                    need["AG", p, slot, 1] = [("AGX", p) if mode == "2" else start]
        return need

    def plan(self):
        need = self.needs()
        place = {op: i for i, op in enumerate(need)}
        tick = {key: i for i, key in enumerate(self.order)}
        done = set()
        while len(done) < len(need):
            best = None
            for op in need:
                if op in done or any(other not in done for other in need[op]):
                    continue
                keys = self.waits(op)
                if any(key not in self.message for role in range(2) for key in keys[role]):
                    continue
                ready = max(max([self.clock[r]] + [self.message[key] for key in keys[r]]) for r in range(2))
                now = max(self.clock)
                urgent = -1.0
                if op[0] in ("SP", "ZS") and ready <= now + 1e-6:
                    form = self.pieces[op[1]][1]
                    r = op[2] if op[0] == "ZS" else op[2][0]
                    urgent = 2.5 + 0.1 * r if form == "B" else tick[op[1], r]
                key = (round(max(ready, now), 3), urgent, place[op])
                if best is None or key < best[0]:
                    best = (key, op)
            self.run(best[1])
            done.add(best[1])
        return self.steps


def line_kernel(sizes, mr_hbm, mi_hbm, hr_hbm, hi_hbm, valid_hbm, inter_hbm, cr_ref, ci_ref, est_ref, *scratch):
    n_seg, n_bin, segs, channels, detectors, nblk, pieces, modes, steps = sizes
    count = len(pieces)
    half = channels // 2
    groups = channels + 2 * detectors
    rows = groups * channels
    wrows = 2 * channels * detectors
    scratch = list(scratch)
    take = lambda n: [scratch.pop(0) for _ in range(n)]
    s_refs, x_refs, z_refs, w_refs = take(count), take(count), take(count), take(count)
    mr_ref, mi_ref, hr_ref, hi_ref, valid_ref, inter_ref = take(6)
    mfr_ref, mfi_ref, hfr_ref, hfi_ref, ebuf_ref, erecv_ref = take(6)
    x_send, x_recv, z_send, z_recv, a_send, a_recv, e_send, e_recv, in_sem, small_sem = take(10)

    me = lax.axis_index("seg")
    my_bin = lax.axis_index("bin")
    x = lax.rem(me, 2)
    z = lax.div(me, 2)
    z_hi, z_lo = lax.div(z, 2), lax.rem(z, 2)
    mid = z_hi + z_lo - 2 * z_hi * z_lo
    is_mid, is_end = mid == 1, mid == 0
    sib = 2 * z_hi + 1 - z_lo
    far_mid = 2 - z_hi
    far_end = 3 - 3 * z_hi
    line = {3: z, 2: sib, 1: far_mid, 0: far_end}
    partner = (2 * z + 1 - x, my_bin)
    peers = [lax.rem(my_bin + d, n_bin) for d in range(1, n_bin)]

    def column(where):
        return (2 * line[where] + x, my_bin)

    def lanes_of(r, side):
        return 2 * line[r] + x + side - 2 * side * x

    barrier = pltpu.get_barrier_semaphore()
    for d in range(1, n_seg):
        pl.semaphore_signal(barrier, inc=1, device_id=(lax.rem(me + d, n_seg), my_bin), device_id_type=MESH)
    for peer in peers:
        pl.semaphore_signal(barrier, inc=1, device_id=(me, peer), device_id_type=MESH)

    small = [
        pltpu.make_async_copy(valid_hbm, valid_ref, small_sem.at[0]),
        pltpu.make_async_copy(inter_hbm, inter_ref, small_sem.at[1]),
    ]
    small[0].start()
    loads = {}
    for i, (r, side) in enumerate([(0, 1), (0, 0), (1, None), (2, None), (3, None)]):
        first = lanes_of(r, side) if side is not None else 2 * line[r]
        width = (1 if side is not None else 2) * nblk * LANES
        lanes = pl.ds(pl.multiple_of(first * nblk * LANES, nblk * LANES), width)
        loads[r, side] = [
            pltpu.make_async_copy(src.at[:, :, lanes], dst.at[:, :, lanes], in_sem.at[i, j])
            for j, (src, dst) in enumerate(
                [(mr_hbm, mr_ref), (mi_hbm, mi_ref), (hr_hbm, hr_ref), (hi_hbm, hi_ref)]
            )
        ]
        for copy in loads[r, side]:
            copy.start()
    small[1].start()
    small[0].wait()

    first_block = [sum(size for size, _ in pieces[:p]) for p in range(count)]
    sub = lax.broadcasted_iota(jnp.int32, (channels, LANES), 0)
    loaded = set()

    def spectra(p, where, sides):
        size = pieces[p][0]
        for r in where:
            for side in sides:
                key = (r, side) if r == 0 else (r, None)
                if key not in loaded:
                    loaded.add(key)
                    for copy in loads[key]:
                        copy.wait()

        def body(i, carry):
            r = where[0] + lax.div(i, size * len(sides))
            side = sides[0] if len(sides) == 1 else 1 - lax.rem(lax.div(i, size), 2)
            blk = lax.rem(i, size)
            if len(where) == 1:
                at = line[where[0]]
            else:
                at = line[where[0]] + (r - where[0]) * (line[where[1]] - line[where[0]])
            owner = 2 * at + x + side - 2 * side * x
            b = owner * nblk + first_block[p] + blk
            lanes = pl.ds(pl.multiple_of(b * LANES, LANES), LANES)
            acc = None
            for s in range(segs):
                mr = mr_ref[s, :, lanes].astype(jnp.float32)
                mi = mi_ref[s, :, lanes].astype(jnp.float32)
                hr = hr_ref[s, :, lanes].astype(jnp.float32)
                hi = hi_ref[s, :, lanes].astype(jnp.float32)
                mfr_ref[b, pl.ds(s * channels, channels), :] = mr
                mfi_ref[b, pl.ds(s * channels, channels), :] = mi
                hfr_ref[b, pl.ds(s * detectors, detectors), :] = hr
                hfi_ref[b, pl.ds(s * detectors, detectors), :] = hi
                v = valid_ref[s].astype(jnp.float32)
                kr, ki = mr * v, mi * v
                terms = [kr * mr + ki * mi]
                for turn in range(1, half + 1):
                    br = pltpu.roll(mr, channels - turn, 0)
                    bi = pltpu.roll(mi, channels - turn, 0)
                    terms.append(kr * br + ki * bi)
                    terms.append(ki * br - kr * bi)
                for k in range(detectors):
                    br = jnp.broadcast_to(hr[k : k + 1], (channels, LANES))
                    bi = jnp.broadcast_to(hi[k : k + 1], (channels, LANES))
                    terms.append(kr * br + ki * bi)
                    terms.append(ki * br - kr * bi)
                acc = terms if acc is None else [a + t for a, t in zip(acc, terms)]
            packed = jnp.where(sub < half, acc[channels - 1], acc[channels])
            out = acc[: channels - 1] + [packed] + acc[channels + 1 :]
            for g in range(groups):
                start = pl.multiple_of((g * size + blk) * channels, channels)
                s_refs[p][r, side, pl.ds(start, channels), :] = out[g]
            return carry

        lax.fori_loop(0, size * len(sides) * len(where), body, 0)

    def solve(p):
        size = pieces[p][0]
        ref = s_refs[p]

        def entry(g, row):
            start = g * size * channels + row
            if size == 1:
                return ref[3, 0, pl.ds(start, 1), :]
            return ref[3, 0, pl.ds(start, size, stride=channels), :]

        def above(a, b):
            r = b - a
            if r < half:
                return (entry(2 * r - 1, a), entry(2 * r, a))
            if r == half:
                return (entry(channels - 1, a), -entry(channels - 1, a + half))
            r = channels - r
            return (entry(2 * r - 1, b), -entry(2 * r, b))

        below = [[None] * channels for _ in range(channels)]
        for i in range(channels):
            for j in range(i):
                value = above(j, i)
                below[i][j] = (value[0], -value[1])
        diag = [entry(0, c) + 1.0 for c in range(channels)]
        right = [
            [(entry(channels + 2 * k, c), entry(channels + 2 * k + 1, c)) for k in range(detectors)]
            for c in range(channels)
        ]
        filt = wiener_solve(below, diag, right)
        for k in range(detectors):
            for c in range(channels):
                for part in range(2):
                    e = (k * channels + c) * 2 + part
                    w_refs[p][3, 0, pl.ds(e * size, size), :] = filt[k][c][part]

    def clean(p, r, sides):
        size = pieces[p][0]

        def body(i, carry):
            if len(sides) == 1:
                side, blk = sides[0], i
            else:
                side, blk = lax.div(i, size), lax.rem(i, size)
            b = lanes_of(r, side) * nblk + first_block[p] + blk
            lanes = pl.ds(pl.multiple_of(b * LANES, LANES), LANES)
            g = [
                (
                    hfr_ref[b, pl.ds(k, segs, stride=detectors), :],
                    hfi_ref[b, pl.ds(k, segs, stride=detectors), :],
                )
                for k in range(detectors)
            ]
            for c in range(channels):
                m = (
                    mfr_ref[b, pl.ds(c, segs, stride=channels), :],
                    mfi_ref[b, pl.ds(c, segs, stride=channels), :],
                )
                for k in range(detectors):
                    e = (k * channels + c) * 2
                    w = [w_refs[p][r, side, pl.ds(f * size + blk, 1), :] for f in (e, e + 1)]
                    g[k] = csub_conj_mul(g[k], w, m)
            real = g[0][0] * g[1][0] + g[0][1] * g[1][1]
            imag = g[0][1] * g[1][0] - g[0][0] * g[1][1]
            cr_ref[:, lanes] = real
            ci_ref[:, lanes] = imag
            ebuf_ref[pl.ds(0, segs), :] = ebuf_ref[pl.ds(0, segs), :] + real * inter_ref[pl.ds(b, 1), :]
            return carry

        if size * len(sides) == 1:
            body(0, 0)
        else:
            lax.fori_loop(0, size * len(sides), body, 0)

    started = []

    def remote(src, dst, send_sem, recv_sem, device):
        return pltpu.make_async_remote_copy(
            src_ref=src, dst_ref=dst, send_sem=send_sem, recv_sem=recv_sem,
            device_id=device, device_id_type=MESH,
        )

    def start(copy, when=None):
        started.append((when, copy))
        if when is None:
            copy.start()
        else:
            pl.when(when)(copy.start)

    def x_copy(p, r):
        src, dst = (s_refs[p].at[r, 1], x_refs[p].at[r]) if pieces[p][1] == "A" else (s_refs[p].at[3, 1], x_refs[p].at[0])
        return remote(src, dst, x_send.at[p, r], x_recv.at[p, r], partner)

    def part(p, r):
        return s_refs[p].at[r, 0] if pieces[p][1] == "A" else s_refs[p].at[r]

    def z_copy(p, r, slot, where):
        return remote(part(p, r), z_refs[p].at[slot], z_send.at[p, r], z_recv.at[p, slot], column(where))

    def send_in(p, r):
        if r < 3:
            start(z_copy(p, r, r, 2), is_end)
        if r == 2:
            start(z_copy(p, r, 0, 2), is_mid)

    def add(p, r, slot):
        ref = part(p, r)
        ref[...] = ref[...] + z_refs[p][slot]

    sends = [0] * count

    def a_copy(p, src, dst, slot_at, device):
        sends[p] += 1
        return remote(src, dst, a_send.at[p, sends[p] - 1], a_recv.at[p, slot_at[0], slot_at[1]], device)

    def a_wait(p, slot, side, both=False):
        ref = w_refs[p].at[slot] if both else w_refs[p].at[slot, side]
        remote(ref, ref, a_send.at[p, 0], a_recv.at[p, slot, side], partner).wait_recv()

    def spread(p, side, both, chain):
        src = w_refs[p].at[3] if both else w_refs[p].at[3, side]

        def to(slot, where, when=None):
            dst = w_refs[p].at[slot] if both else w_refs[p].at[slot, side]
            start(a_copy(p, src, dst, (slot, side), column(where)), when)

        to(2, 2)
        to(mid, 1, is_mid if chain else None)
        if not chain:
            to(mid, 0)

    def relay(p, slot):
        both = modes[p] == "C"
        pick = (lambda n: w_refs[p].at[n]) if both else (lambda n: w_refs[p].at[n, 0])
        to, where = (0, 1) if slot == 2 else (slot, 2)
        copy = a_copy(p, pick(slot), pick(to), (to, 0), column(where))
        started.append((is_mid, copy))

        @pl.when(is_mid)
        def _():
            a_wait(p, slot, 0, both)
            copy.start()

    ebuf_ref[pl.ds(0, segs), :] = jnp.zeros((segs, LANES), jnp.float32)
    entered = weighed = False
    for op in steps:
        kind, p = op[0], op[1]
        form, mode = pieces[p][1], modes[p]
        if kind == "SP":
            spectra(p, op[2], op[3])
            continue
        if not entered:
            pl.semaphore_wait(barrier, n_seg + n_bin - 2)
            entered = True
        if kind == "XS":
            start(x_copy(p, op[2]))
        elif kind == "XR":
            r = op[2]
            x_copy(p, r).wait_recv()
            if form == "A":
                s_refs[p][r, 0] = s_refs[p][r, 0] + x_refs[p][r]
                send_in(p, r)
            else:
                s_refs[p][3, 0] = s_refs[p][3, 0] + x_refs[p][0]
        elif kind == "ZS":
            send_in(p, op[2])
        elif kind == "ZI":
            r = op[2]
            copy = z_copy(p, r, 3, 1) if r == 1 else z_copy(p, r, 1, 0)
            started.append((is_mid, copy))

            @pl.when(is_mid)
            def _():
                z_copy(p, r, r, 2).wait_recv()
                add(p, r, r)
                copy.start()
        elif kind == "FIN":
            for when, slots in ((is_end, (0, 1)), (is_mid, (2, 3))):

                @pl.when(when)
                def _():
                    for slot in slots:
                        z_copy(p, 3, slot, 2).wait_recv()
                        add(p, 3, slot)
        elif kind == "SOLVE":
            solve(p)
            start(a_copy(p, w_refs[p].at[3, 0], w_refs[p].at[3, 1], (3, 1), partner))
            if mode in "2DYZ":
                spread(p, 0, False, mode == "Y")
            if mode == "D":
                for slot, where in ((2, 2), (mid, 1), (mid, 0)):
                    device = (2 * line[where] + 1 - x, my_bin)
                    start(a_copy(p, w_refs[p].at[3, 0], w_refs[p].at[slot, 1], (slot, 1), device))
            if not weighed:
                weighed = True
                small[1].wait()
                weight = inter_ref[...]
                weight = weight * weight
                total = weight[:segs]
                for i in range(1, weight.shape[0] // segs):
                    total = total + weight[i * segs : (i + 1) * segs]
                ebuf_ref[pl.ds(segs, segs), :] = total
            clean(p, 3, (0,))
        elif kind == "AGX":
            a_wait(p, 3, 1)
            if mode == "C":
                spread(p, 0, True, True)
            elif mode == "2":
                spread(p, 1, False, False)
            clean(p, 3, (1,))
        elif kind == "RL":
            relay(p, op[2])
        elif kind == "AG":
            slot, side = op[2], op[3]
            both = mode == "C"
            if mode in "CY" and side == 0:
                pl.when(is_end)(functools.partial(a_wait, p, slot, side, both))
            else:
                a_wait(p, slot, side)
            if mode in "YZ" and side == 0:
                start(a_copy(p, w_refs[p].at[slot, 0], w_refs[p].at[slot, 1], (slot, 1), partner))
            clean(p, slot, (0, 1) if both else (side,))

    def e_copy(d):
        return pltpu.make_async_remote_copy(
            src_ref=ebuf_ref,
            dst_ref=erecv_ref.at[d],
            send_sem=e_send.at[d],
            recv_sem=e_recv.at[d],
            device_id=(me, peers[d]),
            device_id_type=MESH,
        )

    for d in range(n_bin - 1):
        e_copy(d).start()
    for when, copy in started:
        if when is None:
            copy.wait_send()
    for when in (is_mid, is_end):

        @pl.when(when)
        def _():
            for other, copy in started:
                if other is when:
                    copy.wait_send()

    total = ebuf_ref[...]
    for d in range(n_bin - 1):
        e_copy(d).wait_recv()
        total = total + erecv_ref[d]
    number = jnp.sum(total[:segs], axis=1, keepdims=True)
    norm = jnp.sum(jnp.sum(total[segs:], axis=1, keepdims=True), axis=0, keepdims=True)
    own = lax.broadcasted_iota(jnp.int32, (segs, LANES), 0) == lax.broadcasted_iota(jnp.int32, (segs, LANES), 1)
    est_ref[...] = jnp.sum(jnp.where(own, number / jnp.sqrt(norm), 0.0), axis=0, keepdims=True)
    for d in range(n_bin - 1):
        e_copy(d).wait_send()


def store_kernel(cr_ref, ci_ref, est_ref, cr_hbm, ci_hbm, est_out, sems):
    copies = [pltpu.make_async_copy(cr_ref, cr_hbm, sems.at[0]), pltpu.make_async_copy(ci_ref, ci_hbm, sems.at[1])]
    for copy in copies:
        copy.start()
    est_out[...] = est_ref[0, : est_out.shape[0]]
    for copy in copies:
        copy.wait()


def line_on_device(n_seg, n_bin, magnet_real, magnet_imag, detector_real, detector_imag, valid, intersection):
    segs, channels, bins = magnet_real.shape
    detectors = detector_real.shape[1]
    blocks = bins // LANES
    nblk = blocks // n_seg
    rows = (channels + 2 * detectors) * channels
    wrows = 2 * channels * detectors
    f32 = jnp.float32
    pieces, modes, order = schedule(nblk)
    steps = Planner(pieces, modes, order, DEPTH, rows, wrows).plan()
    sizes = (n_seg, n_bin, segs, channels, detectors, nblk, pieces, modes, steps)
    count = len(pieces)
    vmem = pl.BlockSpec(memory_space=pltpu.VMEM)
    hbm = pl.BlockSpec(memory_space=pltpu.HBM)
    scratch = [pltpu.VMEM((LINE, 2, rows * n, LANES), f32) for n, _ in pieces]
    scratch += [pltpu.VMEM((LINE if form == "A" else 1, rows * n, LANES), f32) for n, form in pieces]
    scratch += [pltpu.VMEM((LINE,) + (() if form == "A" else (2,)) + (rows * n, LANES), f32) for n, form in pieces]
    scratch += [pltpu.VMEM((LINE, 2, wrows * n, LANES), f32) for n, _ in pieces]
    scratch += [pltpu.VMEM(a.shape, a.dtype) for a in (magnet_real, magnet_imag, detector_real, detector_imag)]
    scratch += [
        pltpu.SMEM((segs,), jnp.int32),
        pltpu.VMEM((blocks, LANES), f32),
        pltpu.VMEM((blocks, segs * channels, LANES), f32),
        pltpu.VMEM((blocks, segs * channels, LANES), f32),
        pltpu.VMEM((blocks, segs * detectors, LANES), f32),
        pltpu.VMEM((blocks, segs * detectors, LANES), f32),
        pltpu.VMEM((2 * segs, LANES), f32),
        pltpu.VMEM((n_bin - 1, 2 * segs, LANES), f32),
    ]
    dma = pltpu.SemaphoreType.DMA
    scratch += [dma((count, LINE))] * 4 + [dma((count, 9)), dma((count, LINE, 2))]
    scratch += [dma((n_bin - 1,))] * 2 + [dma((LINE + 1, 4)), dma((2,))]
    operands = [magnet_real, magnet_imag, detector_real, detector_imag, valid, intersection.reshape(blocks, LANES)]
    cleaned_real, cleaned_imag, estimate = pl.pallas_call(
        functools.partial(line_kernel, sizes),
        out_shape=(
            pltpu.VMEM((segs, bins), f32),
            pltpu.VMEM((segs, bins), f32),
            pltpu.VMEM((1, LANES), f32),
        ),
        in_specs=[hbm] * 6,
        out_specs=(vmem, vmem, vmem),
        scratch_shapes=scratch,
        compiler_params=pltpu.CompilerParams(
            collective_id=0, has_side_effects=True, vmem_limit_bytes=GRANT
        ),
    )(*[pltpu.with_memory_space_constraint(a, pltpu.HBM) for a in operands])
    return pl.pallas_call(
        store_kernel,
        out_shape=(
            jax.ShapeDtypeStruct((segs, bins), f32),
            jax.ShapeDtypeStruct((segs, bins), f32),
            jax.ShapeDtypeStruct((segs,), f32),
        ),
        in_specs=[vmem] * 3,
        out_specs=(hbm, hbm, vmem),
        scratch_shapes=[dma((2,))],
        compiler_params=pltpu.CompilerParams(vmem_limit_bytes=4 * 1024 * 1024),
    )(cleaned_real, cleaned_imag, estimate)


def solution(mesh):
    placed = (
        P("seg", None, "bin"),
        P("seg", None, "bin"),
        P("seg", None, "bin"),
        P("seg", None, "bin"),
        P("seg"),
        P("bin"),
    )
    n_seg, n_bin = mesh.shape["seg"], mesh.shape["bin"]
    on_device = line_on_device if n_seg == 2 * LINE else halving_on_device
    return jax.shard_map(
        functools.partial(on_device, n_seg, n_bin),
        mesh=mesh,
        in_specs=placed,
        out_specs=(P("seg", "bin"), P("seg", "bin"), P("seg")),
        check_vma=False,
    )
```
